32 devices in a mesh: tm: 8 (over z, y), coef: 4 (over x, core).
Axes of the slice: x: 2, y: 2, z: 4, core: 2. Of those that a mesh axis runs over, the one named last changes fastest.
Arguments:
- design: bfloat16 [2048, 50176], P('tm', 'coef'), may hold values from -0.0390625 to 0.0390625
- observed: float32 [2048, 128], P('tm'), may hold values from -6 to 6
- slab_counts: int32 [8], P('tm'), may hold values from 128 to 256, as said below
- gap_mask: int32 [2048], P('tm'), may hold values 0 or 1
- filter_taps: float32 [128], replicated, may hold values from -0.5 to 1.2, as said below
- kaula_diag: float32 [50176], P('coef'), may hold values from 0.1 to 1
- precond: float32 [50176], P('coef'), may hold values from 0.3 to 3
Outputs:
- solution: float32 [50176, 128], P(('coef', 'tm'))
- residual: float32 [50176, 128], P(('coef', 'tm'))
The draws below stay inside these ranges and needn't reach their ends.
Inputs may be any that keep to these rules, and one draw needn't show every extreme that they name: `slab_counts`: every slab holds at most 256 valid epochs, and some slab holds exactly 256. filter_taps[0] lies between 1 and 1.2.
All inputs are finite; a program needn't handle non-finite values. No bound on the sum of `gap_mask` on one device may be relied on, other than what follows from the above.
Results may differ from the reference program's by a relative error of at most 0.0065.
The reference program's roundings to bfloat16 on the way (of `weighted`) count: a program that leaves them out, or rounds other values in their place, can miss the bound.
Values may be sent and summed in bfloat16 or wider, within the bound.
A program may use at most 64 MiB of HBM per device.

```python
import math
import jax
import jax.numpy as jnp
from jax import lax

NC = 50176
R = 128
E_DEV = 256
BAND = 128
ITERS = 2
EPOCHS = 2048
N_TM = 8


def draw_slab_counts(key, part):
    first_key = jax.random.fold_in(key, 11)
    second_key = jax.random.fold_in(key, 12)
    values = jax.random.randint(first_key, (N_TM,), E_DEV // 2, E_DEV + 1)
    chosen = jax.random.randint(second_key, (), 0, N_TM)
    return jnp.where(jnp.arange(N_TM) == chosen, E_DEV, values).astype(jnp.int32)


def draw_filter_taps(key, part):
    first_key = jax.random.fold_in(key, 21)
    second_key = jax.random.fold_in(key, 22)
    lags = jnp.arange(BAND).astype(jnp.float32)
    decay = jnp.exp(-1.5 * lags / BAND)
    noise = 0.12 * jnp.clip(jax.random.normal(first_key, (BAND,), jnp.float32), -4.0, 4.0)
    leading = 1.0 + 0.2 * jax.random.uniform(second_key, (BAND,), jnp.float32)
    return jnp.where(lags == 0.0, leading, decay * noise).astype(jnp.float32)


def plant(values, rng, smallest, high):
    place = [jax.random.randint(jax.random.fold_in(rng, axis), (), 0, length) for axis, length in enumerate(values.shape)]
    widest = values.shape.index(max(values.shape))
    next_to = place[:widest] + [(place[widest] + 1) % values.shape[widest]] + place[widest + 1:]
    return values.at[tuple(place)].set(smallest).at[tuple(next_to)].set(high)


def with_spikes(drawn, rng, source, target, parts, factor):
    def block_of(dim):
        return (jnp.arange(drawn.shape[dim]) // (drawn.shape[dim] // parts)).reshape((-1,) + (1,) * (drawn.ndim - 1 - dim))

    one_side = jax.random.permutation(rng, parts)[block_of(target)]
    second = (block_of(target) + parts // 2) % parts
    return jnp.where((block_of(source) == one_side) | (block_of(source) == second), factor * drawn, drawn)


def shard_levels(stream_key, extent, split, low, top_value):
    factor_of, own = 1.0, jax.random.fold_in(stream_key, 6)
    for axis_at, parts in split:
        heights = jnp.exp(jax.random.uniform(jax.random.fold_in(own, axis_at), (parts,), jnp.float32, low / len(split), top_value / len(split)))
        factor_of = factor_of * jnp.repeat(heights, extent[axis_at] // parts).reshape([-1 if axis == axis_at else 1 for axis in range(len(extent))])
    return factor_of


def centred(own_key, dims, scale, reach, pieces=(), kind=jnp.bfloat16):
    values = scale * jax.random.normal(own_key, dims, jnp.float32)
    if pieces:
        values = values * shard_levels(own_key, dims, pieces, -0.22, 0.18)
    return jnp.clip(values, -reach, reach).astype(kind)


def noise_with(rng, dims, scale, reach, split, heavy, held_as=jnp.bfloat16):
    values = scale * jax.random.normal(rng, dims, jnp.float32)
    if split:
        values = values * shard_levels(rng, dims, split, -0.22, 0.18)
    return jnp.clip(with_spikes(values, jax.random.fold_in(rng, 3), *heavy), -reach, reach).astype(held_as)


def setup_inputs(seed: int = 0) -> dict:
    key_list = jax.random.split(jax.random.key(seed), 8)
    return {
        "design": noise_with(key_list[0], (EPOCHS, NC), NC ** -0.5, 0.0390625, ((0, 8), (1, 4)), (0, 1, 8, 2.0)),
        "observed": centred(key_list[1], (EPOCHS, R), 1.0, 6.0, ((0, 8),), jnp.float32),
        "slab_counts": draw_slab_counts(jax.random.fold_in(key_list[7], 71), 0),
        "gap_mask": plant((jax.random.randint(key_list[3], (EPOCHS,), 0, 8) < 7).astype(jnp.int32), jax.random.fold_in(key_list[3], 1), 0, 1),
        "filter_taps": draw_filter_taps(jax.random.fold_in(key_list[7], 71), 0),
        "kaula_diag": jnp.clip(jnp.exp(math.log(1.0) - 2.3025851 * jax.random.uniform(key_list[5], (NC,), jnp.float32) ** shard_levels(key_list[5], (NC,), ((0, 4),), -0.2, 0.2)), 0.1, 1.0),
        "precond": jnp.clip(jnp.exp(math.log(3.0) - 2.3025851 * jax.random.uniform(key_list[6], (NC,), jnp.float32) ** shard_levels(key_list[6], (NC,), ((0, 4),), -0.2, 0.2)), 0.3, 3.0),
    }


def toeplitz(pattern, band_len):
    tiled = jnp.tile(pattern, band_len)[: band_len * (2 * band_len - 1)]
    return tiled.reshape(band_len, 2 * band_len - 1)[:, :band_len]


def block_pair(filter_taps):
    band_len = filter_taps.shape[0]
    spacer = jnp.zeros((band_len,), jnp.float32)
    reversed_taps = filter_taps[:0:-1]
    lower = jnp.concatenate([filter_taps[:1], spacer, reversed_taps])
    upper = jnp.concatenate([jnp.zeros((1,), jnp.float32), reversed_taps, spacer])
    return toeplitz(lower, band_len), toeplitz(upper, band_len)


def forward(values, lower_block, upper_block):
    band_len = lower_block.shape[0]
    blocks = values.reshape(-1, band_len, values.shape[1])
    previous = jnp.concatenate([jnp.zeros_like(blocks[:1]), blocks[:-1]], 0)
    result = jnp.einsum("ij,bjr->bir", lower_block, blocks, precision=lax.Precision.HIGHEST)
    result = result + jnp.einsum("ij,bjr->bir", upper_block, previous, precision=lax.Precision.HIGHEST)
    return result.reshape(values.shape)


def backward(values, lower_block, upper_block):
    band_len = lower_block.shape[0]
    blocks = values.reshape(-1, band_len, values.shape[1])
    following = jnp.concatenate([blocks[1:], jnp.zeros_like(blocks[:1])], 0)
    result = jnp.einsum("ji,bjr->bir", lower_block, blocks, precision=lax.Precision.HIGHEST)
    result = result + jnp.einsum("ji,bjr->bir", upper_block, following, precision=lax.Precision.HIGHEST)
    return result.reshape(values.shape)


def reference(design, observed, slab_counts, gap_mask, filter_taps, kaula_diag, precond):
    lower_block, upper_block = block_pair(filter_taps)
    position = jnp.arange(EPOCHS, dtype=jnp.int32)
    slab_index = position // E_DEV
    weight = ((gap_mask == 1) & (position % E_DEV < slab_counts[slab_index])).astype(jnp.float32)[:, None]

    def weighted(values):
        inner = forward(weight * values, lower_block, upper_block)
        return (weight * backward(inner, lower_block, upper_block)).astype(jnp.bfloat16)

    def transposed(filtered):
        return lax.dot_general(design, filtered, (((0,), (0,)), ((), ())), preferred_element_type=jnp.float32)

    kaula_col = kaula_diag[:, None]
    precond_col = precond[:, None]
    residual = transposed(weighted(observed))
    solution = jnp.zeros_like(residual)
    scaled = precond_col * residual
    direction = scaled
    norm_now = jnp.sum(residual * scaled, 0)
    for iteration in range(ITERS):
        slab_values = jnp.dot(design, direction.astype(jnp.bfloat16), preferred_element_type=jnp.float32)
        image = transposed(weighted(slab_values)) + kaula_col * direction
        step_len = norm_now / jnp.sum(direction * image, 0)
        solution = solution + step_len * direction
        residual = residual - step_len * image
        scaled = precond_col * residual
        norm_next = jnp.sum(residual * scaled, 0)
        direction = scaled + (norm_next / norm_now) * direction
        norm_now = norm_next
    return solution, residual
```

```python
import functools

import jax
import jax.numpy as jnp
from jax import lax
from jax.experimental import pallas as pl
from jax.experimental.pallas import tpu as pltpu
from jax.sharding import PartitionSpec as P

ITERS = 2
HIGHEST = lax.Precision.HIGHEST


def toeplitz(pattern, band_len):
    tiled = jnp.tile(pattern, band_len)[: band_len * (2 * band_len - 1)]
    return tiled.reshape(band_len, 2 * band_len - 1)[:, :band_len]


def block_pair(filter_taps):
    band_len = filter_taps.shape[0]
    spacer = jnp.zeros((band_len,), jnp.float32)
    reversed_taps = filter_taps[:0:-1]
    lower = jnp.concatenate([filter_taps[:1], spacer, reversed_taps])
    upper = jnp.concatenate([jnp.zeros((1,), jnp.float32), reversed_taps, spacer])
    return (toeplitz(lower, band_len), toeplitz(upper, band_len))


def forward(values, lower_block, upper_block):
    band_len = lower_block.shape[0]
    blocks = values.reshape(-1, band_len, values.shape[1])
    previous = jnp.concatenate([jnp.zeros_like(blocks[:1]), blocks[:-1]], 0)
    result = jnp.einsum("ij,bjr->bir", lower_block, blocks, precision=HIGHEST)
    result = result + jnp.einsum("ij,bjr->bir", upper_block, previous, precision=HIGHEST)
    return result.reshape(values.shape)


def backward(values, lower_block, upper_block):
    band_len = lower_block.shape[0]
    blocks = values.reshape(-1, band_len, values.shape[1])
    following = jnp.concatenate([blocks[1:], jnp.zeros_like(blocks[:1])], 0)
    result = jnp.einsum("ji,bjr->bir", lower_block, blocks, precision=HIGHEST)
    result = result + jnp.einsum("ji,bjr->bir", upper_block, following, precision=HIGHEST)
    return result.reshape(values.shape)


def general_shards(design, observed, slab_counts, gap_mask, filter_taps, kaula_diag, precond):
    epoch_rows, coef_rows = design.shape
    columns = observed.shape[1]
    slabs = lax.axis_size("tm")
    epochs = slabs * epoch_rows
    owned_rows = coef_rows // slabs
    owner_index = lax.axis_index("tm")
    lower_block, upper_block = block_pair(filter_taps)
    position = jnp.arange(epoch_rows, dtype=jnp.int32)
    local_weight = ((gap_mask == 1) & (position < slab_counts[0])).astype(jnp.float32)
    packed = jnp.concatenate([observed, local_weight.reshape(-1, columns)], 0)
    gathered = lax.all_gather(packed, "tm", axis=0, tiled=False)
    all_observed = gathered[:, :epoch_rows].reshape(epochs, columns)
    weight = gathered[:, epoch_rows:].reshape(epochs, 1)
    block = lax.all_to_all(design, "tm", split_axis=1, concat_axis=0, tiled=True)

    def weighted(values):
        inner = forward(weight * values, lower_block, upper_block)
        return (weight * backward(inner, lower_block, upper_block)).astype(jnp.bfloat16)

    def transposed(filtered):
        return lax.dot_general(
            block, filtered, (((0,), (0,)), ((), ())), preferred_element_type=jnp.float32
        )

    def summed(scaled, terms):
        partial = jnp.dot(block, scaled.astype(jnp.bfloat16), preferred_element_type=jnp.float32)
        rows = [jnp.sum(term, 0)[None] for term in terms]
        rows.append(jnp.zeros((8 - len(rows), columns), jnp.float32))
        total = lax.psum(jnp.concatenate([partial] + rows, 0), ("tm", "coef"))
        return total[:epochs], [total[epochs + at] for at in range(len(terms))]

    start = owner_index * owned_rows
    kaula_col = lax.dynamic_slice_in_dim(kaula_diag, start, owned_rows, 0)[:, None]
    precond_col = lax.dynamic_slice_in_dim(precond, start, owned_rows, 0)[:, None]
    residual = transposed(weighted(all_observed))
    solution = jnp.zeros_like(residual)
    for iteration in range(ITERS):
        scaled = precond_col * residual
        terms = [residual * scaled, kaula_col * scaled * scaled]
        if iteration == 0:
            slab_values, (norm_now, ridge) = summed(scaled, terms)
            direction = scaled
        else:
            terms.append(kaula_col * scaled * direction)
            fresh, (norm_next, own_ridge, cross) = summed(scaled, terms)
            ratio = norm_next / norm_now
            slab_values = fresh + ratio * slab_values
            ridge = own_ridge + ratio * (2.0 * cross + ratio * ridge)
            direction = scaled + ratio * direction
            norm_now = norm_next
        filtered = weighted(slab_values)
        curvature = ridge + jnp.sum(slab_values * filtered.astype(jnp.float32), 0)
        step_len = norm_now / curvature
        image = transposed(filtered) + kaula_col * direction
        solution = solution + step_len * direction
        residual = residual - step_len * image
    return (solution, residual)


LANES = 128
MESH = pl.DeviceIdType.MESH


class Plan:
    def __init__(self, slabs, coefs, epoch_rows, coef_rows, columns):
        self.slabs, self.coefs, self.epoch_rows, self.columns = slabs, coefs, epoch_rows, columns
        self.owned = coef_rows // slabs
        last = coef_rows // LANES
        tiles = 0
        for owner in range(slabs):
            first = owner * self.owned // LANES
            tiles = max(tiles, (owner * self.owned + self.owned - 1) // LANES - first + 1)
        self.width = tiles * LANES
        self.last_tile = last - tiles
        self.across = coefs // 2
        self.chips = slabs * self.across
        self.group = columns // self.chips
        self.blocks = slabs * epoch_rows // LANES
        self.half = slabs * epoch_rows // 2
        self.message = self.half + LANES

    def first_tile(self, owner):
        return lax.min(lax.div(owner * self.owned, LANES), self.last_tile)


def fits(slabs, coefs, epoch_rows, coef_rows, columns, taps):
    power = slabs & (slabs - 1) == 0
    if not power or slabs < 2 or coefs % 2 or coef_rows % LANES or coef_rows % slabs or epoch_rows % LANES:
        return False
    return taps == LANES and columns == LANES and columns == 8 * slabs * coefs // 2


def flipped(index, bits, count):
    result, weight = 0, 1
    while weight < count:
        bit = lax.rem(lax.div(index, weight), 2)
        result = result + weight * (1 - bit if bits & weight else bit)
        weight *= 2
    return result


def pieces(values):
    high = values.astype(jnp.bfloat16).astype(jnp.float32)
    rest = values - high
    middle = rest.astype(jnp.bfloat16).astype(jnp.float32)
    low = (rest - middle).astype(jnp.bfloat16).astype(jnp.float32)
    return high + pltpu.roll(middle, 8, 1) + pltpu.roll(low, 16, 1)


def joined(values, at):
    lane = lax.broadcasted_iota(jnp.int32, values.shape, 1)
    taken = (lane % 8 == at) & (lane < 24)
    return jnp.sum(jnp.where(taken, values, 0.0), 1, keepdims=True)


def in_lanes(terms, rows):
    lane = lax.broadcasted_iota(jnp.int32, (rows, LANES), 1)
    result = jnp.zeros((rows, LANES), jnp.float32)
    for at, term in enumerate(terms):
        result = jnp.where(lane == at, term, result)
    return result


def product(left, right, contract, precision=None):
    return lax.dot_general(
        left, right, ((contract[0], contract[1]), ((), ())),
        precision=precision, preferred_element_type=jnp.float32,
    )


NN = ((1,), (0,))
NT = ((1,), (1,))


def fused(plan, design, observed, gap, counts, taps, kaula, precond, solution_out, residual_out,
          block, shown, seen, sums, sent, received, total, whole, folded, filtered, gathered, folded_in,
          resid, direc, scal, solut, image, first_values,
          own_sem, block_send, block_recv, show_send, show_recv, pair_send, pair_recv,
          fold_send, fold_recv, whole_send, whole_recv, gather_send, gather_recv, relay_send, relay_recv):
    slabs, chips, group, rows = plan.slabs, plan.chips, plan.group, plan.epoch_rows
    half_slabs = slabs // 2
    slab, coef = lax.axis_index("tm"), lax.axis_index("coef")
    across, core = lax.div(coef, 2), lax.rem(coef, 2)
    chip = slab * plan.across + across

    def device(at):
        return {"tm": lax.div(at, plan.across), "coef": 2 * lax.rem(at, plan.across) + core}

    partner = {"tm": slab, "coef": 2 * across + 1 - core}

    def other(step):
        return lax.rem(chip + step, chips)

    def remote(src, dst, send, recv, target):
        return pltpu.make_async_remote_copy(
            src_ref=src, dst_ref=dst, send_sem=send, recv_sem=recv, device_id=target, device_id_type=MESH
        )

    barrier = pltpu.get_barrier_semaphore()
    for step in range(1, chips):
        pl.semaphore_signal(barrier, inc=1, device_id=device(other(step)), device_id_type=MESH)
    pl.semaphore_signal(barrier, inc=1, device_id=partner, device_id_type=MESH)

    place = lax.broadcasted_iota(jnp.int32, (1, rows), 1)
    weight_row = jnp.where((gap[...] == 1) & (place < counts[0]), 1.0, 0.0)
    turned = observed[...].T * weight_row
    shown[:, :group, :] = turned.reshape(chips, group, rows)
    shown[:, group:, :] = jnp.broadcast_to(weight_row[None], (chips, group, rows))
    seen[slab] = shown[chip]

    first = plan.first_tile(slab)
    cut = plan.width // LANES // 2 * LANES
    parts = ((0, cut), (cut, plan.width - cut))

    def block_copy(bits, part):
        peer = flipped(slab, bits, slabs)
        low, size = parts[part]
        src = design.at[:, pl.ds(pl.multiple_of(plan.first_tile(peer) * LANES + low, LANES), size)]
        dst = block.at[slab, :, pl.ds(low, size)]
        return remote(src, dst, block_send.at[part, peer], block_recv.at[part, slab], {"tm": peer, "coef": coef})

    def block_arrival(bits, part):
        peer = flipped(slab, bits, slabs)
        low, size = parts[part]
        dst = block.at[peer, :, pl.ds(low, size)]
        return remote(dst, dst, block_send.at[part, peer], block_recv.at[part, peer], {"tm": peer, "coef": coef})

    def show_copy(bits):
        peer = flipped(slab, bits, slabs)
        src = shown.at[peer * plan.across + across]
        return remote(src, seen.at[slab], show_send.at[peer], show_recv.at[slab], {"tm": peer, "coef": coef})

    def show_arrival(bits):
        peer = flipped(slab, bits, slabs)
        return remote(seen.at[peer], seen.at[peer], show_send.at[peer], show_recv.at[peer], {"tm": peer, "coef": coef})

    own = pltpu.make_async_copy(
        design.at[:, pl.ds(pl.multiple_of(first * LANES, LANES), plan.width)], block.at[slab], own_sem
    )
    own.start()
    pl.semaphore_wait(barrier, chips)
    for bits in range(1, slabs):
        show_copy(bits).start()
    for bits in range(1, slabs):
        block_copy(bits, 0).start()

    base = jnp.concatenate([taps[...], jnp.zeros((1, LANES), jnp.float32)], 1)
    shifted = pltpu.roll(jnp.broadcast_to(base, (LANES, 2 * LANES)), 0, 1, stride=1, stride_axis=0)
    lower, upper = shifted[:, :LANES], shifted[:, LANES:]
    blank = jnp.zeros((group, LANES), jnp.float32)

    for bits in range(1, slabs):
        show_arrival(bits).wait_recv()

    def stack(ref, low):
        return jnp.concatenate(
            [ref[at, low:low + group, j * LANES:(j + 1) * LANES] for at in range(slabs) for j in range(rows // LANES)], 0
        )

    weight = stack(seen, group)

    def weighted(values):
        entering = weight * values
        before = jnp.concatenate([blank, entering[:-group]], 0)
        inner = product(entering, lower, NN, lax.Precision.HIGHEST) + product(before, upper, NN, lax.Precision.HIGHEST)
        after = jnp.concatenate([inner[group:], blank], 0)
        outer = product(inner, lower, NT, lax.Precision.HIGHEST) + product(after, upper, NT, lax.Precision.HIGHEST)
        return (weight * outer).astype(jnp.bfloat16)

    def gather_start(phase, values, terms):
        wide = values.astype(jnp.float32)
        for half in range(2):
            for j in range(plan.blocks // 2):
                low = (half * (plan.blocks // 2) + j) * group
                folded[half, :, j * LANES:(j + 1) * LANES] = wide[low:low + group]
            folded[half, :, plan.half:] = pieces(in_lanes(terms, group))
        gathered[phase, core, chip] = folded[core].astype(jnp.bfloat16)

        def send(step, carry):
            to = other(step)
            here = gathered.at[phase, core, chip]
            remote(here, here, gather_send.at[phase, to], gather_recv.at[phase, chip], device(to)).start()
            return carry

        lax.fori_loop(1, chips, send, 0)

    def gather_finish(phase):
        def arrive(step, carry):
            at = other(step)
            here = gathered.at[phase, core, at]
            remote(here, here, gather_send.at[phase, at], gather_recv.at[phase, at], device(at)).wait_recv()
            return carry

        lax.fori_loop(1, chips, arrive, 0)
        mine, theirs = gathered.at[phase, core], gathered.at[phase, 1 - core]
        remote(mine, mine, relay_send.at[phase], relay_recv.at[phase], partner).start()
        remote(theirs, theirs, relay_send.at[phase], relay_recv.at[phase], partner).wait_recv()
        for half in range(2):
            for j in range(half_slabs):
                values = gathered[phase, half, :, :, j * rows:(j + 1) * rows].astype(jnp.float32)
                filtered[half * half_slabs + j] = values.reshape(plan.columns, rows).astype(jnp.bfloat16)
        terms = gathered[phase, 0, :, :, plan.half:].astype(jnp.float32).reshape(plan.columns, LANES)
        return joined(terms, 0), joined(terms, 1)

    gather_start(0, weighted(stack(seen, 0)), [])
    for bits in range(1, slabs):
        block_copy(bits, 1).start()

    spread = pl.ds(pl.multiple_of(first * LANES, LANES), plan.width)
    ridge_row = kaula[:, spread]
    lane = lax.broadcasted_iota(jnp.int32, (1, plan.width), 1) + (first * LANES - slab * plan.owned)
    scale_row = jnp.where((lane >= 0) & (lane < plan.owned), precond[:, spread], 0.0)

    gather_finish(0)
    own.wait()
    resid[...] = product(filtered[slab], block[slab], NN)
    for bits in range(1, slabs):
        for part in range(2):
            block_arrival(bits, part).wait_recv()
        peer = flipped(slab, bits, slabs)
        resid[...] += product(filtered[peer], block[peer], NN)

    def summed(turn, values, terms):
        low = values.astype(jnp.bfloat16)

        def one(half):
            def body(at, carry):
                sums[turn, half, at] = product(low, block[half * half_slabs + at], NT)
                return carry

            lax.fori_loop(0, half_slabs, body, 0)

        one(0)
        one(1)
        scalars = in_lanes(terms, plan.columns)
        for half in range(2):
            sums[turn, half, half_slabs, :, :LANES] = scalars
        remote(sums.at[turn, 1 - core], received.at[turn], pair_send.at[turn], pair_recv.at[turn], partner).start()
        remote(sums.at[turn, 1 - core], received.at[turn], pair_send.at[turn], pair_recv.at[turn], partner).wait_recv()
        for at in range(half_slabs):
            values = (sums[turn, core, at] + received[turn, at]).reshape(chips, group, rows)
            total[:, :, at * rows:(at + 1) * rows] = values
            sent[turn, :, :, at * rows:(at + 1) * rows] = values.astype(jnp.bfloat16)
        scalars = sums[turn, core, half_slabs, :, :LANES] + received[turn, half_slabs, :, :LANES]
        total[:, :, plan.half:] = scalars.reshape(chips, group, LANES)
        sent[turn, :, :, plan.half:] = pieces(scalars).reshape(chips, group, LANES).astype(jnp.bfloat16)

        def send(step, carry):
            to = other(step)
            remote(sent.at[turn, to], folded_in.at[turn, chip], fold_send.at[turn, to], fold_recv.at[turn, chip], device(to)).start()
            return carry

        lax.fori_loop(1, chips, send, 0)

        def arrive(step, carry):
            at = other(step)
            here = folded_in.at[turn, at]
            remote(here, here, fold_send.at[turn, at], fold_recv.at[turn, at], device(at)).wait_recv()
            return carry + folded_in[turn, at].astype(jnp.float32)

        whole[turn, core] = lax.fori_loop(1, chips, arrive, total[chip])
        mine, theirs = whole.at[turn, core], whole.at[turn, 1 - core]
        remote(mine, mine, whole_send.at[turn], whole_recv.at[turn], partner).start()
        remote(theirs, theirs, whole_send.at[turn], whole_recv.at[turn], partner).wait_recv()
        values = jnp.concatenate(
            [whole[turn, half, :, j * LANES:(j + 1) * LANES] for half in range(2) for j in range(plan.blocks // 2)], 0
        )
        terms = whole[turn, 0, :, plan.half:]
        return values, joined(terms, 0), joined(terms, 1), joined(terms, 2)

    def inner(left, right):
        together = (left * right).reshape(plan.blocks, group, LANES)
        return jnp.sum(jnp.sum(together, 0), 1, keepdims=True)

    def transposed():
        image[...] = product(filtered[0], block[0], NN)

        def body(at, carry):
            image[...] += product(filtered[at], block[at], NN)
            return carry

        lax.fori_loop(1, slabs, body, 0)

    def over(terms):
        return jnp.sum(terms, 1, keepdims=True)

    direc[...] = scale_row * resid[...]
    ridged = ridge_row * direc[...]
    terms = [over(resid[...] * direc[...]), over(ridged * direc[...])]
    values, norm, ridge, _ = summed(0, direc[...], terms)
    first_values[...] = values
    kept = weighted(values)
    step_len = norm / (ridge + inner(values, kept.astype(jnp.float32)))
    gather_start(1, kept, [step_len])
    step_col, _ = gather_finish(1)
    transposed()
    resid[...] = resid[...] - step_col * (image[...] + ridge_row * direc[...])
    solut[...] = step_col * direc[...]
    scal[...] = scale_row * resid[...]
    ridged = ridge_row * scal[...]
    terms = [over(resid[...] * scal[...]), over(ridged * scal[...]), over(ridged * direc[...])]
    fresh, norm_next, own_ridge, cross = summed(1, scal[...], terms)
    ratio = norm_next / norm
    ridge = own_ridge + ratio * (2.0 * cross + ratio * ridge)
    values = fresh + jnp.concatenate([ratio] * plan.blocks, 0) * first_values[...]
    kept = weighted(values)
    step_len = norm_next / (ridge + inner(values, kept.astype(jnp.float32)))
    gather_start(2, kept, [step_len, ratio])
    step_col, ratio_col = gather_finish(2)
    transposed()
    for at in range(plan.width // LANES):
        cols = slice(at * LANES, (at + 1) * LANES)
        along = scal[:, cols] + ratio_col * direc[:, cols]
        ahead = solut[:, cols] + step_col * along
        left = resid[:, cols] - step_col * (image[:, cols] + ridge_row[:, cols] * along)
        solution_out[cols, :] = ahead.T
        residual_out[cols, :] = left.T

    for bits in range(1, slabs):
        show_copy(bits).wait_send()
        for part in range(2):
            block_copy(bits, part).wait_send()
    for phase in range(3):
        here = gathered.at[phase, core, chip]
        for step in range(1, chips):
            to = other(step)
            remote(here, here, gather_send.at[phase, to], gather_recv.at[phase, chip], device(to)).wait_send()
        mine = gathered.at[phase, core]
        remote(mine, mine, relay_send.at[phase], relay_recv.at[phase], partner).wait_send()
    for turn in range(2):
        remote(sums.at[turn, 1 - core], received.at[turn], pair_send.at[turn], pair_recv.at[turn], partner).wait_send()
        for step in range(1, chips):
            to = other(step)
            remote(sent.at[turn, to], folded_in.at[turn, chip], fold_send.at[turn, to], fold_recv.at[turn, chip], device(to)).wait_send()
        mine = whole.at[turn, core]
        remote(mine, mine, whole_send.at[turn], whole_recv.at[turn], partner).wait_send()


def fused_shards(design, observed, slab_counts, gap_mask, filter_taps, kaula_diag, precond):
    epoch_rows, coef_rows = design.shape
    columns = observed.shape[1]
    slabs, coefs = lax.axis_size("tm"), lax.axis_size("coef")
    plan = Plan(slabs, coefs, epoch_rows, coef_rows, columns)
    wide, chips, group = plan.width, plan.chips, plan.group
    f32, bf16 = jnp.float32, jnp.bfloat16
    vmem = pl.BlockSpec(memory_space=pltpu.VMEM)
    sem = pltpu.SemaphoreType.DMA
    shape = jax.ShapeDtypeStruct((wide, columns), f32)
    outs = pl.pallas_call(
        functools.partial(fused, plan),
        out_shape=(shape, shape),
        in_specs=[pl.BlockSpec(memory_space=pl.ANY), vmem, vmem, pl.BlockSpec(memory_space=pltpu.SMEM), vmem, vmem, vmem],
        out_specs=(vmem, vmem),
        scratch_shapes=[
            pltpu.VMEM((slabs, epoch_rows, wide), bf16),
            pltpu.VMEM((chips, 2 * group, epoch_rows), f32),
            pltpu.VMEM((slabs, 2 * group, epoch_rows), f32),
            pltpu.VMEM((2, 2, slabs // 2 + 1, columns, epoch_rows), f32),
            pltpu.VMEM((2, chips, group, plan.message), bf16),
            pltpu.VMEM((2, slabs // 2 + 1, columns, epoch_rows), f32),
            pltpu.VMEM((chips, group, plan.message), f32),
            pltpu.VMEM((2, 2, group, plan.message), f32),
            pltpu.VMEM((2, group, plan.message), f32),
            pltpu.VMEM((slabs, columns, epoch_rows), bf16),
            pltpu.VMEM((3, 2, chips, group, plan.message), bf16),
            pltpu.VMEM((2, chips, group, plan.message), bf16),
            pltpu.VMEM((columns, wide), f32),
            pltpu.VMEM((columns, wide), f32),
            pltpu.VMEM((columns, wide), f32),
            pltpu.VMEM((columns, wide), f32),
            pltpu.VMEM((columns, wide), f32),
            pltpu.VMEM((plan.blocks * group, LANES), f32),
            sem(()), sem((2, slabs)), sem((2, slabs)), sem((slabs,)), sem((slabs,)), sem((2,)), sem((2,)),
            sem((2, chips)), sem((2, chips)), sem((2,)), sem((2,)),
            sem((3, chips)), sem((3, chips)), sem((3,)), sem((3,)),
        ],
        compiler_params=pltpu.CompilerParams(
            collective_id=0, has_side_effects=True, vmem_limit_bytes=48 * 1024 * 1024
        ),
    )(design, observed, gap_mask[None], slab_counts, filter_taps[None], kaula_diag[None], precond[None])
    start = lax.axis_index("tm") * plan.owned
    low = start - plan.first_tile(lax.axis_index("tm")) * LANES
    return tuple(lax.dynamic_slice_in_dim(out, low, plan.owned, 0) for out in outs)


def shards(*arrays):
    design, observed, filter_taps = arrays[0], arrays[1], arrays[4]
    sizes = (lax.axis_size("tm"), lax.axis_size("coef"), *design.shape, observed.shape[1], filter_taps.shape[0])
    return fused_shards(*arrays) if fits(*sizes) else general_shards(*arrays)


def solution(mesh):
    placed = (P("tm", "coef"), P("tm", None), P("tm"), P("tm"), P(), P("coef"), P("coef"))
    return jax.shard_map(
        shards,
        mesh=mesh,
        in_specs=placed,
        out_specs=(P(("coef", "tm"), None), P(("coef", "tm"), None)),
        check_vma=False,
    )
```

```python
import functools

import jax
import jax.numpy as jnp
from jax import lax
from jax.experimental import pallas as pl
from jax.experimental.pallas import tpu as pltpu
from jax.sharding import PartitionSpec as P

ITERS = 2
HIGHEST = lax.Precision.HIGHEST


def toeplitz(pattern, band_len):
    tiled = jnp.tile(pattern, band_len)[: band_len * (2 * band_len - 1)]
    return tiled.reshape(band_len, 2 * band_len - 1)[:, :band_len]


def block_pair(filter_taps):
    band_len = filter_taps.shape[0]
    spacer = jnp.zeros((band_len,), jnp.float32)
    reversed_taps = filter_taps[:0:-1]
    lower = jnp.concatenate([filter_taps[:1], spacer, reversed_taps])
    upper = jnp.concatenate([jnp.zeros((1,), jnp.float32), reversed_taps, spacer])
    return (toeplitz(lower, band_len), toeplitz(upper, band_len))


def forward(values, lower_block, upper_block):
    band_len = lower_block.shape[0]
    blocks = values.reshape(-1, band_len, values.shape[1])
    previous = jnp.concatenate([jnp.zeros_like(blocks[:1]), blocks[:-1]], 0)
    result = jnp.einsum("ij,bjr->bir", lower_block, blocks, precision=HIGHEST)
    result = result + jnp.einsum("ij,bjr->bir", upper_block, previous, precision=HIGHEST)
    return result.reshape(values.shape)


def backward(values, lower_block, upper_block):
    band_len = lower_block.shape[0]
    blocks = values.reshape(-1, band_len, values.shape[1])
    following = jnp.concatenate([blocks[1:], jnp.zeros_like(blocks[:1])], 0)
    result = jnp.einsum("ji,bjr->bir", lower_block, blocks, precision=HIGHEST)
    result = result + jnp.einsum("ji,bjr->bir", upper_block, following, precision=HIGHEST)
    return result.reshape(values.shape)


def general_shards(design, observed, slab_counts, gap_mask, filter_taps, kaula_diag, precond):
    epoch_rows, coef_rows = design.shape
    columns = observed.shape[1]
    slabs = lax.axis_size("tm")
    epochs = slabs * epoch_rows
    owned_rows = coef_rows // slabs
    owner_index = lax.axis_index("tm")
    lower_block, upper_block = block_pair(filter_taps)
    position = jnp.arange(epoch_rows, dtype=jnp.int32)
    local_weight = ((gap_mask == 1) & (position < slab_counts[0])).astype(jnp.float32)
    packed = jnp.concatenate([observed, local_weight.reshape(-1, columns)], 0)
    gathered = lax.all_gather(packed, "tm", axis=0, tiled=False)
    all_observed = gathered[:, :epoch_rows].reshape(epochs, columns)
    weight = gathered[:, epoch_rows:].reshape(epochs, 1)
    block = lax.all_to_all(design, "tm", split_axis=1, concat_axis=0, tiled=True)

    def weighted(values):
        inner = forward(weight * values, lower_block, upper_block)
        return (weight * backward(inner, lower_block, upper_block)).astype(jnp.bfloat16)

    def transposed(filtered):
        return lax.dot_general(
            block, filtered, (((0,), (0,)), ((), ())), preferred_element_type=jnp.float32
        )

    def summed(scaled, terms):
        partial = jnp.dot(block, scaled.astype(jnp.bfloat16), preferred_element_type=jnp.float32)
        rows = [jnp.sum(term, 0)[None] for term in terms]
        rows.append(jnp.zeros((8 - len(rows), columns), jnp.float32))
        total = lax.psum(jnp.concatenate([partial] + rows, 0), ("tm", "coef"))
        return total[:epochs], [total[epochs + at] for at in range(len(terms))]

    start = owner_index * owned_rows
    kaula_col = lax.dynamic_slice_in_dim(kaula_diag, start, owned_rows, 0)[:, None]
    precond_col = lax.dynamic_slice_in_dim(precond, start, owned_rows, 0)[:, None]
    residual = transposed(weighted(all_observed))
    solution = jnp.zeros_like(residual)
    for iteration in range(ITERS):
        scaled = precond_col * residual
        terms = [residual * scaled, kaula_col * scaled * scaled]
        if iteration == 0:
            slab_values, (norm_now, ridge) = summed(scaled, terms)
            direction = scaled
        else:
            terms.append(kaula_col * scaled * direction)
            fresh, (norm_next, own_ridge, cross) = summed(scaled, terms)
            ratio = norm_next / norm_now
            slab_values = fresh + ratio * slab_values
            ridge = own_ridge + ratio * (2.0 * cross + ratio * ridge)
            direction = scaled + ratio * direction
            norm_now = norm_next
        filtered = weighted(slab_values)
        curvature = ridge + jnp.sum(slab_values * filtered.astype(jnp.float32), 0)
        step_len = norm_now / curvature
        image = transposed(filtered) + kaula_col * direction
        solution = solution + step_len * direction
        residual = residual - step_len * image
    return (solution, residual)


LANES = 128
GROUP = 8
MESH = pl.DeviceIdType.MESH
NN = ((1,), (0,))
NT = ((1,), (1,))


class Plan:
    def __init__(self, slabs, coefs, epoch_rows, coef_rows, columns):
        self.slabs, self.coefs, self.epoch_rows, self.columns = slabs, coefs, epoch_rows, columns
        self.tiles = coef_rows // LANES
        self.owned = coef_rows // slabs
        self.full = self.owned // LANES - 1
        self.rest = self.owned % LANES
        self.packed_rows = epoch_rows * self.rest // LANES
        self.mixed_at = self.full * LANES
        self.width = (self.full + 2) * LANES
        self.cut = self.full * 3 // 4 * LANES
        self.across = coefs // 2
        self.chips = slabs * self.across
        self.blocks = slabs * epoch_rows // LANES
        self.half = slabs * epoch_rows // 2
        self.message = self.half + LANES

    def first_tile(self, owner):
        return lax.div(owner * self.owned, LANES)


def fits(slabs, coefs, epoch_rows, coef_rows, columns, taps):
    if slabs & (slabs - 1) or slabs < 4 or coefs % 2 or epoch_rows % (2 * LANES) or coef_rows % LANES:
        return False
    if coef_rows % slabs or taps != LANES or columns != LANES or columns != GROUP * slabs * coefs // 2:
        return False
    owned = coef_rows // slabs
    rest = owned % LANES
    return owned >= 4 * LANES and rest >= 16 and LANES % rest == 0


def flipped(index, bits, count):
    result, weight = 0, 1
    while weight < count:
        bit = lax.rem(lax.div(index, weight), 2)
        result = result + weight * (1 - bit if bits & weight else bit)
        weight *= 2
    return result


def pieces(values):
    high = values.astype(jnp.bfloat16).astype(jnp.float32)
    left = values - high
    middle = left.astype(jnp.bfloat16).astype(jnp.float32)
    low = (left - middle).astype(jnp.bfloat16).astype(jnp.float32)
    return high + pltpu.roll(middle, 8, 1) + pltpu.roll(low, 16, 1)


def joined(values, at):
    lane = lax.broadcasted_iota(jnp.int32, values.shape, 1)
    taken = (lane % 8 == at) & (lane < 24)
    return jnp.sum(jnp.where(taken, values, 0.0), 1, keepdims=True)


def in_lanes(terms, rows):
    lane = lax.broadcasted_iota(jnp.int32, (rows, LANES), 1)
    result = jnp.zeros((rows, LANES), jnp.float32)
    for at, term in enumerate(terms):
        result = jnp.where(lane == at, term, result)
    return result


def product(left, right, contract, precision=None):
    return lax.dot_general(
        left, right, (contract, ((), ())), precision=precision, preferred_element_type=jnp.float32
    )


def fused(plan, design, observed_in, gap_in, counts, taps_in, kaula_in, precond_in, solution_out, residual_out,
          observed, gap, taps, kaula, precond,
          block, edges, packed, loose, shown, seen, early, sums, received, total, sent, folded_in, sent_terms, terms_in,
          whole, folded, filtered, gathered, resid, direc, scal, solut, first_values,
          own_sem, small_sem, edge_sem, block_send, block_recv, show_send, show_recv, early_send, early_recv,
          early_relay_send, early_relay_recv, pair_send, pair_recv, fold_send, fold_recv, term_send, term_recv,
          whole_send, whole_recv, gather_send, gather_recv, relay_send, relay_recv):
    slabs, chips, rows = plan.slabs, plan.chips, plan.epoch_rows
    half_slabs, half_chips, half_blocks = slabs // 2, chips // 2, plan.blocks // 2
    slab, coef = lax.axis_index("tm"), lax.axis_index("coef")
    across, core = lax.div(coef, 2), lax.rem(coef, 2)
    chip = slab * plan.across + across
    near_chip = lax.rem(chip, half_chips)
    this_half = lax.div(chip, half_chips)
    partner = {"tm": slab, "coef": 2 * across + 1 - core}

    def device(at):
        return {"tm": lax.div(at, plan.across), "coef": 2 * lax.rem(at, plan.across) + core}

    def other(step):
        return lax.rem(chip + step, chips)

    def near_other(step):
        return lax.rem(near_chip + step, half_chips)

    def remote(src, dst, send, recv, target):
        return pltpu.make_async_remote_copy(
            src_ref=src, dst_ref=dst, send_sem=send, recv_sem=recv, device_id=target, device_id_type=MESH
        )

    barrier = pltpu.get_barrier_semaphore()
    for step in range(1, chips):
        pl.semaphore_signal(barrier, inc=1, device_id=device(other(step)), device_id_type=MESH)
    pl.semaphore_signal(barrier, inc=1, device_id=partner, device_id_type=MESH)

    small = [
        pltpu.make_async_copy(src, dst, small_sem.at[at])
        for at, (src, dst) in enumerate(
            ((observed_in, observed), (gap_in, gap), (taps_in, taps), (kaula_in, kaula), (precond_in, precond))
        )
    ]
    for copy in small:
        copy.start()
    first = plan.first_tile(slab)
    offset = slab * plan.owned - first * LANES

    def tile_columns(tile, size):
        return pl.ds(pl.multiple_of(tile * LANES, LANES), size)

    own = pltpu.make_async_copy(
        design.at[:, tile_columns(first + 1, plan.mixed_at)], block.at[slab, :, pl.ds(0, plan.mixed_at)], own_sem
    )
    own.start()
    edge_copies = []
    for owner in range(slabs):
        begin = owner * plan.owned // LANES
        for at, tile in enumerate((begin, begin + plan.full + 1)):
            edge_copies.append(pltpu.make_async_copy(
                design.at[:, pl.ds(tile * LANES, LANES)], edges.at[owner, at], edge_sem.at[owner, at]
            ))
            edge_copies[-1].start()

    for copy in small[:3]:
        copy.wait()
    place = lax.broadcasted_iota(jnp.int32, (1, rows), 1)
    present = jnp.concatenate([gap[at:at + 1, :] for at in range(rows // LANES)], 1)
    weight_row = jnp.where((present == 1) & (place < counts[0]), 1.0, 0.0)
    turned = observed[...].T * weight_row
    shown[:, :GROUP, :] = turned.reshape(chips, GROUP, rows)
    shown[:, GROUP:, :] = jnp.broadcast_to(weight_row[None], (chips, GROUP, rows))
    seen[slab] = shown[2 * near_chip + core]

    def block_copy(bits, part):
        peer = flipped(slab, bits, slabs)
        tile = plan.first_tile(peer) + 1
        if part == 0:
            src, dst = design.at[:, tile_columns(tile, plan.cut)], block.at[slab, :, pl.ds(0, plan.cut)]
        elif part == 1:
            src = design.at[:, tile_columns(tile + plan.cut // LANES, plan.mixed_at - plan.cut)]
            dst = block.at[slab, :, pl.ds(plan.cut, plan.mixed_at - plan.cut)]
        elif part == 2:
            src, dst = packed.at[peer, pl.ds(0, rows)], block.at[slab, :, pl.ds(plan.mixed_at, LANES)]
        else:
            src, dst = packed.at[peer, pl.ds(rows, plan.packed_rows)], loose.at[slab]
        return remote(src, dst, block_send.at[part, peer], block_recv.at[part, slab], {"tm": peer, "coef": coef})

    def block_arrival(bits, part):
        peer = flipped(slab, bits, slabs)
        if part == 0:
            dst = block.at[peer, :, pl.ds(0, plan.cut)]
        elif part == 1:
            dst = block.at[peer, :, pl.ds(plan.cut, plan.mixed_at - plan.cut)]
        elif part == 2:
            dst = block.at[peer, :, pl.ds(plan.mixed_at, LANES)]
        else:
            dst = loose.at[peer]
        return remote(dst, dst, block_send.at[part, peer], block_recv.at[part, peer], {"tm": peer, "coef": coef})

    def show_copy(bits):
        peer = flipped(slab, bits, slabs)
        src = shown.at[2 * lax.rem(peer * plan.across + across, half_chips) + core]
        return remote(src, seen.at[slab], show_send.at[peer], show_recv.at[slab], {"tm": peer, "coef": coef})

    def show_arrival(bits):
        peer = flipped(slab, bits, slabs)
        return remote(seen.at[peer], seen.at[peer], show_send.at[peer], show_recv.at[peer], {"tm": peer, "coef": coef})

    pl.semaphore_wait(barrier, chips)
    for bits in range(1, slabs):
        show_copy(bits).start()
    for bits in range(1, half_slabs):
        block_copy(bits, 0).start()
        block_copy(bits, 1).start()
    for bits in range(half_slabs, slabs):
        block_copy(bits, 0).start()

    for copy in edge_copies:
        copy.wait()
    lane_row = lax.broadcasted_iota(jnp.int32, (1, LANES), 1)
    for owner in range(slabs):
        skip = owner * plan.owned % LANES
        ahead = edges[owner, 0].astype(jnp.float32)
        behind = edges[owner, 1].astype(jnp.float32)
        packed[owner, :rows] = jnp.where(lane_row >= skip, ahead, behind).astype(jnp.bfloat16)
        tight = jnp.zeros((plan.packed_rows, LANES), jnp.float32)
        for at in range(LANES // plan.rest):
            part = behind[at * plan.packed_rows:(at + 1) * plan.packed_rows]
            shift = (at * plan.rest - skip) % LANES
            part = pltpu.roll(part, shift, 1) if shift else part
            tight = jnp.where(lax.div(lane_row, plan.rest) == at, part, tight)
        packed[owner, rows:] = tight.astype(jnp.bfloat16)
    for bits in range(1, slabs):
        block_copy(bits, 2).start()
        block_copy(bits, 3).start()

    def unpack(at):
        tight = loose[at].astype(jnp.float32)
        for piece in range(LANES // plan.rest):
            part = pltpu.roll(tight, LANES - piece * plan.rest, 1) if piece else tight
            part = jnp.where(lane_row < plan.rest, part, 0.0).astype(jnp.bfloat16)
            block[at, piece * plan.packed_rows:(piece + 1) * plan.packed_rows, plan.mixed_at + LANES:] = part

    block[slab, :, plan.mixed_at:plan.mixed_at + LANES] = packed[slab, :rows]
    loose[slab] = packed[slab, rows:]
    unpack(slab)

    base = jnp.concatenate([taps[...], jnp.zeros((1, LANES), jnp.float32)], 1)
    shifted = pltpu.roll(jnp.broadcast_to(base, (LANES, 2 * LANES)), 0, 1, stride=1, stride_axis=0)
    lower, upper = shifted[:, :LANES], shifted[:, LANES:]
    blank = jnp.zeros((GROUP, LANES), jnp.float32)

    for bits in range(1, slabs):
        show_arrival(bits).wait_recv()

    def stack(ref, low):
        return jnp.concatenate(
            [ref[at, low:low + GROUP, j * LANES:(j + 1) * LANES] for at in range(slabs) for j in range(rows // LANES)], 0
        )

    weight = stack(seen, GROUP)

    def weighted(values):
        entering = weight * values
        before = jnp.concatenate([blank, entering[:-GROUP]], 0)
        inner = product(entering, lower, NN, lax.Precision.HIGHEST) + product(before, upper, NN, lax.Precision.HIGHEST)
        after = jnp.concatenate([inner[GROUP:], blank], 0)
        outer = product(inner, lower, NT, lax.Precision.HIGHEST) + product(after, upper, NT, lax.Precision.HIGHEST)
        return (weight * outer).astype(jnp.bfloat16)

    kept = weighted(stack(seen, 0)).astype(jnp.float32)
    for j in range(plan.blocks):
        early[core, near_chip, :, j * LANES:(j + 1) * LANES] = kept[j * GROUP:(j + 1) * GROUP].astype(jnp.bfloat16)
    for step in range(1, half_chips):
        to = near_other(step)
        here = early.at[core, near_chip]
        target = device(this_half * half_chips + to)
        remote(here, here, early_send.at[to], early_recv.at[near_chip], target).start()
    for bits in range(half_slabs, slabs):
        block_copy(bits, 1).start()

    small[3].wait()
    small[4].wait()

    def local_row(table):
        inside = [table[pl.ds(first + 1 + at, 1), :] for at in range(plan.full)]
        ahead, behind = table[pl.ds(first, 1), :], table[pl.ds(first + plan.full + 1, 1), :]
        moved = pltpu.roll(jnp.broadcast_to(behind, (GROUP, LANES)), lax.rem(LANES - offset, LANES), 1)[:1]
        mixed = jnp.where(lane_row >= offset, ahead, behind)
        return jnp.concatenate(inside + [mixed, jnp.where(lane_row < plan.rest, moved, 0.0)], 1)

    ridge_row, scale_row = local_row(kaula), local_row(precond)

    def early_arrival(step):
        at = near_other(step)
        here = early.at[core, at]
        return remote(here, here, early_send.at[at], early_recv.at[at], device(this_half * half_chips + at))

    for step in range(1, half_chips):
        early_arrival(step).wait_recv()
    mine, theirs = early.at[core], early.at[1 - core]
    remote(mine, mine, early_relay_send, early_relay_recv, partner).start()
    remote(theirs, theirs, early_relay_send, early_relay_recv, partner).wait_recv()
    for at in range(slabs):
        span = slice(at * rows, (at + 1) * rows)
        both = jnp.stack([early[0, :, :, span].astype(jnp.float32), early[1, :, :, span].astype(jnp.float32)], 1)
        filtered[:, span] = both.reshape(plan.columns, rows).astype(jnp.bfloat16)

    def series(at):
        return filtered[:, pl.ds(pl.multiple_of(at * rows, rows), rows)]

    def over(terms):
        return jnp.sum(terms, 1, keepdims=True)

    own.wait()
    spans = (slice(0, plan.cut), slice(plan.cut, plan.width))
    for part, span in enumerate(spans):
        resid[:, span] = product(series(slab), block[slab, :, span], NN)
        for bits in range(1, slabs):
            peer = flipped(slab, bits, slabs)
            for piece in ((0,), (1, 2, 3))[part]:
                block_arrival(bits, piece).wait_recv()
            if part:
                unpack(peer)
            resid[:, span] += product(series(peer), block[peer, :, span], NN)
        direc[:, span] = scale_row[:, span] * resid[:, span]
        if part == 0:
            low = direc[:, span].astype(jnp.bfloat16)

            def body(at, carry):
                sums[0, at] = product(low, block[at, :, :plan.cut], NT)
                return carry

            lax.fori_loop(0, slabs, body, 0)

    def pair_copy(turn, j):
        src = sums.at[turn, (1 - core) * half_slabs + j]
        return remote(src, received.at[turn, j], pair_send.at[turn, j], pair_recv.at[turn, j], partner)

    def fold_copy(turn, j, step):
        to = other(step)
        src, dst = sent.at[turn, j, to], folded_in.at[turn, j, chip]
        return remote(src, dst, fold_send.at[turn, j, to], fold_recv.at[turn, j, chip], device(to))

    def fold_arrival(turn, j, at):
        here = folded_in.at[turn, j, at]
        return remote(here, here, fold_send.at[turn, j, at], fold_recv.at[turn, j, at], device(at))

    def term_copy(turn, step):
        to = other(step)
        src, dst = sent_terms.at[turn, to], terms_in.at[turn, chip]
        return remote(src, dst, term_send.at[turn, to], term_recv.at[turn, chip], device(to))

    def term_arrival(turn, at):
        here = terms_in.at[turn, at]
        return remote(here, here, term_send.at[turn, at], term_recv.at[turn, at], device(at))

    def each_chip(action):
        def body(step, carry):
            action(step)
            return carry

        lax.fori_loop(1, chips, body, 0)

    def summed(turn, low, terms, span):
        scalars = in_lanes(terms, plan.columns)
        sent_terms[turn] = pieces(scalars).reshape(chips, GROUP, LANES).astype(jnp.bfloat16)
        terms_in[turn, chip] = sent_terms[turn, chip]
        each_chip(lambda step: term_copy(turn, step).start())

        def partial(at):
            value = product(low, block[at, :, span], NT)
            return value + sums[turn, at] if turn == 0 else value

        def give(j, carry):
            at = (1 - core) * half_slabs + j
            sums[turn, at] = partial(at)
            pair_copy(turn, j).start()
            return carry

        lax.fori_loop(0, half_slabs, give, 0)

        def keep(j, carry):
            value = partial(core * half_slabs + j)
            pair_copy(turn, j).wait_recv()
            value = (value + received[turn, j]).reshape(chips, GROUP, rows)
            total[j] = value
            sent[turn, j] = value.astype(jnp.bfloat16)
            each_chip(lambda step: fold_copy(turn, j, step).start())
            return carry

        lax.fori_loop(0, half_slabs, keep, 0)

        def take(step, carry):
            at = other(step)
            term_arrival(turn, at).wait_recv()
            return carry + terms_in[turn, at].astype(jnp.float32)

        whole[turn, core, :, plan.half:] = lax.fori_loop(1, chips, take, terms_in[turn, chip].astype(jnp.float32))
        for j in range(half_slabs):
            def arrive(step, carry):
                at = other(step)
                fold_arrival(turn, j, at).wait_recv()
                return carry + folded_in[turn, j, at].astype(jnp.float32)

            whole[turn, core, :, j * rows:(j + 1) * rows] = lax.fori_loop(1, chips, arrive, total[j, chip])
        mine, theirs = whole.at[turn, core], whole.at[turn, 1 - core]
        remote(mine, mine, whole_send.at[turn], whole_recv.at[turn], partner).start()
        remote(theirs, theirs, whole_send.at[turn], whole_recv.at[turn], partner).wait_recv()
        values = jnp.concatenate(
            [whole[turn, half, :, j * LANES:(j + 1) * LANES] for half in range(2) for j in range(half_blocks)], 0
        )
        scalars = whole[turn, 0, :, plan.half:] + whole[turn, 1, :, plan.half:]
        return values, [joined(scalars, at) for at in range(len(terms))]

    def gather_copy(phase, step):
        to = other(step)
        here = gathered.at[phase, core, chip]
        return remote(here, here, gather_send.at[phase, to], gather_recv.at[phase, chip], device(to))

    def gather_arrival(phase, at):
        here = gathered.at[phase, core, at]
        return remote(here, here, gather_send.at[phase, at], gather_recv.at[phase, at], device(at))

    def relay_copy(phase, at):
        here = gathered.at[phase, core, at]
        return remote(here, here, relay_send.at[phase, at], relay_recv.at[phase, at], partner)

    def relay_arrival(phase, at):
        here = gathered.at[phase, 1 - core, at]
        return remote(here, here, relay_send.at[phase, at], relay_recv.at[phase, at], partner)

    def shared(phase, values, terms):
        wide = values.astype(jnp.float32)
        for half in range(2):
            for j in range(half_blocks):
                low = (half * half_blocks + j) * GROUP
                folded[half, :, j * LANES:(j + 1) * LANES] = wide[low:low + GROUP]
            folded[half, :, plan.half:] = pieces(in_lanes(terms, GROUP))
        gathered[phase, core, chip] = folded[core].astype(jnp.bfloat16)
        each_chip(lambda step: gather_copy(phase, step).start())
        relay_copy(phase, chip).start()

        def pass_on(step):
            at = other(step)
            gather_arrival(phase, at).wait_recv()
            relay_copy(phase, at).start()

        each_chip(pass_on)
        relay_arrival(phase, chip).wait_recv()
        each_chip(lambda step: relay_arrival(phase, other(step)).wait_recv())
        for half in range(2):
            for j in range(half_slabs):
                part = gathered[phase, half, :, :, j * rows:(j + 1) * rows].astype(jnp.float32)
                low = half * plan.half + j * rows
                filtered[:, low:low + rows] = part.reshape(plan.columns, rows).astype(jnp.bfloat16)
        scalars = gathered[phase, 0, :, :, plan.half:].astype(jnp.float32).reshape(plan.columns, LANES)
        return [joined(scalars, at) for at in range(len(terms))]

    def inner(left, right):
        together = (left * right).reshape(plan.blocks, GROUP, LANES)
        return over(jnp.sum(together, 0))

    chunks = [slice(low, min(low + 2 * LANES, plan.width)) for low in range(0, plan.width, 2 * LANES)]

    def transposed(span):
        part = block[:, :, span]
        return product(filtered[...], part.reshape(slabs * rows, part.shape[2]), NN)

    ridged = ridge_row * direc[...]
    terms = [over(resid[...] * direc[...]), over(ridged * direc[...])]
    values, (norm, ridge) = summed(0, direc[:, spans[1]].astype(jnp.bfloat16), terms, spans[1])
    first_values[...] = values
    kept = weighted(values)
    step_len = norm / (ridge + inner(values, kept.astype(jnp.float32)))
    (step_col,) = shared(0, kept, [step_len])
    terms = [0.0, 0.0, 0.0]
    for span in chunks:
        along, ridge_part = direc[:, span], ridge_row[:, span]
        left = resid[:, span] - step_col * (transposed(span) + ridge_part * along)
        ahead = scale_row[:, span] * left
        resid[:, span] = left
        solut[:, span] = step_col * along
        scal[:, span] = ahead
        ridged = ridge_part * ahead
        added = (over(left * ahead), over(ridged * ahead), over(ridged * along))
        terms = [term + more for term, more in zip(terms, added)]
    fresh, (norm_next, own_ridge, cross) = summed(1, scal[...].astype(jnp.bfloat16), terms, slice(0, plan.width))
    ratio = norm_next / norm
    ridge = own_ridge + ratio * (2.0 * cross + ratio * ridge)
    values = fresh + jnp.concatenate([ratio] * plan.blocks, 0) * first_values[...]
    kept = weighted(values)
    step_len = norm_next / (ridge + inner(values, kept.astype(jnp.float32)))
    step_col, ratio_col = shared(1, kept, [step_len, ratio])

    def put(out, tile, value):
        out[pl.ds(pl.multiple_of((tile + 2) * LANES - offset, plan.rest), LANES), :] = value

    held = {}
    for span in chunks:
        along = scal[:, span] + ratio_col * direc[:, span]
        ahead = solut[:, span] + step_col * along
        left = resid[:, span] - step_col * (transposed(span) + ridge_row[:, span] * along)
        for low in range(0, span.stop - span.start, LANES):
            held[(span.start + low) // LANES] = (ahead[:, low:low + LANES].T, left[:, low:low + LANES].T)
        for tile in [tile for tile in held if tile < plan.full]:
            new_ahead, new_left = held.pop(tile)
            put(solution_out, tile, new_ahead)
            put(residual_out, tile, new_left)
    mixed = held[plan.full]
    last = held[plan.full + 1]
    for out, first_value, second in ((solution_out, mixed[0], last[0]), (residual_out, mixed[1], last[1])):
        low = pl.multiple_of(LANES - offset, plan.rest)
        out[pl.ds(low, LANES), :] = first_value
        low = pl.multiple_of((plan.full + 2) * LANES - offset, plan.rest)
        out[pl.ds(low, LANES), :] = first_value
        low = (plan.full + 2) * LANES
        out[low:low + plan.rest, :] = second[:plan.rest]

    for bits in range(1, slabs):
        show_copy(bits).wait_send()
        for part in range(4):
            block_copy(bits, part).wait_send()
    for step in range(1, half_chips):
        to = near_other(step)
        here = early.at[core, near_chip]
        target = device(this_half * half_chips + to)
        remote(here, here, early_send.at[to], early_recv.at[near_chip], target).wait_send()
    mine = early.at[core]
    remote(mine, mine, early_relay_send, early_relay_recv, partner).wait_send()
    for turn in range(2):
        for j in range(half_slabs):
            pair_copy(turn, j).wait_send()
            each_chip(lambda step: fold_copy(turn, j, step).wait_send())
        each_chip(lambda step: term_copy(turn, step).wait_send())
        mine = whole.at[turn, core]
        remote(mine, mine, whole_send.at[turn], whole_recv.at[turn], partner).wait_send()
        each_chip(lambda step: gather_copy(turn, step).wait_send())
        relay_copy(turn, chip).wait_send()
        each_chip(lambda step: relay_copy(turn, other(step)).wait_send())


def fused_shards(design, observed, slab_counts, gap_mask, filter_taps, kaula_diag, precond):
    epoch_rows, coef_rows = design.shape
    columns = observed.shape[1]
    slabs, coefs = lax.axis_size("tm"), lax.axis_size("coef")
    plan = Plan(slabs, coefs, epoch_rows, coef_rows, columns)
    wide, chips, message = plan.width, plan.chips, plan.message
    half_slabs, half_chips = slabs // 2, chips // 2
    f32, bf16 = jnp.float32, jnp.bfloat16
    vmem = pl.BlockSpec(memory_space=pltpu.VMEM)
    hbm = pl.BlockSpec(memory_space=pltpu.HBM)
    sem = pltpu.SemaphoreType.DMA
    shape = jax.ShapeDtypeStruct((wide + LANES, columns), f32)
    tiles = (plan.tiles, LANES)
    outs = pl.pallas_call(
        functools.partial(fused, plan),
        out_shape=(shape, shape),
        in_specs=[hbm, hbm, hbm, pl.BlockSpec(memory_space=pltpu.SMEM), hbm, hbm, hbm],
        out_specs=(vmem, vmem),
        scratch_shapes=[
            pltpu.VMEM((epoch_rows, columns), f32),
            pltpu.VMEM((epoch_rows // LANES, LANES), jnp.int32),
            pltpu.VMEM((1, LANES), f32),
            pltpu.VMEM(tiles, f32),
            pltpu.VMEM(tiles, f32),
            pltpu.VMEM((slabs, epoch_rows, wide), bf16),
            pltpu.VMEM((slabs, 2, epoch_rows, LANES), bf16),
            pltpu.VMEM((slabs, epoch_rows + plan.packed_rows, LANES), bf16),
            pltpu.VMEM((slabs, plan.packed_rows, LANES), bf16),
            pltpu.VMEM((chips, 2 * GROUP, epoch_rows), f32),
            pltpu.VMEM((slabs, 2 * GROUP, epoch_rows), f32),
            pltpu.VMEM((2, half_chips, GROUP, slabs * epoch_rows), bf16),
            pltpu.VMEM((2, slabs, columns, epoch_rows), f32),
            pltpu.VMEM((2, half_slabs, columns, epoch_rows), f32),
            pltpu.VMEM((half_slabs, chips, GROUP, epoch_rows), f32),
            pltpu.VMEM((2, half_slabs, chips, GROUP, epoch_rows), bf16),
            pltpu.VMEM((2, half_slabs, chips, GROUP, epoch_rows), bf16),
            pltpu.VMEM((2, chips, GROUP, LANES), bf16),
            pltpu.VMEM((2, chips, GROUP, LANES), bf16),
            pltpu.VMEM((2, 2, GROUP, message), f32),
            pltpu.VMEM((2, GROUP, message), f32),
            pltpu.VMEM((columns, slabs * epoch_rows), bf16),
            pltpu.VMEM((2, 2, chips, GROUP, message), bf16),
            pltpu.VMEM((columns, wide), f32),
            pltpu.VMEM((columns, wide), f32),
            pltpu.VMEM((columns, wide), f32),
            pltpu.VMEM((columns, wide), f32),
            pltpu.VMEM((plan.blocks * GROUP, LANES), f32),
            sem(()), sem((5,)), sem((slabs, 2)), sem((4, slabs)), sem((4, slabs)), sem((slabs,)), sem((slabs,)),
            sem((half_chips,)), sem((half_chips,)), sem(()), sem(()),
            sem((2, half_slabs)), sem((2, half_slabs)), sem((2, half_slabs, chips)), sem((2, half_slabs, chips)),
            sem((2, chips)), sem((2, chips)), sem((2,)), sem((2,)),
            sem((2, chips)), sem((2, chips)), sem((2, chips)), sem((2, chips)),
        ],
        compiler_params=pltpu.CompilerParams(
            collective_id=0, has_side_effects=True, vmem_limit_bytes=48 * 1024 * 1024
        ),
    )(
        design, observed, gap_mask.reshape(-1, LANES), slab_counts, filter_taps[None],
        kaula_diag.reshape(tiles), precond.reshape(tiles),
    )
    return tuple(out[LANES:LANES + plan.owned] for out in outs)


def shards(*arrays):
    design, observed, filter_taps = arrays[0], arrays[1], arrays[4]
    sizes = (lax.axis_size("tm"), lax.axis_size("coef"), *design.shape, observed.shape[1], filter_taps.shape[0])
    return fused_shards(*arrays) if fits(*sizes) else general_shards(*arrays)


def solution(mesh):
    placed = (P("tm", "coef"), P("tm", None), P("tm"), P("tm"), P(), P("coef"), P("coef"))
    return jax.shard_map(
        shards,
        mesh=mesh,
        in_specs=placed,
        out_specs=(P(("coef", "tm"), None), P(("coef", "tm"), None)),
        check_vma=False,
    )
```

```python
import functools

import jax
import jax.numpy as jnp
from jax import lax
from jax.experimental import pallas as pl
from jax.experimental.pallas import tpu as pltpu
from jax.sharding import PartitionSpec as P

ITERS = 2
HIGHEST = lax.Precision.HIGHEST


def toeplitz(pattern, band_len):
    tiled = jnp.tile(pattern, band_len)[: band_len * (2 * band_len - 1)]
    return tiled.reshape(band_len, 2 * band_len - 1)[:, :band_len]


def block_pair(filter_taps):
    band_len = filter_taps.shape[0]
    spacer = jnp.zeros((band_len,), jnp.float32)
    reversed_taps = filter_taps[:0:-1]
    lower = jnp.concatenate([filter_taps[:1], spacer, reversed_taps])
    upper = jnp.concatenate([jnp.zeros((1,), jnp.float32), reversed_taps, spacer])
    return (toeplitz(lower, band_len), toeplitz(upper, band_len))


def forward(values, lower_block, upper_block):
    band_len = lower_block.shape[0]
    blocks = values.reshape(-1, band_len, values.shape[1])
    previous = jnp.concatenate([jnp.zeros_like(blocks[:1]), blocks[:-1]], 0)
    result = jnp.einsum("ij,bjr->bir", lower_block, blocks, precision=HIGHEST)
    result = result + jnp.einsum("ij,bjr->bir", upper_block, previous, precision=HIGHEST)
    return result.reshape(values.shape)


def backward(values, lower_block, upper_block):
    band_len = lower_block.shape[0]
    blocks = values.reshape(-1, band_len, values.shape[1])
    following = jnp.concatenate([blocks[1:], jnp.zeros_like(blocks[:1])], 0)
    result = jnp.einsum("ji,bjr->bir", lower_block, blocks, precision=HIGHEST)
    result = result + jnp.einsum("ji,bjr->bir", upper_block, following, precision=HIGHEST)
    return result.reshape(values.shape)


def general_shards(design, observed, slab_counts, gap_mask, filter_taps, kaula_diag, precond):
    epoch_rows, coef_rows = design.shape
    columns = observed.shape[1]
    slabs = lax.axis_size("tm")
    epochs = slabs * epoch_rows
    owned_rows = coef_rows // slabs
    owner_index = lax.axis_index("tm")
    lower_block, upper_block = block_pair(filter_taps)
    position = jnp.arange(epoch_rows, dtype=jnp.int32)
    local_weight = ((gap_mask == 1) & (position < slab_counts[0])).astype(jnp.float32)
    packed = jnp.concatenate([observed, local_weight.reshape(-1, columns)], 0)
    gathered = lax.all_gather(packed, "tm", axis=0, tiled=False)
    all_observed = gathered[:, :epoch_rows].reshape(epochs, columns)
    weight = gathered[:, epoch_rows:].reshape(epochs, 1)
    block = lax.all_to_all(design, "tm", split_axis=1, concat_axis=0, tiled=True)

    def weighted(values):
        inner = forward(weight * values, lower_block, upper_block)
        return (weight * backward(inner, lower_block, upper_block)).astype(jnp.bfloat16)

    def transposed(filtered):
        return lax.dot_general(
            block, filtered, (((0,), (0,)), ((), ())), preferred_element_type=jnp.float32
        )

    def summed(scaled, terms):
        partial = jnp.dot(block, scaled.astype(jnp.bfloat16), preferred_element_type=jnp.float32)
        rows = [jnp.sum(term, 0)[None] for term in terms]
        rows.append(jnp.zeros((8 - len(rows), columns), jnp.float32))
        total = lax.psum(jnp.concatenate([partial] + rows, 0), ("tm", "coef"))
        return total[:epochs], [total[epochs + at] for at in range(len(terms))]

    start = owner_index * owned_rows
    kaula_col = lax.dynamic_slice_in_dim(kaula_diag, start, owned_rows, 0)[:, None]
    precond_col = lax.dynamic_slice_in_dim(precond, start, owned_rows, 0)[:, None]
    residual = transposed(weighted(all_observed))
    solution = jnp.zeros_like(residual)
    for iteration in range(ITERS):
        scaled = precond_col * residual
        terms = [residual * scaled, kaula_col * scaled * scaled]
        if iteration == 0:
            slab_values, (norm_now, ridge) = summed(scaled, terms)
            direction = scaled
        else:
            terms.append(kaula_col * scaled * direction)
            fresh, (norm_next, own_ridge, cross) = summed(scaled, terms)
            ratio = norm_next / norm_now
            slab_values = fresh + ratio * slab_values
            ridge = own_ridge + ratio * (2.0 * cross + ratio * ridge)
            direction = scaled + ratio * direction
            norm_now = norm_next
        filtered = weighted(slab_values)
        curvature = ridge + jnp.sum(slab_values * filtered.astype(jnp.float32), 0)
        step_len = norm_now / curvature
        image = transposed(filtered) + kaula_col * direction
        solution = solution + step_len * direction
        residual = residual - step_len * image
    return (solution, residual)


LANES = 128
GROUP = 8
MESH = pl.DeviceIdType.MESH
NN = ((1,), (0,))
NT = ((1,), (1,))


class Plan:
    def __init__(self, slabs, coefs, epoch_rows, coef_rows, columns):
        self.slabs, self.coefs, self.epoch_rows, self.columns = slabs, coefs, epoch_rows, columns
        self.tiles = coef_rows // LANES
        self.owned = coef_rows // slabs
        self.full = self.owned // LANES - 1
        self.rest = self.owned % LANES
        self.packed_rows = epoch_rows * self.rest // LANES
        self.mixed_at = self.full * LANES
        self.width = (self.full + 2) * LANES
        self.cut = self.full * 3 // 4 * LANES
        self.across = coefs // 2
        self.chips = slabs * self.across
        self.blocks = slabs * epoch_rows // LANES
        self.half = slabs * epoch_rows // 2
        self.message = self.half + LANES

    def first_tile(self, owner):
        return lax.div(owner * self.owned, LANES)


def fits(slabs, coefs, epoch_rows, coef_rows, columns, taps):
    if slabs & (slabs - 1) or slabs < 4 or coefs % 2 or epoch_rows % (2 * LANES) or coef_rows % LANES:
        return False
    if coef_rows % slabs or taps != LANES or columns != LANES or columns != GROUP * slabs * coefs // 2:
        return False
    owned = coef_rows // slabs
    rest = owned % LANES
    return owned >= 4 * LANES and rest >= 16 and LANES % rest == 0


def flipped(index, bits, count):
    result, weight = 0, 1
    while weight < count:
        bit = lax.rem(lax.div(index, weight), 2)
        result = result + weight * (1 - bit if bits & weight else bit)
        weight *= 2
    return result


def pieces(values):
    high = values.astype(jnp.bfloat16).astype(jnp.float32)
    left = values - high
    middle = left.astype(jnp.bfloat16).astype(jnp.float32)
    low = (left - middle).astype(jnp.bfloat16).astype(jnp.float32)
    return high + pltpu.roll(middle, 8, 1) + pltpu.roll(low, 16, 1)


def joined(values, at):
    lane = lax.broadcasted_iota(jnp.int32, values.shape, 1)
    taken = (lane % 8 == at) & (lane < 24)
    return jnp.sum(jnp.where(taken, values, 0.0), 1, keepdims=True)


def in_lanes(terms, rows):
    lane = lax.broadcasted_iota(jnp.int32, (rows, LANES), 1)
    result = jnp.zeros((rows, LANES), jnp.float32)
    for at, term in enumerate(terms):
        result = jnp.where(lane == at, term, result)
    return result


def product(left, right, contract, precision=None):
    return lax.dot_general(
        left, right, (contract, ((), ())), precision=precision, preferred_element_type=jnp.float32
    )


def fused(plan, design, observed_in, gap_in, counts, taps_in, kaula_in, precond_in, solution_out, residual_out,
          observed, gap, taps, kaula, precond,
          block, turned_block, edges, packed, loose, shown, seen, early, sums, received, total, sent, folded_in, sent_terms, terms_in,
          whole, folded, filtered, gathered, resid, direc, scal, solut, first_values,
          own_sem, small_sem, edge_sem, block_send, block_recv, loose_recv, show_send, show_recv, early_send, early_recv,
          early_relay_send, early_relay_recv, pair_send, pair_recv, fold_send, fold_recv, term_send, term_recv,
          whole_send, whole_recv, gather_send, gather_recv, relay_send, relay_recv):
    slabs, chips, rows = plan.slabs, plan.chips, plan.epoch_rows
    half_slabs, half_chips, half_blocks = slabs // 2, chips // 2, plan.blocks // 2
    slab, coef = lax.axis_index("tm"), lax.axis_index("coef")
    across, core = lax.div(coef, 2), lax.rem(coef, 2)
    chip = slab * plan.across + across
    near_chip = lax.rem(chip, half_chips)
    this_half = lax.div(chip, half_chips)
    partner = {"tm": slab, "coef": 2 * across + 1 - core}

    def device(at):
        return {"tm": lax.div(at, plan.across), "coef": 2 * lax.rem(at, plan.across) + core}

    def other(step):
        return lax.rem(chip + step, chips)

    def near_other(step):
        return lax.rem(near_chip + step, half_chips)

    def remote(src, dst, send, recv, target):
        return pltpu.make_async_remote_copy(
            src_ref=src, dst_ref=dst, send_sem=send, recv_sem=recv, device_id=target, device_id_type=MESH
        )

    barrier = pltpu.get_barrier_semaphore()
    for step in range(1, chips):
        pl.semaphore_signal(barrier, inc=1, device_id=device(other(step)), device_id_type=MESH)
    pl.semaphore_signal(barrier, inc=1, device_id=partner, device_id_type=MESH)

    small = [
        pltpu.make_async_copy(src, dst, small_sem.at[at])
        for at, (src, dst) in enumerate(
            ((observed_in, observed), (gap_in, gap), (taps_in, taps), (kaula_in, kaula), (precond_in, precond))
        )
    ]
    for copy in small:
        copy.start()
    first = plan.first_tile(slab)
    offset = slab * plan.owned - first * LANES

    def tile_columns(tile, size):
        return pl.ds(pl.multiple_of(tile * LANES, LANES), size)

    own = pltpu.make_async_copy(
        design.at[:, tile_columns(first + 1, plan.mixed_at)], block.at[slab, :, pl.ds(0, plan.mixed_at)], own_sem
    )
    own.start()
    for owner in range(slabs):
        begin = owner * plan.owned // LANES
        for at, tile in enumerate((begin, begin + plan.full + 1)):
            pltpu.make_async_copy(
                design.at[:, pl.ds(tile * LANES, LANES)], edges.at[owner, at], edge_sem
            ).start()

    for copy in small[:3]:
        copy.wait()
    place = lax.broadcasted_iota(jnp.int32, (1, rows), 1)
    present = jnp.concatenate([gap[at:at + 1, :] for at in range(rows // LANES)], 1)
    weight_row = jnp.where((present == 1) & (place < counts[0]), 1.0, 0.0)
    turned = observed[...].T * weight_row
    shown[:, :GROUP, :] = turned.reshape(chips, GROUP, rows)
    shown[:, GROUP:, :] = jnp.broadcast_to(weight_row[None], (chips, GROUP, rows))
    seen[slab] = shown[2 * near_chip + core]

    def block_copy(bits, part):
        peer = flipped(slab, bits, slabs)
        tile = plan.first_tile(peer) + 1
        if part == 0:
            src, dst = design.at[:, tile_columns(tile, plan.cut)], block.at[slab, :, pl.ds(0, plan.cut)]
        elif part == 1:
            src = design.at[:, tile_columns(tile + plan.cut // LANES, plan.mixed_at - plan.cut)]
            dst = block.at[slab, :, pl.ds(plan.cut, plan.mixed_at - plan.cut)]
        elif part == 2:
            src, dst = packed.at[peer, pl.ds(0, rows)], block.at[slab, :, pl.ds(plan.mixed_at, LANES)]
        else:
            src, dst = packed.at[peer, pl.ds(rows, plan.packed_rows)], loose.at[slab]
        return remote(src, dst, block_send.at[part], loose_recv if part == 3 else block_recv.at[min(part, 1), slab], {"tm": peer, "coef": coef})

    def block_arrival(bits, part):
        peer = flipped(slab, bits, slabs)
        low, size = ((0, plan.cut), (plan.cut, plan.mixed_at + LANES - plan.cut))[part]
        dst = block.at[peer, :, pl.ds(low, size)]
        return remote(dst, dst, block_send.at[part], block_recv.at[part, peer], {"tm": peer, "coef": coef})

    def all_of(ref, send, recv):
        return remote(ref, ref, send, recv, partner)

    def show_copy(bits):
        peer = flipped(slab, bits, slabs)
        src = shown.at[2 * lax.rem(peer * plan.across + across, half_chips) + core]
        return remote(src, seen.at[slab], show_send, show_recv, {"tm": peer, "coef": coef})

    others = pl.ds(0, slabs - 1)
    pl.semaphore_wait(barrier, chips)
    for bits in range(1, slabs):
        show_copy(bits).start()
    for bits in range(1, half_slabs):
        block_copy(bits, 0).start()
        block_copy(bits, 1).start()
    for bits in range(half_slabs, slabs):
        block_copy(bits, 0).start()

    pltpu.make_async_copy(edges, edges, edge_sem).wait()
    lane_row = lax.broadcasted_iota(jnp.int32, (1, LANES), 1)
    for owner in range(slabs):
        skip = owner * plan.owned % LANES
        ahead = edges[owner, 0].astype(jnp.float32)
        behind = edges[owner, 1].astype(jnp.float32)
        packed[owner, :rows] = jnp.where(lane_row >= skip, ahead, behind).astype(jnp.bfloat16)
        tight = jnp.zeros((plan.packed_rows, LANES), jnp.float32)
        for at in range(LANES // plan.rest):
            part = behind[at * plan.packed_rows:(at + 1) * plan.packed_rows]
            shift = (at * plan.rest - skip) % LANES
            part = pltpu.roll(part, shift, 1) if shift else part
            tight = jnp.where(lax.div(lane_row, plan.rest) == at, part, tight)
        packed[owner, rows:] = tight.astype(jnp.bfloat16)
    for bits in range(1, slabs):
        block_copy(bits, 2).start()
        block_copy(bits, 3).start()

    def unpack(at, tight):
        tight = tight.astype(jnp.float32)
        for piece in range(LANES // plan.rest):
            part = pltpu.roll(tight, LANES - piece * plan.rest, 1) if piece else tight
            part = jnp.where(lane_row < plan.rest, part, 0.0).astype(jnp.bfloat16)
            block[at, piece * plan.packed_rows:(piece + 1) * plan.packed_rows, plan.mixed_at + LANES:] = part

    block[slab, :, plan.mixed_at:plan.mixed_at + LANES] = packed[slab, :rows]
    unpack(slab, packed[slab, rows:])

    base = jnp.concatenate([taps[...], jnp.zeros((1, LANES), jnp.float32)], 1)
    shifted = pltpu.roll(jnp.broadcast_to(base, (LANES, 2 * LANES)), 0, 1, stride=1, stride_axis=0)
    lower, upper = shifted[:, :LANES], shifted[:, LANES:]
    blank = jnp.zeros((GROUP, LANES), jnp.float32)

    all_of(seen.at[others], show_send, show_recv).wait_recv()

    def stack(ref, low):
        return jnp.concatenate(
            [ref[at, low:low + GROUP, j * LANES:(j + 1) * LANES] for at in range(slabs) for j in range(rows // LANES)], 0
        )

    weight = stack(seen, GROUP)

    def weighted(values):
        entering = weight * values
        before = jnp.concatenate([blank, entering[:-GROUP]], 0)
        inner = product(entering, lower, NN, lax.Precision.HIGHEST) + product(before, upper, NN, lax.Precision.HIGHEST)
        after = jnp.concatenate([inner[GROUP:], blank], 0)
        outer = product(inner, lower, NT, lax.Precision.HIGHEST) + product(after, upper, NT, lax.Precision.HIGHEST)
        return (weight * outer).astype(jnp.bfloat16)

    kept = weighted(stack(seen, 0)).astype(jnp.float32)
    for j in range(plan.blocks):
        early[core, near_chip, :, j * LANES:(j + 1) * LANES] = kept[j * GROUP:(j + 1) * GROUP].astype(jnp.bfloat16)
    for step in range(1, half_chips):
        to = near_other(step)
        here = early.at[core, near_chip]
        target = device(this_half * half_chips + to)
        remote(here, here, early_send, early_recv, target).start()
    for bits in range(half_slabs, slabs):
        block_copy(bits, 1).start()

    small[3].wait()
    small[4].wait()

    def local_row(table):
        inside = [table[pl.ds(first + 1 + at, 1), :] for at in range(plan.full)]
        ahead, behind = table[pl.ds(first, 1), :], table[pl.ds(first + plan.full + 1, 1), :]
        moved = pltpu.roll(jnp.broadcast_to(behind, (GROUP, LANES)), lax.rem(LANES - offset, LANES), 1)[:1]
        mixed = jnp.where(lane_row >= offset, ahead, behind)
        return jnp.concatenate(inside + [mixed, jnp.where(lane_row < plan.rest, moved, 0.0)], 1)

    ridge_row, scale_row = local_row(kaula), local_row(precond)

    near_others = pl.ds(0, half_chips - 1)
    all_of(early.at[core, near_others], early_send, early_recv).wait_recv()
    mine, theirs = early.at[core], early.at[1 - core]
    remote(mine, mine, early_relay_send, early_relay_recv, partner).start()
    remote(theirs, theirs, early_relay_send, early_relay_recv, partner).wait_recv()
    for at in range(slabs):
        span = slice(at * rows, (at + 1) * rows)
        both = jnp.stack([early[0, :, :, span].astype(jnp.float32), early[1, :, :, span].astype(jnp.float32)], 1)
        filtered[:, span] = both.reshape(plan.columns, rows).astype(jnp.bfloat16)

    def series(at):
        return filtered[:, pl.ds(pl.multiple_of(at * rows, rows), rows)]

    def over(terms):
        return jnp.sum(terms, 1, keepdims=True)

    own.wait()
    spans = (slice(0, plan.cut), slice(plan.cut, plan.width))

    def turn_over(at, span):
        turned_block[at, span] = block[at, :, span].T

    for part, span in enumerate(spans):
        if part:
            all_of(loose.at[others], block_send.at[3], loose_recv).wait_recv()
        turn_over(slab, span)
        resid[:, span] = product(series(slab), block[slab, :, span], NN)
        for bits in range(1, slabs):
            peer = flipped(slab, bits, slabs)
            block_arrival(bits, part).wait_recv()
            if part:
                unpack(peer, loose[peer])
            turn_over(peer, span)
            resid[:, span] += product(series(peer), block[peer, :, span], NN)
        direc[:, span] = scale_row[:, span] * resid[:, span]
        if part == 0:
            low = direc[:, span].astype(jnp.bfloat16)

            def body(at, carry):
                sums[0, at] = product(low, turned_block[at, :plan.cut], NN)
                return carry

            lax.fori_loop(0, slabs, body, 0)

    def pair_copy(turn, j):
        src = sums.at[turn, (1 - core) * half_slabs + j]
        return remote(src, received.at[turn, j], pair_send.at[turn], pair_recv.at[turn, j], partner)

    def fold_copy(turn, j, step):
        to = other(step)
        src, dst = sent.at[turn, j, to], folded_in.at[turn, j, chip]
        return remote(src, dst, fold_send.at[turn], fold_recv.at[turn, j], device(to))

    other_chips = pl.ds(0, chips - 1)

    def term_copy(turn, step):
        to = other(step)
        src, dst = sent_terms.at[turn, to], terms_in.at[turn, chip]
        return remote(src, dst, term_send.at[turn], term_recv.at[turn], device(to))

    def each_chip(action):
        def body(step, carry):
            action(step)
            return carry

        lax.fori_loop(1, chips, body, 0)

    def summed(turn, low, terms, span):
        scalars = in_lanes(terms, plan.columns)
        sent_terms[turn] = pieces(scalars).reshape(chips, GROUP, LANES).astype(jnp.bfloat16)
        terms_in[turn, chip] = sent_terms[turn, chip]
        each_chip(lambda step: term_copy(turn, step).start())

        def partial(at):
            value = product(low, turned_block[at, span], NN)
            return value + sums[turn, at] if turn == 0 else value

        def give(j, carry):
            at = (1 - core) * half_slabs + j
            sums[turn, at] = partial(at)
            pair_copy(turn, j).start()
            return carry

        lax.fori_loop(0, half_slabs, give, 0)

        def keep(j, carry):
            value = partial(core * half_slabs + j)
            pair_copy(turn, j).wait_recv()
            value = (value + received[turn, j]).reshape(chips, GROUP, rows)
            total[j] = value
            sent[turn, j] = value.astype(jnp.bfloat16)
            each_chip(lambda step: fold_copy(turn, j, step).start())
            return carry

        lax.fori_loop(0, half_slabs, keep, 0)

        def added(ref, start):
            def body(step, carry):
                return carry + ref[other(step)].astype(jnp.float32)

            return lax.fori_loop(1, chips, body, start, unroll=True)

        all_of(terms_in.at[turn, other_chips], term_send.at[turn], term_recv.at[turn]).wait_recv()
        whole[turn, core, :, plan.half:] = added(terms_in.at[turn], terms_in[turn, chip].astype(jnp.float32))
        for j in range(half_slabs):
            all_of(folded_in.at[turn, j, other_chips], fold_send.at[turn], fold_recv.at[turn, j]).wait_recv()
            whole[turn, core, :, j * rows:(j + 1) * rows] = added(folded_in.at[turn, j], total[j, chip])
        mine, theirs = whole.at[turn, core], whole.at[turn, 1 - core]
        remote(mine, mine, whole_send.at[turn], whole_recv.at[turn], partner).start()
        remote(theirs, theirs, whole_send.at[turn], whole_recv.at[turn], partner).wait_recv()
        values = jnp.concatenate(
            [whole[turn, half, :, j * LANES:(j + 1) * LANES] for half in range(2) for j in range(half_blocks)], 0
        )
        scalars = whole[turn, 0, :, plan.half:] + whole[turn, 1, :, plan.half:]
        return values, [joined(scalars, at) for at in range(len(terms))]

    def gather_copy(phase, step):
        here = gathered.at[phase, core, chip]
        return remote(here, here, gather_send.at[phase], gather_recv.at[phase], device(other(step)))

    def relay_copy(phase, which):
        here = gathered.at[phase, which]
        return remote(here, here, relay_send.at[phase], relay_recv.at[phase], partner)

    def shared(phase, values, terms):
        wide = values.astype(jnp.float32)
        for half in range(2):
            for j in range(half_blocks):
                low = (half * half_blocks + j) * GROUP
                folded[half, :, j * LANES:(j + 1) * LANES] = wide[low:low + GROUP]
            folded[half, :, plan.half:] = pieces(in_lanes(terms, GROUP))
        gathered[phase, core, chip] = folded[core].astype(jnp.bfloat16)
        each_chip(lambda step: gather_copy(phase, step).start())
        all_of(gathered.at[phase, core, other_chips], gather_send.at[phase], gather_recv.at[phase]).wait_recv()
        relay_copy(phase, core).start()
        relay_copy(phase, 1 - core).wait_recv()
        for half in range(2):
            for j in range(half_slabs):
                part = gathered[phase, half, :, :, j * rows:(j + 1) * rows].astype(jnp.float32)
                low = half * plan.half + j * rows
                filtered[:, low:low + rows] = part.reshape(plan.columns, rows).astype(jnp.bfloat16)
        scalars = gathered[phase, 0, :, :, plan.half:].astype(jnp.float32).reshape(plan.columns, LANES)
        return [joined(scalars, at) for at in range(len(terms))]

    def inner(left, right):
        together = (left * right).reshape(plan.blocks, GROUP, LANES)
        return over(jnp.sum(together, 0))

    chunks = [slice(low, min(low + 2 * LANES, plan.width)) for low in range(0, plan.width, 2 * LANES)]

    def transposed(span):
        part = block[:, :, span]
        return product(filtered[...], part.reshape(slabs * rows, part.shape[2]), NN)

    ridged = ridge_row * direc[...]
    terms = [over(resid[...] * direc[...]), over(ridged * direc[...])]
    values, (norm, ridge) = summed(0, direc[:, spans[1]].astype(jnp.bfloat16), terms, spans[1])
    first_values[...] = values
    kept = weighted(values)
    step_len = norm / (ridge + inner(values, kept.astype(jnp.float32)))
    (step_col,) = shared(0, kept, [step_len])
    terms = [0.0, 0.0, 0.0]
    for span in chunks:
        along, ridge_part = direc[:, span], ridge_row[:, span]
        left = resid[:, span] - step_col * (transposed(span) + ridge_part * along)
        ahead = scale_row[:, span] * left
        resid[:, span] = left
        solut[:, span] = step_col * along
        scal[:, span] = ahead
        ridged = ridge_part * ahead
        added = (over(left * ahead), over(ridged * ahead), over(ridged * along))
        terms = [term + more for term, more in zip(terms, added)]
    fresh, (norm_next, own_ridge, cross) = summed(1, scal[...].astype(jnp.bfloat16), terms, slice(0, plan.width))
    ratio = norm_next / norm
    ridge = own_ridge + ratio * (2.0 * cross + ratio * ridge)
    values = fresh + jnp.concatenate([ratio] * plan.blocks, 0) * first_values[...]
    kept = weighted(values)
    step_len = norm_next / (ridge + inner(values, kept.astype(jnp.float32)))
    step_col, ratio_col = shared(1, kept, [step_len, ratio])

    def put(out, tile, value):
        out[(tile + 1) * LANES:(tile + 2) * LANES, :] = value

    held = {}
    for span in chunks:
        along = scal[:, span] + ratio_col * direc[:, span]
        ahead = solut[:, span] + step_col * along
        left = resid[:, span] - step_col * (transposed(span) + ridge_row[:, span] * along)
        for low in range(0, span.stop - span.start, LANES):
            held[(span.start + low) // LANES] = (ahead[:, low:low + LANES].T, left[:, low:low + LANES].T)
        for tile in [tile for tile in held if tile < plan.full]:
            new_ahead, new_left = held.pop(tile)
            put(solution_out, tile, new_ahead)
            put(residual_out, tile, new_left)
    mixed, last = held[plan.full], held[plan.full + 1]
    for out, edge, end in ((solution_out, mixed[0], last[0]), (residual_out, mixed[1], last[1])):
        out[:LANES, :] = edge
        put(out, plan.full, edge)
        low = pl.multiple_of((plan.full + 1) * LANES + offset, plan.rest)
        out[pl.ds(low, plan.rest), :] = end[:plan.rest]

    all_of(shown.at[others], show_send, show_recv).wait_send()
    for part, (low, size) in enumerate(((0, plan.cut), (plan.cut, plan.mixed_at - plan.cut), (plan.mixed_at, LANES))):
        all_of(block.at[others, :, pl.ds(low, size)], block_send.at[part], loose_recv).wait_send()
    all_of(loose.at[others], block_send.at[3], loose_recv).wait_send()
    all_of(early.at[core, near_others], early_send, early_recv).wait_send()
    all_of(early.at[core], early_relay_send, early_relay_recv).wait_send()
    for turn in range(2):
        all_of(received.at[turn], pair_send.at[turn], pair_recv.at[turn, 0]).wait_send()
        all_of(sent.at[turn, :, other_chips], fold_send.at[turn], fold_recv.at[turn, 0]).wait_send()
        all_of(sent_terms.at[turn, other_chips], term_send.at[turn], term_recv.at[turn]).wait_send()
        all_of(whole.at[turn, core], whole_send.at[turn], whole_recv.at[turn]).wait_send()
        all_of(gathered.at[turn, core, other_chips], gather_send.at[turn], gather_recv.at[turn]).wait_send()
        all_of(gathered.at[turn, core], relay_send.at[turn], relay_recv.at[turn]).wait_send()


def far(value):
    return pltpu.with_memory_space_constraint(value, pltpu.HBM)


def fused_shards(design, observed, slab_counts, gap_mask, filter_taps, kaula_diag, precond):
    epoch_rows, coef_rows = design.shape
    columns = observed.shape[1]
    slabs, coefs = lax.axis_size("tm"), lax.axis_size("coef")
    plan = Plan(slabs, coefs, epoch_rows, coef_rows, columns)
    wide, chips, message = plan.width, plan.chips, plan.message
    half_slabs, half_chips = slabs // 2, chips // 2
    f32, bf16 = jnp.float32, jnp.bfloat16
    vmem = pl.BlockSpec(memory_space=pltpu.VMEM)
    hbm = pl.BlockSpec(memory_space=pltpu.HBM)
    sem = pltpu.SemaphoreType.DMA
    shape = jax.ShapeDtypeStruct((wide + LANES, columns), f32)
    tiles = (plan.tiles, LANES)
    outs = pl.pallas_call(
        functools.partial(fused, plan),
        out_shape=(shape, shape),
        in_specs=[hbm, hbm, hbm, pl.BlockSpec(memory_space=pltpu.SMEM), hbm, hbm, hbm],
        out_specs=(vmem, vmem),
        scratch_shapes=[
            pltpu.VMEM((epoch_rows, columns), f32),
            pltpu.VMEM((epoch_rows // LANES, LANES), jnp.int32),
            pltpu.VMEM((1, LANES), f32),
            pltpu.VMEM(tiles, f32),
            pltpu.VMEM(tiles, f32),
            pltpu.VMEM((slabs, epoch_rows, wide), bf16),
            pltpu.VMEM((slabs, wide, epoch_rows), bf16),
            pltpu.VMEM((slabs, 2, epoch_rows, LANES), bf16),
            pltpu.VMEM((slabs, epoch_rows + plan.packed_rows, LANES), bf16),
            pltpu.VMEM((slabs, plan.packed_rows, LANES), bf16),
            pltpu.VMEM((chips, 2 * GROUP, epoch_rows), f32),
            pltpu.VMEM((slabs, 2 * GROUP, epoch_rows), f32),
            pltpu.VMEM((2, half_chips, GROUP, slabs * epoch_rows), bf16),
            pltpu.VMEM((2, slabs, columns, epoch_rows), f32),
            pltpu.VMEM((2, half_slabs, columns, epoch_rows), f32),
            pltpu.VMEM((half_slabs, chips, GROUP, epoch_rows), f32),
            pltpu.VMEM((2, half_slabs, chips, GROUP, epoch_rows), bf16),
            pltpu.VMEM((2, half_slabs, chips, GROUP, epoch_rows), bf16),
            pltpu.VMEM((2, chips, GROUP, LANES), bf16),
            pltpu.VMEM((2, chips, GROUP, LANES), bf16),
            pltpu.VMEM((2, 2, GROUP, message), f32),
            pltpu.VMEM((2, GROUP, message), f32),
            pltpu.VMEM((columns, slabs * epoch_rows), bf16),
            pltpu.VMEM((2, 2, chips, GROUP, message), bf16),
            pltpu.VMEM((columns, wide), f32),
            pltpu.VMEM((columns, wide), f32),
            pltpu.VMEM((columns, wide), f32),
            pltpu.VMEM((columns, wide), f32),
            pltpu.VMEM((plan.blocks * GROUP, LANES), f32),
            sem(()), sem((5,)), sem(()), sem((4,)), sem((2, slabs)), sem(()), sem(()), sem(()),
            sem(()), sem(()), sem(()), sem(()),
            sem((2,)), sem((2, half_slabs)), sem((2,)), sem((2, half_slabs)), sem((2,)), sem((2,)), sem((2,)), sem((2,)),
            sem((2,)), sem((2,)), sem((2,)), sem((2,)),
        ],
        compiler_params=pltpu.CompilerParams(
            collective_id=0, has_side_effects=True, vmem_limit_bytes=48 * 1024 * 1024
        ),
    )(
        design, far(observed), far(gap_mask.reshape(-1, LANES)), slab_counts, far(filter_taps[None]),
        far(kaula_diag.reshape(tiles)), far(precond.reshape(tiles)),
    )
    owner = lax.axis_index("tm")
    low = owner * plan.owned - plan.first_tile(owner) * LANES
    return tuple(lax.dynamic_slice_in_dim(out, low, plan.owned, 0) for out in outs)


def shards(*arrays):
    design, observed, filter_taps = arrays[0], arrays[1], arrays[4]
    sizes = (lax.axis_size("tm"), lax.axis_size("coef"), *design.shape, observed.shape[1], filter_taps.shape[0])
    return fused_shards(*arrays) if fits(*sizes) else general_shards(*arrays)


def solution(mesh):
    placed = (P("tm", "coef"), P("tm", None), P("tm"), P("tm"), P(), P("coef"), P("coef"))
    return jax.shard_map(
        shards,
        mesh=mesh,
        in_specs=placed,
        out_specs=(P(("coef", "tm"), None), P(("coef", "tm"), None)),
        check_vma=False,
    )
```

```python
import functools

import jax
import jax.numpy as jnp
from jax import lax
from jax.experimental import pallas as pl
from jax.experimental.pallas import tpu as pltpu
from jax.sharding import PartitionSpec as P

ITERS = 2
HIGHEST = lax.Precision.HIGHEST


def toeplitz(pattern, band_len):
    tiled = jnp.tile(pattern, band_len)[: band_len * (2 * band_len - 1)]
    return tiled.reshape(band_len, 2 * band_len - 1)[:, :band_len]


def block_pair(filter_taps):
    band_len = filter_taps.shape[0]
    spacer = jnp.zeros((band_len,), jnp.float32)
    reversed_taps = filter_taps[:0:-1]
    lower = jnp.concatenate([filter_taps[:1], spacer, reversed_taps])
    upper = jnp.concatenate([jnp.zeros((1,), jnp.float32), reversed_taps, spacer])
    return (toeplitz(lower, band_len), toeplitz(upper, band_len))


def forward(values, lower_block, upper_block):
    band_len = lower_block.shape[0]
    blocks = values.reshape(-1, band_len, values.shape[1])
    previous = jnp.concatenate([jnp.zeros_like(blocks[:1]), blocks[:-1]], 0)
    result = jnp.einsum("ij,bjr->bir", lower_block, blocks, precision=HIGHEST)
    result = result + jnp.einsum("ij,bjr->bir", upper_block, previous, precision=HIGHEST)
    return result.reshape(values.shape)


def backward(values, lower_block, upper_block):
    band_len = lower_block.shape[0]
    blocks = values.reshape(-1, band_len, values.shape[1])
    following = jnp.concatenate([blocks[1:], jnp.zeros_like(blocks[:1])], 0)
    result = jnp.einsum("ji,bjr->bir", lower_block, blocks, precision=HIGHEST)
    result = result + jnp.einsum("ji,bjr->bir", upper_block, following, precision=HIGHEST)
    return result.reshape(values.shape)


def general_shards(design, observed, slab_counts, gap_mask, filter_taps, kaula_diag, precond):
    epoch_rows, coef_rows = design.shape
    columns = observed.shape[1]
    slabs = lax.axis_size("tm")
    epochs = slabs * epoch_rows
    owned_rows = coef_rows // slabs
    owner_index = lax.axis_index("tm")
    lower_block, upper_block = block_pair(filter_taps)
    position = jnp.arange(epoch_rows, dtype=jnp.int32)
    local_weight = ((gap_mask == 1) & (position < slab_counts[0])).astype(jnp.float32)
    packed = jnp.concatenate([observed, local_weight.reshape(-1, columns)], 0)
    gathered = lax.all_gather(packed, "tm", axis=0, tiled=False)
    all_observed = gathered[:, :epoch_rows].reshape(epochs, columns)
    weight = gathered[:, epoch_rows:].reshape(epochs, 1)
    block = lax.all_to_all(design, "tm", split_axis=1, concat_axis=0, tiled=True)

    def weighted(values):
        inner = forward(weight * values, lower_block, upper_block)
        return (weight * backward(inner, lower_block, upper_block)).astype(jnp.bfloat16)

    def transposed(filtered):
        return lax.dot_general(
            block, filtered, (((0,), (0,)), ((), ())), preferred_element_type=jnp.float32
        )

    def summed(scaled, terms):
        partial = jnp.dot(block, scaled.astype(jnp.bfloat16), preferred_element_type=jnp.float32)
        rows = [jnp.sum(term, 0)[None] for term in terms]
        rows.append(jnp.zeros((8 - len(rows), columns), jnp.float32))
        total = lax.psum(jnp.concatenate([partial] + rows, 0), ("tm", "coef"))
        return total[:epochs], [total[epochs + at] for at in range(len(terms))]

    start = owner_index * owned_rows
    kaula_col = lax.dynamic_slice_in_dim(kaula_diag, start, owned_rows, 0)[:, None]
    precond_col = lax.dynamic_slice_in_dim(precond, start, owned_rows, 0)[:, None]
    residual = transposed(weighted(all_observed))
    solution = jnp.zeros_like(residual)
    for iteration in range(ITERS):
        scaled = precond_col * residual
        terms = [residual * scaled, kaula_col * scaled * scaled]
        if iteration == 0:
            slab_values, (norm_now, ridge) = summed(scaled, terms)
            direction = scaled
        else:
            terms.append(kaula_col * scaled * direction)
            fresh, (norm_next, own_ridge, cross) = summed(scaled, terms)
            ratio = norm_next / norm_now
            slab_values = fresh + ratio * slab_values
            ridge = own_ridge + ratio * (2.0 * cross + ratio * ridge)
            direction = scaled + ratio * direction
            norm_now = norm_next
        filtered = weighted(slab_values)
        curvature = ridge + jnp.sum(slab_values * filtered.astype(jnp.float32), 0)
        step_len = norm_now / curvature
        image = transposed(filtered) + kaula_col * direction
        solution = solution + step_len * direction
        residual = residual - step_len * image
    return (solution, residual)


LANES = 128
GROUP = 8
MESH = pl.DeviceIdType.MESH
NN = ((1,), (0,))
NT = ((1,), (1,))


class Plan:
    def __init__(self, slabs, coefs, epoch_rows, coef_rows, columns):
        self.slabs, self.coefs, self.epoch_rows, self.columns = slabs, coefs, epoch_rows, columns
        self.tiles = coef_rows // LANES
        self.owned = coef_rows // slabs
        self.full = self.owned // LANES - 1
        self.rest = self.owned % LANES
        self.packed_rows = epoch_rows * self.rest // LANES
        self.mixed_at = self.full * LANES
        self.width = (self.full + 2) * LANES
        self.cut = (self.full - 1) * LANES
        self.across = coefs // 2
        self.chips = slabs * self.across
        self.blocks = slabs * epoch_rows // LANES
        self.half_blocks = self.blocks // 2
        per_slab, half_slabs = epoch_rows // LANES, slabs // 2
        ends = [(upto + 1) * per_slab - 1 for upto in range(1, half_slabs - 1)] + [self.half_blocks]
        self.groups = list(zip([0] + ends[:-1], ends))
        self.message = LANES * (1 + max(end - begin for begin, end in self.groups))

    def first_tile(self, owner):
        return lax.div(owner * self.owned, LANES)


def fits(slabs, coefs, epoch_rows, coef_rows, columns, taps):
    if slabs & (slabs - 1) or slabs < 4 or coefs % 2 or epoch_rows % (2 * LANES) or coef_rows % LANES:
        return False
    if coef_rows % slabs or taps != LANES or columns != LANES or columns != GROUP * slabs * coefs // 2:
        return False
    owned = coef_rows // slabs
    rest = owned % LANES
    return owned >= 4 * LANES and rest >= 16 and LANES % rest == 0


def flipped(index, bits, count):
    result, weight = 0, 1
    while weight < count:
        bit = lax.rem(lax.div(index, weight), 2)
        result = result + weight * (1 - bit if bits & weight else bit)
        weight *= 2
    return result


def pieces(values):
    high = values.astype(jnp.bfloat16).astype(jnp.float32)
    left = values - high
    middle = left.astype(jnp.bfloat16).astype(jnp.float32)
    low = (left - middle).astype(jnp.bfloat16).astype(jnp.float32)
    return high + pltpu.roll(middle, 8, 1) + pltpu.roll(low, 16, 1)


def joined(values, at):
    lane = lax.broadcasted_iota(jnp.int32, values.shape, 1)
    taken = (lane % 8 == at) & (lane < 24)
    return jnp.sum(jnp.where(taken, values, 0.0), 1, keepdims=True)


def in_lanes(terms, rows):
    lane = lax.broadcasted_iota(jnp.int32, (rows, LANES), 1)
    result = jnp.zeros((rows, LANES), jnp.float32)
    for at, term in enumerate(terms):
        result = jnp.where(lane == at, term, result)
    return result


def product(left, right, contract, precision=None):
    return lax.dot_general(
        left, right, (contract, ((), ())), precision=precision, preferred_element_type=jnp.float32
    )


def fused(plan, design, observed_in, gap_in, counts, taps_in, kaula_in, precond_in, solution_out, residual_out,
          observed, gap, taps, kaula, precond,
          block, turned_block, edges, packed, loose, shown, seen, early, sums, received, total, sent, folded_in, sent_terms, terms_in,
          whole, entering, weights, filtered, gathered, resid, direc, scal, solut, first_values,
          own_sem, small_sem, edge_sem, block_send, block_recv, loose_recv, show_send, show_recv, early_send, early_recv,
          early_relay_send, early_relay_recv, pair_send, pair_recv, fold_send, fold_recv, term_send, term_recv,
          whole_send, whole_recv, middle_send, middle_recv, gather_send, gather_recv, relay_send, relay_recv):
    slabs, chips, rows = plan.slabs, plan.chips, plan.epoch_rows
    half_slabs, half_chips, half_blocks = slabs // 2, chips // 2, plan.half_blocks
    slab, coef = lax.axis_index("tm"), lax.axis_index("coef")
    across, core = lax.div(coef, 2), lax.rem(coef, 2)
    chip = slab * plan.across + across
    near_chip = lax.rem(chip, half_chips)
    this_half = lax.div(chip, half_chips)
    partner = {"tm": slab, "coef": 2 * across + 1 - core}

    def device(at):
        return {"tm": lax.div(at, plan.across), "coef": 2 * lax.rem(at, plan.across) + core}

    def other(step):
        return lax.rem(chip + step, chips)

    def near_other(step):
        return lax.rem(near_chip + step, half_chips)

    def remote(src, dst, send, recv, target):
        return pltpu.make_async_remote_copy(
            src_ref=src, dst_ref=dst, send_sem=send, recv_sem=recv, device_id=target, device_id_type=MESH
        )

    barrier = pltpu.get_barrier_semaphore()
    for step in range(1, chips):
        pl.semaphore_signal(barrier, inc=1, device_id=device(other(step)), device_id_type=MESH)
    pl.semaphore_signal(barrier, inc=1, device_id=partner, device_id_type=MESH)

    small = [
        pltpu.make_async_copy(src, dst, small_sem.at[at])
        for at, (src, dst) in enumerate(
            ((observed_in, observed), (gap_in, gap), (taps_in, taps), (kaula_in, kaula), (precond_in, precond))
        )
    ]
    for copy in small:
        copy.start()
    first = plan.first_tile(slab)
    offset = slab * plan.owned - first * LANES

    def tile_columns(tile, size):
        return pl.ds(pl.multiple_of(tile * LANES, LANES), size)

    own = pltpu.make_async_copy(
        design.at[:, tile_columns(first + 1, plan.mixed_at)], block.at[slab, :, pl.ds(0, plan.mixed_at)], own_sem
    )
    own.start()
    for owner in range(slabs):
        begin = owner * plan.owned // LANES
        for at, tile in enumerate((begin, begin + plan.full + 1)):
            pltpu.make_async_copy(
                design.at[:, pl.ds(tile * LANES, LANES)], edges.at[owner, at], edge_sem
            ).start()

    for copy in small[:3]:
        copy.wait()
    place = lax.broadcasted_iota(jnp.int32, (1, rows), 1)
    present = jnp.concatenate([gap[at:at + 1, :] for at in range(rows // LANES)], 1)
    weight_row = jnp.where((present == 1) & (place < counts[0]), 1.0, 0.0)
    turned = observed[...].T * weight_row
    shown[:, :GROUP, :] = turned.reshape(chips, GROUP, rows)
    shown[:, GROUP:, :] = jnp.broadcast_to(weight_row[None], (chips, GROUP, rows))
    seen[slab] = shown[2 * near_chip + core]

    def block_copy(bits, part):
        peer = flipped(slab, bits, slabs)
        tile = plan.first_tile(peer) + 1
        if part == 0:
            src, dst = design.at[:, tile_columns(tile, plan.cut)], block.at[slab, :, pl.ds(0, plan.cut)]
        elif part == 1:
            src = design.at[:, tile_columns(tile + plan.cut // LANES, plan.mixed_at - plan.cut)]
            dst = block.at[slab, :, pl.ds(plan.cut, plan.mixed_at - plan.cut)]
        elif part == 2:
            src, dst = packed.at[peer, pl.ds(0, rows)], block.at[slab, :, pl.ds(plan.mixed_at, LANES)]
        else:
            src, dst = packed.at[peer, pl.ds(rows, plan.packed_rows)], loose.at[slab]
        return remote(src, dst, block_send.at[part], loose_recv if part == 3 else block_recv.at[min(part, 1), slab], {"tm": peer, "coef": coef})

    def block_arrival(bits, part):
        peer = flipped(slab, bits, slabs)
        low, size = ((0, plan.cut), (plan.cut, plan.mixed_at + LANES - plan.cut))[part]
        dst = block.at[peer, :, pl.ds(low, size)]
        return remote(dst, dst, block_send.at[part], block_recv.at[part, peer], {"tm": peer, "coef": coef})

    def all_of(ref, send, recv):
        return remote(ref, ref, send, recv, partner)

    def show_copy(bits):
        peer = flipped(slab, bits, slabs)
        src = shown.at[2 * lax.rem(peer * plan.across + across, half_chips) + core]
        return remote(src, seen.at[slab], show_send, show_recv, {"tm": peer, "coef": coef})

    others = pl.ds(0, slabs - 1)
    pl.semaphore_wait(barrier, chips)
    for bits in range(1, slabs):
        show_copy(bits).start()
    for bits in range(1, half_slabs):
        block_copy(bits, 0).start()
        block_copy(bits, 1).start()
    for bits in range(half_slabs, slabs):
        block_copy(bits, 0).start()

    pltpu.make_async_copy(edges, edges, edge_sem).wait()
    lane_row = lax.broadcasted_iota(jnp.int32, (1, LANES), 1)
    for owner in range(slabs):
        skip = owner * plan.owned % LANES
        ahead = edges[owner, 0].astype(jnp.float32)
        behind = edges[owner, 1].astype(jnp.float32)
        packed[owner, :rows] = jnp.where(lane_row >= skip, ahead, behind).astype(jnp.bfloat16)
        tight = jnp.zeros((plan.packed_rows, LANES), jnp.float32)
        for at in range(LANES // plan.rest):
            part = behind[at * plan.packed_rows:(at + 1) * plan.packed_rows]
            shift = (at * plan.rest - skip) % LANES
            part = pltpu.roll(part, shift, 1) if shift else part
            tight = jnp.where(lax.div(lane_row, plan.rest) == at, part, tight)
        packed[owner, rows:] = tight.astype(jnp.bfloat16)
    for bits in range(1, slabs):
        block_copy(bits, 2).start()
        block_copy(bits, 3).start()

    def unpack(at, tight):
        tight = tight.astype(jnp.float32)
        for piece in range(LANES // plan.rest):
            part = pltpu.roll(tight, LANES - piece * plan.rest, 1) if piece else tight
            part = jnp.where(lane_row < plan.rest, part, 0.0).astype(jnp.bfloat16)
            block[at, piece * plan.packed_rows:(piece + 1) * plan.packed_rows, plan.mixed_at + LANES:] = part

    block[slab, :, plan.mixed_at:plan.mixed_at + LANES] = packed[slab, :rows]
    unpack(slab, packed[slab, rows:])

    base = jnp.concatenate([taps[...], jnp.zeros((1, LANES), jnp.float32)], 1)
    shifted = pltpu.roll(jnp.broadcast_to(base, (LANES, 2 * LANES)), 0, 1, stride=1, stride_axis=0)
    lower, upper = shifted[:, :LANES], shifted[:, LANES:]
    blank = jnp.zeros((GROUP, LANES), jnp.float32)

    all_of(seen.at[others], show_send, show_recv).wait_recv()

    def stack(ref, low):
        return jnp.concatenate(
            [ref[at, low:low + GROUP, j * LANES:(j + 1) * LANES] for at in range(slabs) for j in range(rows // LANES)], 0
        )

    weight = stack(seen, GROUP)

    def weighted(values):
        entering = weight * values
        before = jnp.concatenate([blank, entering[:-GROUP]], 0)
        inner = product(entering, lower, NN, lax.Precision.HIGHEST) + product(before, upper, NN, lax.Precision.HIGHEST)
        after = jnp.concatenate([inner[GROUP:], blank], 0)
        outer = product(inner, lower, NT, lax.Precision.HIGHEST) + product(after, upper, NT, lax.Precision.HIGHEST)
        return (weight * outer).astype(jnp.bfloat16)

    def nearer(span):
        parts = [span[:, at * LANES:(at + 1) * LANES] for at in range(rows // LANES)]
        return [jnp.where(core == 0, left, right) for left, right in zip(parts[::-1], parts)]

    def outward(at, which):
        return which * (half_slabs + at) + (1 - which) * (half_slabs - 1 - at)

    for at in range(half_slabs):
        for j, part in enumerate(nearer(seen[outward(at, core), GROUP:, :])):
            weights[at * (rows // LANES) + j] = part
    exact = lax.Precision.HIGHEST
    ends_block = product(lower, lower, NT, exact)
    same_block = ends_block + product(upper, upper, NT, exact)
    before_block, after_block = product(upper, lower, NT, exact), product(lower, upper, NT, exact)
    inside_block = jnp.where(core == 0, after_block, before_block)
    outside_block = jnp.where(core == 0, before_block, after_block)
    ends_block = jnp.where(core == 0, same_block, ends_block)

    kept = weighted(stack(seen, 0)).astype(jnp.float32)
    for j in range(plan.blocks):
        early[core, near_chip, :, j * LANES:(j + 1) * LANES] = kept[j * GROUP:(j + 1) * GROUP].astype(jnp.bfloat16)
    for step in range(1, half_chips):
        to = near_other(step)
        here = early.at[core, near_chip]
        target = device(this_half * half_chips + to)
        remote(here, here, early_send, early_recv, target).start()
    for bits in range(half_slabs, slabs):
        block_copy(bits, 1).start()

    small[3].wait()
    small[4].wait()

    def local_row(table):
        inside = [table[pl.ds(first + 1 + at, 1), :] for at in range(plan.full)]
        ahead, behind = table[pl.ds(first, 1), :], table[pl.ds(first + plan.full + 1, 1), :]
        moved = pltpu.roll(jnp.broadcast_to(behind, (GROUP, LANES)), lax.rem(LANES - offset, LANES), 1)[:1]
        mixed = jnp.where(lane_row >= offset, ahead, behind)
        return jnp.concatenate(inside + [mixed, jnp.where(lane_row < plan.rest, moved, 0.0)], 1)

    ridge_row, scale_row = local_row(kaula), local_row(precond)

    near_others = pl.ds(0, half_chips - 1)
    all_of(early.at[core, near_others], early_send, early_recv).wait_recv()
    mine, theirs = early.at[core], early.at[1 - core]
    remote(mine, mine, early_relay_send, early_relay_recv, partner).start()
    remote(theirs, theirs, early_relay_send, early_relay_recv, partner).wait_recv()
    for at in range(slabs):
        span = slice(at * rows, (at + 1) * rows)
        both = jnp.stack([early[0, :, :, span].astype(jnp.float32), early[1, :, :, span].astype(jnp.float32)], 1)
        filtered[:, span] = both.reshape(plan.columns, rows).astype(jnp.bfloat16)

    def series(at):
        return filtered[:, pl.ds(pl.multiple_of(at * rows, rows), rows)]

    def over(terms):
        return jnp.sum(terms, 1, keepdims=True)

    own.wait()
    spans = (slice(0, plan.cut), slice(plan.cut, plan.width))

    def turn_over(at, span):
        turned_block[at, span] = block[at, :, span].T

    for part, span in enumerate(spans):
        if part:
            all_of(loose.at[others], block_send.at[3], loose_recv).wait_recv()
        turn_over(slab, span)
        resid[:, span] = product(series(slab), block[slab, :, span], NN)
        for bits in range(1, slabs):
            peer = flipped(slab, bits, slabs)
            block_arrival(bits, part).wait_recv()
            if part:
                unpack(peer, loose[peer])
            turn_over(peer, span)
            resid[:, span] += product(series(peer), block[peer, :, span], NN)
        direc[:, span] = scale_row[:, span] * resid[:, span]
        if part == 0:
            low = direc[:, span].astype(jnp.bfloat16)

            def body(at, carry):
                sums[0, at] = product(low, turned_block[at, :plan.cut], NN)
                return carry

            lax.fori_loop(0, slabs, body, 0)

    def pair_copy(turn, j):
        src = sums.at[turn, outward(j, 1 - core)]
        return remote(src, received.at[turn, j], pair_send.at[turn], pair_recv.at[turn, j], partner)

    def fold_copy(turn, j, step):
        to = other(step)
        src, dst = sent.at[turn, j, to], folded_in.at[turn, j, chip]
        return remote(src, dst, fold_send.at[turn], fold_recv.at[turn, j], device(to))

    other_chips = pl.ds(0, chips - 1)

    def term_copy(turn, step):
        to = other(step)
        src, dst = sent_terms.at[turn, to], terms_in.at[turn, chip]
        return remote(src, dst, term_send.at[turn], term_recv.at[turn], device(to))

    def each_chip(action):
        def body(at, carry):
            action(half_chips + (1 - 2 * lax.rem(at, 2)) * lax.div(at + 1, 2))
            return carry

        lax.fori_loop(0, chips - 1, body, 0)

    def filtered_sum(turn, low, terms, span, settle):
        scalars = in_lanes(terms, plan.columns)
        sent_terms[turn] = pieces(scalars).reshape(chips, GROUP, LANES).astype(jnp.bfloat16)
        terms_in[turn, chip] = sent_terms[turn, chip]
        each_chip(lambda step: term_copy(turn, step).start())

        def partial(at):
            value = product(low, turned_block[at, span], NN)
            return value + sums[turn, at] if turn == 0 else value

        def give(j):
            at = outward(j, 1 - core)
            sums[turn, at] = partial(at)
            pair_copy(turn, j).start()

        def keep(j):
            value = partial(outward(j, core))
            pair_copy(turn, j).wait_recv()
            value = (value + received[turn, j]).reshape(chips, GROUP, rows)
            total[j] = value
            sent[turn, j] = value.astype(jnp.bfloat16)
            each_chip(lambda step: fold_copy(turn, j, step).start())

        def both(j, carry):
            give(j + 1)
            keep(j)
            return carry

        give(0)
        lax.fori_loop(0, half_slabs - 1, both, 0)
        keep(half_slabs - 1)

        def added(ref, start):
            def body(step, carry):
                return carry + ref[other(step)].astype(jnp.float32)

            return lax.fori_loop(1, chips, body, start, unroll=True)

        all_of(terms_in.at[turn, other_chips], term_send.at[turn], term_recv.at[turn]).wait_recv()
        whole[turn, core] = added(terms_in.at[turn], terms_in[turn, chip].astype(jnp.float32))
        mine, theirs = whole.at[turn, core], whole.at[turn, 1 - core]
        remote(mine, mine, whole_send.at[turn], whole_recv.at[turn], partner).start()
        remote(theirs, theirs, whole_send.at[turn], whole_recv.at[turn], partner).wait_recv()
        scalars = whole[turn, 0] + whole[turn, 1]
        scalars = [joined(scalars, at) for at in range(len(terms))]
        ratio, more = settle(scalars)

        per_slab = rows // LANES
        overlap = jnp.zeros((GROUP, LANES), jnp.float32)
        group = 0
        entering[turn, half_blocks + 1] = blank
        for j in range(half_slabs):
            all_of(folded_in.at[turn, j, other_chips], fold_send.at[turn], fold_recv.at[turn, j]).wait_recv()
            for at, value in enumerate(nearer(added(folded_in.at[turn, j], total[j, chip]))):
                at = j * per_slab + at
                if ratio is not None:
                    value = value + ratio * first_values[0, at]
                first_values[turn, at] = value
                entering[turn, at + 1] = weights[at] * value
            if j == 0:
                middle_copy(turn, 1).start()
                continue
            if j == 1:
                middle_copy(turn, 0).wait_recv()
            begin, end = plan.groups[group]
            count = end - begin

            def rows_of(ref):
                return ref.reshape(count * GROUP, LANES)

            here = rows_of(entering[turn, begin + 1:end + 1])
            outer = product(rows_of(entering[turn, begin:end]), inside_block, NN, exact)
            outer = outer + product(rows_of(entering[turn, begin + 2:end + 2]), outside_block, NN, exact)
            if end == half_blocks:
                kept = jnp.concatenate([
                    product(here[:-GROUP], same_block, NN, exact), product(here[-GROUP:], ends_block, NN, exact)
                ], 0)
            else:
                kept = product(here, same_block, NN, exact)
            kept = (rows_of(weights[begin:end]) * (outer + kept)).astype(jnp.bfloat16).astype(jnp.float32)
            with_values = rows_of(first_values[turn, begin:end]) * kept
            overlap = overlap + jnp.sum(with_values.reshape(count, GROUP, LANES), 0)
            parts = [kept[at * GROUP:(at + 1) * GROUP] for at in range(count)]
            if end == half_blocks:
                parts.append(pieces(in_lanes([over(overlap)] + more, GROUP)))
            gathered[turn, group, core, chip, :, :len(parts) * LANES] = jnp.concatenate(parts, 1).astype(jnp.bfloat16)
            each_chip(lambda step: gather_copy(turn, group, step).start())
            group += 1
        for group in range(len(plan.groups)):
            everyone = gathered.at[turn, group, core, other_chips, :, pl.ds(0, extent(group))]
            all_of(everyone, gather_send.at[turn, group], gather_recv.at[turn, group]).wait_recv()
            relay_copy(turn, group, core).start()
        for group, (begin, end) in enumerate(plan.groups):
            relay_copy(turn, group, 1 - core).wait_recv()
            for half in range(2):
                for at in range(begin, end):
                    part = gathered[turn, group, half, :, :, (at - begin) * LANES:(at - begin + 1) * LANES]
                    part = part.astype(jnp.float32).reshape(plan.columns, LANES).astype(jnp.bfloat16)
                    low = (half_blocks + at if half else half_blocks - 1 - at) * LANES
                    filtered[:, low:low + LANES] = part
        last = len(plan.groups) - 1
        span = slice(extent(last) - LANES, extent(last))
        first_terms, second_terms = [
            gathered[turn, last, half, :, :, span].astype(jnp.float32).reshape(plan.columns, LANES) for half in range(2)
        ]
        norm, ridge = joined(first_terms, 1), joined(first_terms, 2)
        step_col = norm / (ridge + joined(first_terms, 0) + joined(second_terms, 0))
        return scalars, ratio, step_col, joined(first_terms, 3)

    def extent(group):
        begin, end = plan.groups[group]
        return LANES * (end - begin + (end == half_blocks))

    def middle_copy(turn, at):
        src, dst = entering.at[turn, 1], entering.at[turn, 0]
        return remote(src if at else dst, dst, middle_send.at[turn], middle_recv.at[turn], partner)

    def gather_copy(turn, group, step):
        here = gathered.at[turn, group, core, chip, :, pl.ds(0, extent(group))]
        return remote(here, here, gather_send.at[turn, group], gather_recv.at[turn, group], device(other(step)))

    def relay_copy(turn, group, which):
        here = gathered.at[turn, group, which, :, :, pl.ds(0, extent(group))]
        return remote(here, here, relay_send.at[turn, group], relay_recv.at[turn, group], partner)

    chunks = [slice(low, min(low + 2 * LANES, plan.width)) for low in range(0, plan.width, 2 * LANES)]

    def transposed(span):
        part = block[:, :, span]
        return product(filtered[...], part.reshape(slabs * rows, part.shape[2]), NN)

    ridged = ridge_row * direc[...]
    terms = [over(resid[...] * direc[...]), over(ridged * direc[...])]
    low = direc[:, spans[1]].astype(jnp.bfloat16)
    (norm, ridge), _, step_col, _ = filtered_sum(0, low, terms, spans[1], lambda sums_of: (None, list(sums_of)))
    terms = [0.0, 0.0, 0.0]
    for span in chunks:
        along, ridge_part = direc[:, span], ridge_row[:, span]
        left = resid[:, span] - step_col * (transposed(span) + ridge_part * along)
        ahead = scale_row[:, span] * left
        resid[:, span] = left
        solut[:, span] = step_col * along
        scal[:, span] = ahead
        ridged = ridge_part * ahead
        added = (over(left * ahead), over(ridged * ahead), over(ridged * along))
        terms = [term + more for term, more in zip(terms, added)]

    def settle(sums_of):
        norm_next, own_ridge, cross = sums_of
        ratio = norm_next / norm
        return ratio, [norm_next, own_ridge + ratio * (2.0 * cross + ratio * ridge), ratio]

    low = scal[...].astype(jnp.bfloat16)
    _, _, step_col, ratio_col = filtered_sum(1, low, terms, slice(0, plan.width), settle)

    def put(out, tile, value):
        out[(tile + 1) * LANES:(tile + 2) * LANES, :] = value

    held = {}
    for span in chunks:
        along = scal[:, span] + ratio_col * direc[:, span]
        ahead = solut[:, span] + step_col * along
        left = resid[:, span] - step_col * (transposed(span) + ridge_row[:, span] * along)
        for low in range(0, span.stop - span.start, LANES):
            held[(span.start + low) // LANES] = (ahead[:, low:low + LANES].T, left[:, low:low + LANES].T)
        for tile in [tile for tile in held if tile < plan.full]:
            new_ahead, new_left = held.pop(tile)
            put(solution_out, tile, new_ahead)
            put(residual_out, tile, new_left)
    mixed, last = held[plan.full], held[plan.full + 1]
    for out, edge, end in ((solution_out, mixed[0], last[0]), (residual_out, mixed[1], last[1])):
        out[:LANES, :] = edge
        put(out, plan.full, edge)
        low = pl.multiple_of((plan.full + 1) * LANES + offset, plan.rest)
        out[pl.ds(low, plan.rest), :] = end[:plan.rest]

    all_of(shown.at[others], show_send, show_recv).wait_send()
    for part, (low, size) in enumerate(((0, plan.cut), (plan.cut, plan.mixed_at - plan.cut), (plan.mixed_at, LANES))):
        all_of(block.at[others, :, pl.ds(low, size)], block_send.at[part], loose_recv).wait_send()
    all_of(loose.at[others], block_send.at[3], loose_recv).wait_send()
    all_of(early.at[core, near_others], early_send, early_recv).wait_send()
    all_of(early.at[core], early_relay_send, early_relay_recv).wait_send()
    for turn in range(2):
        all_of(received.at[turn], pair_send.at[turn], pair_recv.at[turn, 0]).wait_send()
        all_of(sent.at[turn, :, other_chips], fold_send.at[turn], fold_recv.at[turn, 0]).wait_send()
        all_of(sent_terms.at[turn, other_chips], term_send.at[turn], term_recv.at[turn]).wait_send()
        all_of(whole.at[turn, core], whole_send.at[turn], whole_recv.at[turn]).wait_send()
        middle_copy(turn, 1).wait_send()
        for group in range(len(plan.groups)):
            everyone = gathered.at[turn, group, core, other_chips, :, pl.ds(0, extent(group))]
            all_of(everyone, gather_send.at[turn, group], gather_recv.at[turn, group]).wait_send()
            relay_copy(turn, group, core).wait_send()


def far(value):
    return pltpu.with_memory_space_constraint(value, pltpu.HBM)


def fused_shards(design, observed, slab_counts, gap_mask, filter_taps, kaula_diag, precond):
    epoch_rows, coef_rows = design.shape
    columns = observed.shape[1]
    slabs, coefs = lax.axis_size("tm"), lax.axis_size("coef")
    plan = Plan(slabs, coefs, epoch_rows, coef_rows, columns)
    wide, chips, message = plan.width, plan.chips, plan.message
    half_slabs, half_chips = slabs // 2, chips // 2
    f32, bf16 = jnp.float32, jnp.bfloat16
    vmem = pl.BlockSpec(memory_space=pltpu.VMEM)
    hbm = pl.BlockSpec(memory_space=pltpu.HBM)
    sem = pltpu.SemaphoreType.DMA
    shape = jax.ShapeDtypeStruct((wide + LANES, columns), f32)
    tiles = (plan.tiles, LANES)
    outs = pl.pallas_call(
        functools.partial(fused, plan),
        out_shape=(shape, shape),
        in_specs=[hbm, hbm, hbm, pl.BlockSpec(memory_space=pltpu.SMEM), hbm, hbm, hbm],
        out_specs=(vmem, vmem),
        scratch_shapes=[
            pltpu.VMEM((epoch_rows, columns), f32),
            pltpu.VMEM((epoch_rows // LANES, LANES), jnp.int32),
            pltpu.VMEM((1, LANES), f32),
            pltpu.VMEM(tiles, f32),
            pltpu.VMEM(tiles, f32),
            pltpu.VMEM((slabs, epoch_rows, wide), bf16),
            pltpu.VMEM((slabs, wide, epoch_rows), bf16),
            pltpu.VMEM((slabs, 2, epoch_rows, LANES), bf16),
            pltpu.VMEM((slabs, epoch_rows + plan.packed_rows, LANES), bf16),
            pltpu.VMEM((slabs, plan.packed_rows, LANES), bf16),
            pltpu.VMEM((chips, 2 * GROUP, epoch_rows), f32),
            pltpu.VMEM((slabs, 2 * GROUP, epoch_rows), f32),
            pltpu.VMEM((2, half_chips, GROUP, slabs * epoch_rows), bf16),
            pltpu.VMEM((2, slabs, columns, epoch_rows), f32),
            pltpu.VMEM((2, half_slabs, columns, epoch_rows), f32),
            pltpu.VMEM((half_slabs, chips, GROUP, epoch_rows), f32),
            pltpu.VMEM((2, half_slabs, chips, GROUP, epoch_rows), bf16),
            pltpu.VMEM((2, half_slabs, chips, GROUP, epoch_rows), bf16),
            pltpu.VMEM((2, chips, GROUP, LANES), bf16),
            pltpu.VMEM((2, chips, GROUP, LANES), bf16),
            pltpu.VMEM((2, 2, GROUP, LANES), f32),
            pltpu.VMEM((2, plan.half_blocks + 2, GROUP, LANES), f32),
            pltpu.VMEM((plan.half_blocks, GROUP, LANES), f32),
            pltpu.VMEM((columns, slabs * epoch_rows), bf16),
            pltpu.VMEM((2, len(plan.groups), 2, chips, GROUP, message), bf16),
            pltpu.VMEM((columns, wide), f32),
            pltpu.VMEM((columns, wide), f32),
            pltpu.VMEM((columns, wide), f32),
            pltpu.VMEM((columns, wide), f32),
            pltpu.VMEM((2, plan.half_blocks, GROUP, LANES), f32),
            sem(()), sem((5,)), sem(()), sem((4,)), sem((2, slabs)), sem(()), sem(()), sem(()),
            sem(()), sem(()), sem(()), sem(()),
            sem((2,)), sem((2, half_slabs)), sem((2,)), sem((2, half_slabs)), sem((2,)), sem((2,)), sem((2,)), sem((2,)),
            sem((2,)), sem((2,)), *[sem((2, len(plan.groups)))] * 4,
        ],
        compiler_params=pltpu.CompilerParams(
            collective_id=0, has_side_effects=True, vmem_limit_bytes=48 * 1024 * 1024
        ),
    )(
        design, far(observed), far(gap_mask.reshape(-1, LANES)), slab_counts, far(filter_taps[None]),
        far(kaula_diag.reshape(tiles)), far(precond.reshape(tiles)),
    )
    owner = lax.axis_index("tm")
    low = owner * plan.owned - plan.first_tile(owner) * LANES
    return tuple(lax.dynamic_slice_in_dim(out, low, plan.owned, 0) for out in outs)


def shards(*arrays):
    design, observed, filter_taps = arrays[0], arrays[1], arrays[4]
    sizes = (lax.axis_size("tm"), lax.axis_size("coef"), *design.shape, observed.shape[1], filter_taps.shape[0])
    return fused_shards(*arrays) if fits(*sizes) else general_shards(*arrays)


def solution(mesh):
    placed = (P("tm", "coef"), P("tm", None), P("tm"), P("tm"), P(), P("coef"), P("coef"))
    return jax.shard_map(
        shards,
        mesh=mesh,
        in_specs=placed,
        out_specs=(P(("coef", "tm"), None), P(("coef", "tm"), None)),
        check_vma=False,
    )
```

```python
import functools

import jax
import jax.numpy as jnp
from jax import lax
from jax.experimental import pallas as pl
from jax.experimental.pallas import tpu as pltpu
from jax.sharding import PartitionSpec as P

ITERS = 2
HIGHEST = lax.Precision.HIGHEST


def toeplitz(pattern, band_len):
    tiled = jnp.tile(pattern, band_len)[: band_len * (2 * band_len - 1)]
    return tiled.reshape(band_len, 2 * band_len - 1)[:, :band_len]


def block_pair(filter_taps):
    band_len = filter_taps.shape[0]
    spacer = jnp.zeros((band_len,), jnp.float32)
    reversed_taps = filter_taps[:0:-1]
    lower = jnp.concatenate([filter_taps[:1], spacer, reversed_taps])
    upper = jnp.concatenate([jnp.zeros((1,), jnp.float32), reversed_taps, spacer])
    return (toeplitz(lower, band_len), toeplitz(upper, band_len))


def forward(values, lower_block, upper_block):
    band_len = lower_block.shape[0]
    blocks = values.reshape(-1, band_len, values.shape[1])
    previous = jnp.concatenate([jnp.zeros_like(blocks[:1]), blocks[:-1]], 0)
    result = jnp.einsum("ij,bjr->bir", lower_block, blocks, precision=HIGHEST)
    result = result + jnp.einsum("ij,bjr->bir", upper_block, previous, precision=HIGHEST)
    return result.reshape(values.shape)


def backward(values, lower_block, upper_block):
    band_len = lower_block.shape[0]
    blocks = values.reshape(-1, band_len, values.shape[1])
    following = jnp.concatenate([blocks[1:], jnp.zeros_like(blocks[:1])], 0)
    result = jnp.einsum("ji,bjr->bir", lower_block, blocks, precision=HIGHEST)
    result = result + jnp.einsum("ji,bjr->bir", upper_block, following, precision=HIGHEST)
    return result.reshape(values.shape)


def general_shards(design, observed, slab_counts, gap_mask, filter_taps, kaula_diag, precond):
    epoch_rows, coef_rows = design.shape
    columns = observed.shape[1]
    slabs = lax.axis_size("tm")
    epochs = slabs * epoch_rows
    owned_rows = coef_rows // slabs
    owner_index = lax.axis_index("tm")
    lower_block, upper_block = block_pair(filter_taps)
    position = jnp.arange(epoch_rows, dtype=jnp.int32)
    local_weight = ((gap_mask == 1) & (position < slab_counts[0])).astype(jnp.float32)
    packed = jnp.concatenate([observed, local_weight.reshape(-1, columns)], 0)
    gathered = lax.all_gather(packed, "tm", axis=0, tiled=False)
    all_observed = gathered[:, :epoch_rows].reshape(epochs, columns)
    weight = gathered[:, epoch_rows:].reshape(epochs, 1)
    block = lax.all_to_all(design, "tm", split_axis=1, concat_axis=0, tiled=True)

    def weighted(values):
        inner = forward(weight * values, lower_block, upper_block)
        return (weight * backward(inner, lower_block, upper_block)).astype(jnp.bfloat16)

    def transposed(filtered):
        return lax.dot_general(
            block, filtered, (((0,), (0,)), ((), ())), preferred_element_type=jnp.float32
        )

    def summed(scaled, terms):
        partial = jnp.dot(block, scaled.astype(jnp.bfloat16), preferred_element_type=jnp.float32)
        rows = [jnp.sum(term, 0)[None] for term in terms]
        rows.append(jnp.zeros((8 - len(rows), columns), jnp.float32))
        total = lax.psum(jnp.concatenate([partial] + rows, 0), ("tm", "coef"))
        return total[:epochs], [total[epochs + at] for at in range(len(terms))]

    start = owner_index * owned_rows
    kaula_col = lax.dynamic_slice_in_dim(kaula_diag, start, owned_rows, 0)[:, None]
    precond_col = lax.dynamic_slice_in_dim(precond, start, owned_rows, 0)[:, None]
    residual = transposed(weighted(all_observed))
    solution = jnp.zeros_like(residual)
    for iteration in range(ITERS):
        scaled = precond_col * residual
        terms = [residual * scaled, kaula_col * scaled * scaled]
        if iteration == 0:
            slab_values, (norm_now, ridge) = summed(scaled, terms)
            direction = scaled
        else:
            terms.append(kaula_col * scaled * direction)
            fresh, (norm_next, own_ridge, cross) = summed(scaled, terms)
            ratio = norm_next / norm_now
            slab_values = fresh + ratio * slab_values
            ridge = own_ridge + ratio * (2.0 * cross + ratio * ridge)
            direction = scaled + ratio * direction
            norm_now = norm_next
        filtered = weighted(slab_values)
        curvature = ridge + jnp.sum(slab_values * filtered.astype(jnp.float32), 0)
        step_len = norm_now / curvature
        image = transposed(filtered) + kaula_col * direction
        solution = solution + step_len * direction
        residual = residual - step_len * image
    return (solution, residual)


LANES = 128
GROUP = 8
MESH = pl.DeviceIdType.MESH
NN = ((1,), (0,))
NT = ((1,), (1,))


class Plan:
    def __init__(self, slabs, coefs, epoch_rows, coef_rows, columns):
        self.slabs, self.coefs, self.epoch_rows, self.columns = slabs, coefs, epoch_rows, columns
        self.tiles = coef_rows // LANES
        self.owned = coef_rows // slabs
        self.full = self.owned // LANES - 1
        self.rest = self.owned % LANES
        self.packed_rows = epoch_rows * self.rest // LANES
        self.mixed_at = self.full * LANES
        self.width = (self.full + 2) * LANES
        self.cut = (self.full - 1) * LANES
        self.across = coefs // 2
        self.chips = slabs * self.across
        self.blocks = slabs * epoch_rows // LANES
        self.half_blocks = self.blocks // 2
        per_slab, half_slabs = epoch_rows // LANES, slabs // 2
        ends = [(upto + 1) * per_slab - 1 for upto in range(1, half_slabs - 1)] + [self.half_blocks]
        self.groups = list(zip([0] + ends[:-1], ends))
        self.message = LANES * (1 + max(end - begin for begin, end in self.groups))

    def first_tile(self, owner):
        return lax.div(owner * self.owned, LANES)


def fits(slabs, coefs, epoch_rows, coef_rows, columns, taps):
    if slabs & (slabs - 1) or slabs < 4 or coefs % 2 or coefs & (coefs - 1) or epoch_rows % (2 * LANES) or coef_rows % LANES:
        return False
    if coef_rows % slabs or taps != LANES or columns != LANES or columns != GROUP * slabs * coefs // 2:
        return False
    owned = coef_rows // slabs
    rest = owned % LANES
    return owned >= 4 * LANES and rest >= 16 and LANES % rest == 0


def flips(index, count):
    steps, weight = [], 1
    while weight < count:
        steps.append(weight * (1 - 2 * lax.rem(lax.div(index, weight), 2)))
        weight *= 2
    return [sum((step for at, step in enumerate(steps) if bits >> at & 1), index) for bits in range(count)]


def pieces(values):
    high = values.astype(jnp.bfloat16).astype(jnp.float32)
    left = values - high
    middle = left.astype(jnp.bfloat16).astype(jnp.float32)
    low = (left - middle).astype(jnp.bfloat16).astype(jnp.float32)
    return high + pltpu.roll(middle, 8, 1) + pltpu.roll(low, 16, 1)


def joined(values, at):
    lane = lax.broadcasted_iota(jnp.int32, values.shape, 1)
    taken = (lane % 8 == at) & (lane < 24)
    return jnp.sum(jnp.where(taken, values, 0.0), 1, keepdims=True)


def in_lanes(terms, rows):
    lane = lax.broadcasted_iota(jnp.int32, (rows, LANES), 1)
    result = jnp.zeros((rows, LANES), jnp.float32)
    for at, term in enumerate(terms):
        result = jnp.where(lane == at, term, result)
    return result


def product(left, right, contract, precision=None):
    return lax.dot_general(
        left, right, (contract, ((), ())), precision=precision, preferred_element_type=jnp.float32
    )


def fused(plan, design, observed_in, gap_in, counts, taps_in, kaula_in, precond_in, solution_out, residual_out,
          observed, gap, taps, kaula, precond,
          block, turned_block, edges, packed, loose, shown, seen, seen_weight, early, sums, received, total, sent, folded_in, sent_terms, terms_in,
          whole, entering, weights, filtered, gathered, resid, direc, scal, solut, first_values,
          own_sem, small_sem, edge_sem, block_send, block_recv, loose_recv, show_send, show_recv, weight_send, weight_recv, early_send, early_recv,
          early_relay_send, early_relay_recv, pair_send, pair_recv, fold_send, fold_recv, term_send, term_recv,
          whole_send, whole_recv, middle_send, middle_recv, gather_send, gather_recv, relay_send, relay_recv):
    slabs, chips, rows = plan.slabs, plan.chips, plan.epoch_rows
    half_slabs, half_chips, half_blocks = slabs // 2, chips // 2, plan.half_blocks
    slab, coef = lax.axis_index("tm"), lax.axis_index("coef")
    across, core = lax.div(coef, 2), lax.rem(coef, 2)
    chip = slab * plan.across + across
    near_chip = lax.rem(chip, half_chips)
    partner = {"tm": slab, "coef": 2 * across + 1 - core}

    peers, sides = flips(slab, slabs), flips(across, plan.across)
    targets = [
        (peers[bits] * plan.across + sides[side], {"tm": peers[bits], "coef": coef + 2 * (sides[side] - across)})
        for bits in reversed(range(slabs)) for side in reversed(range(plan.across)) if bits or side
    ]
    near_targets = targets[-(half_chips - 1):]

    def remote(src, dst, send, recv, target):
        return pltpu.make_async_remote_copy(
            src_ref=src, dst_ref=dst, send_sem=send, recv_sem=recv, device_id=target, device_id_type=MESH
        )

    barrier = pltpu.get_barrier_semaphore()
    for _, target in targets:
        pl.semaphore_signal(barrier, inc=1, device_id=target, device_id_type=MESH)
    pl.semaphore_signal(barrier, inc=1, device_id=partner, device_id_type=MESH)

    small = [
        pltpu.make_async_copy(src, dst, small_sem.at[at])
        for at, (src, dst) in enumerate(
            ((observed_in, observed), (gap_in, gap), (taps_in, taps), (kaula_in, kaula), (precond_in, precond))
        )
    ]
    for copy in small:
        copy.start()
    first = plan.first_tile(slab)
    offset = slab * plan.owned - first * LANES

    def tile_columns(tile, size):
        return pl.ds(pl.multiple_of(tile * LANES, LANES), size)

    own = pltpu.make_async_copy(
        design.at[:, tile_columns(first + 1, plan.mixed_at)], block.at[slab, :, pl.ds(0, plan.mixed_at)], own_sem
    )
    own.start()
    for owner in range(slabs):
        begin = owner * plan.owned // LANES
        for at, tile in enumerate((begin, begin + plan.full + 1)):
            pltpu.make_async_copy(
                design.at[:, pl.ds(tile * LANES, LANES)], edges.at[owner, at], edge_sem
            ).start()

    for copy in small[:3]:
        copy.wait()
    tall = rows // LANES
    place = lax.broadcasted_iota(jnp.int32, (tall, LANES), 0) * LANES + lax.broadcasted_iota(jnp.int32, (tall, LANES), 1)
    local_weight = jnp.where((gap[...] == 1) & (place < counts[0]), 1.0, 0.0)
    seen_weight[slab] = local_weight
    weight_row = jnp.concatenate([local_weight[at:at + 1] for at in range(tall)], 1)
    turned = observed[...].T * weight_row
    shown[...] = turned.reshape(chips, GROUP, rows)
    seen[slab] = shown[2 * near_chip + core]
    for turn in range(2):
        for j in range(half_slabs):
            folded_in[turn, j, chip] = jnp.zeros((GROUP, rows), jnp.bfloat16)

    def block_copy(bits, part):
        peer = peers[bits]
        tile = plan.first_tile(peer) + 1
        if part == 0:
            src, dst = design.at[:, tile_columns(tile, plan.cut)], block.at[slab, :, pl.ds(0, plan.cut)]
        elif part == 1:
            src = design.at[:, tile_columns(tile + plan.cut // LANES, plan.mixed_at - plan.cut)]
            dst = block.at[slab, :, pl.ds(plan.cut, plan.mixed_at - plan.cut)]
        elif part == 2:
            src, dst = packed.at[peer, pl.ds(0, rows)], block.at[slab, :, pl.ds(plan.mixed_at, LANES)]
        else:
            src, dst = packed.at[peer, pl.ds(rows, plan.packed_rows)], loose.at[slab]
        return remote(src, dst, block_send.at[part], loose_recv if part == 3 else block_recv.at[min(part, 1), slab], {"tm": peer, "coef": coef})

    def block_arrival(bits, part):
        peer = peers[bits]
        low, size = ((0, plan.cut), (plan.cut, plan.mixed_at + LANES - plan.cut))[part]
        dst = block.at[peer, :, pl.ds(low, size)]
        return remote(dst, dst, block_send.at[part], block_recv.at[part, peer], {"tm": peer, "coef": coef})

    def all_of(ref, send, recv):
        return remote(ref, ref, send, recv, partner)

    def show_copy(bits):
        peer = peers[bits]
        src = shown.at[2 * lax.rem(peer * plan.across + across, half_chips) + core]
        return remote(src, seen.at[slab], show_send, show_recv, {"tm": peer, "coef": coef})

    def weight_copy(bits):
        src = seen_weight.at[slab]
        return remote(src, src, weight_send, weight_recv, {"tm": peers[bits], "coef": coef})

    others = pl.ds(0, slabs - 1)
    pl.semaphore_wait(barrier, chips)
    for bits in range(1, slabs):
        show_copy(bits).start()
        weight_copy(bits).start()
    for bits in range(1, half_slabs):
        block_copy(bits, 0).start()
        block_copy(bits, 1).start()
    for bits in range(half_slabs, slabs):
        block_copy(bits, 0).start()

    pltpu.make_async_copy(edges, edges, edge_sem).wait()
    lane_row = lax.broadcasted_iota(jnp.int32, (1, LANES), 1)
    for owner in range(slabs):
        skip = owner * plan.owned % LANES
        ahead = edges[owner, 0].astype(jnp.float32)
        behind = edges[owner, 1].astype(jnp.float32)
        packed[owner, :rows] = jnp.where(lane_row >= skip, ahead, behind).astype(jnp.bfloat16)
        tight = jnp.zeros((plan.packed_rows, LANES), jnp.float32)
        for at in range(LANES // plan.rest):
            part = behind[at * plan.packed_rows:(at + 1) * plan.packed_rows]
            shift = (at * plan.rest - skip) % LANES
            part = pltpu.roll(part, shift, 1) if shift else part
            tight = jnp.where(lax.div(lane_row, plan.rest) == at, part, tight)
        packed[owner, rows:] = tight.astype(jnp.bfloat16)
    for bits in range(1, slabs):
        block_copy(bits, 2).start()
        block_copy(bits, 3).start()

    def unpack(at, tight):
        tight = tight.astype(jnp.float32)
        for piece in range(LANES // plan.rest):
            part = pltpu.roll(tight, LANES - piece * plan.rest, 1) if piece else tight
            part = jnp.where(lane_row < plan.rest, part, 0.0).astype(jnp.bfloat16)
            block[at, piece * plan.packed_rows:(piece + 1) * plan.packed_rows, plan.mixed_at + LANES:] = part

    block[slab, :, plan.mixed_at:plan.mixed_at + LANES] = packed[slab, :rows]
    unpack(slab, packed[slab, rows:])

    base = jnp.concatenate([taps[...], jnp.zeros((1, LANES), jnp.float32)], 1)
    shifted = pltpu.roll(jnp.broadcast_to(base, (LANES, 2 * LANES)), 0, 1, stride=1, stride_axis=0)
    lower, upper = shifted[:, :LANES], shifted[:, LANES:]
    blank = jnp.zeros((GROUP, LANES), jnp.float32)

    all_of(seen.at[others], show_send, show_recv).wait_recv()
    all_of(seen_weight.at[others], weight_send, weight_recv).wait_recv()

    def repeated(at, j):
        return jnp.broadcast_to(seen_weight[at, j:j + 1, :], (GROUP, LANES))

    weight = jnp.concatenate([repeated(at, j) for at in range(slabs) for j in range(tall)], 0)
    own_series = jnp.concatenate([seen[at, :, j * LANES:(j + 1) * LANES] for at in range(slabs) for j in range(tall)], 0)

    def weighted(values):
        entering = weight * values
        before = jnp.concatenate([blank, entering[:-GROUP]], 0)
        inner = product(entering, lower, NN, lax.Precision.HIGHEST) + product(before, upper, NN, lax.Precision.HIGHEST)
        after = jnp.concatenate([inner[GROUP:], blank], 0)
        outer = product(inner, lower, NT, lax.Precision.HIGHEST) + product(after, upper, NT, lax.Precision.HIGHEST)
        return (weight * outer).astype(jnp.bfloat16)

    def nearer(span):
        parts = [span[:, at * LANES:(at + 1) * LANES] for at in range(rows // LANES)]
        return [jnp.where(core == 0, left, right) for left, right in zip(parts[::-1], parts)]

    def outward(at, which):
        return which * (half_slabs + at) + (1 - which) * (half_slabs - 1 - at)

    for at in range(half_slabs):
        place_of = outward(at, core)
        wide = jnp.concatenate([repeated(place_of, j) for j in range(tall)], 1)
        for j, part in enumerate(nearer(wide)):
            weights[at * tall + j] = part
    exact = lax.Precision.HIGHEST
    ends_block = product(lower, lower, NT, exact)
    same_block = ends_block + product(upper, upper, NT, exact)
    before_block, after_block = product(upper, lower, NT, exact), product(lower, upper, NT, exact)
    inside_block = jnp.where(core == 0, after_block, before_block)
    outside_block = jnp.where(core == 0, before_block, after_block)
    ends_block = jnp.where(core == 0, same_block, ends_block)

    kept = weighted(own_series).astype(jnp.float32)
    for j in range(plan.blocks):
        early[core, near_chip, :, j * LANES:(j + 1) * LANES] = kept[j * GROUP:(j + 1) * GROUP].astype(jnp.bfloat16)
    here = early.at[core, near_chip]
    for _, target in near_targets:
        remote(here, here, early_send, early_recv, target).start()
    for bits in range(half_slabs, slabs):
        block_copy(bits, 1).start()

    small[3].wait()
    small[4].wait()

    def local_row(table):
        inside = [table[pl.ds(first + 1 + at, 1), :] for at in range(plan.full)]
        ahead, behind = table[pl.ds(first, 1), :], table[pl.ds(first + plan.full + 1, 1), :]
        moved = pltpu.roll(jnp.broadcast_to(behind, (GROUP, LANES)), lax.rem(LANES - offset, LANES), 1)[:1]
        mixed = jnp.where(lane_row >= offset, ahead, behind)
        return jnp.concatenate(inside + [mixed, jnp.where(lane_row < plan.rest, moved, 0.0)], 1)

    ridge_row, scale_row = local_row(kaula), local_row(precond)

    near_others = pl.ds(0, half_chips - 1)
    all_of(early.at[core, near_others], early_send, early_recv).wait_recv()
    mine, theirs = early.at[core], early.at[1 - core]
    remote(mine, mine, early_relay_send, early_relay_recv, partner).start()
    remote(theirs, theirs, early_relay_send, early_relay_recv, partner).wait_recv()
    for at in range(slabs):
        span = slice(at * rows, (at + 1) * rows)
        both = jnp.stack([early[0, :, :, span].astype(jnp.float32), early[1, :, :, span].astype(jnp.float32)], 1)
        filtered[:, span] = both.reshape(plan.columns, rows).astype(jnp.bfloat16)

    def series(at):
        return filtered[:, pl.ds(pl.multiple_of(at * rows, rows), rows)]

    def over(terms):
        return jnp.sum(terms, 1, keepdims=True)

    own.wait()
    spans = (slice(0, plan.cut), slice(plan.cut, plan.width))

    def turn_over(at, span):
        turned_block[at, span] = block[at, :, span].T

    for part, span in enumerate(spans):
        if part:
            all_of(loose.at[others], block_send.at[3], loose_recv).wait_recv()
        turn_over(slab, span)
        resid[:, span] = product(series(slab), block[slab, :, span], NN)
        for bits in range(1, slabs):
            peer = peers[bits]
            block_arrival(bits, part).wait_recv()
            if part:
                unpack(peer, loose[peer])
            turn_over(peer, span)
            resid[:, span] += product(series(peer), block[peer, :, span], NN)
        direc[:, span] = scale_row[:, span] * resid[:, span]
        if part == 0:
            low = direc[:, span].astype(jnp.bfloat16)

            def body(at, carry):
                sums[0, at] = product(low, turned_block[at, :plan.cut], NN)
                return carry

            lax.fori_loop(0, slabs, body, 0)

    def pair_copy(turn, j):
        src = sums.at[turn, outward(j, 1 - core)]
        return remote(src, received.at[turn, j], pair_send.at[turn], pair_recv.at[turn, j], partner)

    def fold_copy(turn, j, to, target):
        src, dst = sent.at[turn, j, to], folded_in.at[turn, j, chip]
        return remote(src, dst, fold_send.at[turn], fold_recv.at[turn, j], target)

    other_chips = pl.ds(0, chips - 1)

    def term_copy(turn, to, target):
        src, dst = sent_terms.at[turn, to], terms_in.at[turn, chip]
        return remote(src, dst, term_send.at[turn], term_recv.at[turn], target)

    def filtered_sum(turn, low, terms, span, settle):
        scalars = in_lanes(terms, plan.columns)
        sent_terms[turn] = pieces(scalars).reshape(chips, GROUP, LANES).astype(jnp.bfloat16)
        terms_in[turn, chip] = sent_terms[turn, chip]
        for to, target in targets:
            term_copy(turn, to, target).start()

        def partial(at):
            value = product(low, turned_block[at, span], NN)
            return value + sums[turn, at] if turn == 0 else value

        def give(j):
            at = outward(j, 1 - core)
            sums[turn, at] = partial(at)
            pair_copy(turn, j).start()

        def keep(j):
            value = partial(outward(j, core))
            pair_copy(turn, j).wait_recv()
            value = (value + received[turn, j]).reshape(chips, GROUP, rows)
            total[j] = value
            sent[turn, j] = value.astype(jnp.bfloat16)
            for to, target in targets:
                fold_copy(turn, j, to, target).start()

        def both(j, carry):
            give(j + 2)
            keep(j)
            return carry

        give(0)
        give(1)
        lax.fori_loop(0, half_slabs - 2, both, 0)
        keep(half_slabs - 2)
        keep(half_slabs - 1)

        def added(values):
            return jnp.sum(values.astype(jnp.float32), 0)

        all_of(terms_in.at[turn, other_chips], term_send.at[turn], term_recv.at[turn]).wait_recv()
        whole[turn, core] = added(terms_in[turn])
        mine, theirs = whole.at[turn, core], whole.at[turn, 1 - core]
        remote(mine, mine, whole_send.at[turn], whole_recv.at[turn], partner).start()
        remote(theirs, theirs, whole_send.at[turn], whole_recv.at[turn], partner).wait_recv()
        scalars = whole[turn, 0] + whole[turn, 1]
        scalars = [joined(scalars, at) for at in range(len(terms))]
        ratio, more = settle(scalars)

        per_slab = rows // LANES
        overlap = jnp.zeros((GROUP, LANES), jnp.float32)
        group = 0
        entering[turn, half_blocks + 1] = blank
        for j in range(half_slabs):
            all_of(folded_in.at[turn, j, other_chips], fold_send.at[turn], fold_recv.at[turn, j]).wait_recv()
            for at, value in enumerate(nearer(added(folded_in[turn, j]) + total[j, chip])):
                at = j * per_slab + at
                if ratio is not None:
                    value = value + ratio * first_values[0, at]
                first_values[turn, at] = value
                entering[turn, at + 1] = weights[at] * value
            if j == 0:
                middle_copy(turn, 1).start()
                continue
            if j == 1:
                middle_copy(turn, 0).wait_recv()
            begin, end = plan.groups[group]
            count = end - begin

            def rows_of(ref):
                return ref.reshape(count * GROUP, LANES)

            here = rows_of(entering[turn, begin + 1:end + 1])
            outer = product(rows_of(entering[turn, begin:end]), inside_block, NN, exact)
            outer = outer + product(rows_of(entering[turn, begin + 2:end + 2]), outside_block, NN, exact)
            if end == half_blocks:
                kept = jnp.concatenate([
                    product(here[:-GROUP], same_block, NN, exact), product(here[-GROUP:], ends_block, NN, exact)
                ], 0)
            else:
                kept = product(here, same_block, NN, exact)
            kept = (rows_of(weights[begin:end]) * (outer + kept)).astype(jnp.bfloat16).astype(jnp.float32)
            with_values = rows_of(first_values[turn, begin:end]) * kept
            overlap = overlap + jnp.sum(with_values.reshape(count, GROUP, LANES), 0)
            parts = [kept[at * GROUP:(at + 1) * GROUP] for at in range(count)]
            if end == half_blocks:
                parts.append(pieces(in_lanes([over(overlap)] + more, GROUP)))
            gathered[turn, group, core, chip, :, :len(parts) * LANES] = jnp.concatenate(parts, 1).astype(jnp.bfloat16)
            for _, target in targets:
                gather_copy(turn, group, target).start()
            group += 1
        for group in range(len(plan.groups)):
            everyone = gathered.at[turn, group, core, other_chips, :, pl.ds(0, extent(group))]
            all_of(everyone, gather_send.at[turn, group], gather_recv.at[turn, group]).wait_recv()
            relay_copy(turn, group, core).start()
        for group, (begin, end) in enumerate(plan.groups):
            relay_copy(turn, group, 1 - core).wait_recv()
            for half in range(2):
                for at in range(begin, end):
                    part = gathered[turn, group, half, :, :, (at - begin) * LANES:(at - begin + 1) * LANES]
                    part = part.astype(jnp.float32).reshape(plan.columns, LANES).astype(jnp.bfloat16)
                    low = (half_blocks + at if half else half_blocks - 1 - at) * LANES
                    filtered[:, low:low + LANES] = part
        last = len(plan.groups) - 1
        span = slice(extent(last) - LANES, extent(last))
        first_terms, second_terms = [
            gathered[turn, last, half, :, :, span].astype(jnp.float32).reshape(plan.columns, LANES) for half in range(2)
        ]
        norm, ridge = joined(first_terms, 1), joined(first_terms, 2)
        step_col = norm / (ridge + joined(first_terms, 0) + joined(second_terms, 0))
        return scalars, ratio, step_col, joined(first_terms, 3)

    def extent(group):
        begin, end = plan.groups[group]
        return LANES * (end - begin + (end == half_blocks))

    def middle_copy(turn, at):
        src, dst = entering.at[turn, 1], entering.at[turn, 0]
        return remote(src if at else dst, dst, middle_send.at[turn], middle_recv.at[turn], partner)

    def gather_copy(turn, group, target):
        here = gathered.at[turn, group, core, chip, :, pl.ds(0, extent(group))]
        return remote(here, here, gather_send.at[turn, group], gather_recv.at[turn, group], target)

    def relay_copy(turn, group, which):
        here = gathered.at[turn, group, which, :, :, pl.ds(0, extent(group))]
        return remote(here, here, relay_send.at[turn, group], relay_recv.at[turn, group], partner)

    chunks = [slice(low, min(low + 2 * LANES, plan.width)) for low in range(0, plan.width, 2 * LANES)]

    def transposed(span):
        part = block[:, :, span]
        return product(filtered[...], part.reshape(slabs * rows, part.shape[2]), NN)

    ridged = ridge_row * direc[...]
    terms = [over(resid[...] * direc[...]), over(ridged * direc[...])]
    low = direc[:, spans[1]].astype(jnp.bfloat16)
    (norm, ridge), _, step_col, _ = filtered_sum(0, low, terms, spans[1], lambda sums_of: (None, list(sums_of)))
    terms = [0.0, 0.0, 0.0]
    for span in chunks:
        along, ridge_part = direc[:, span], ridge_row[:, span]
        left = resid[:, span] - step_col * (transposed(span) + ridge_part * along)
        ahead = scale_row[:, span] * left
        resid[:, span] = left
        solut[:, span] = step_col * along
        scal[:, span] = ahead
        ridged = ridge_part * ahead
        added = (over(left * ahead), over(ridged * ahead), over(ridged * along))
        terms = [term + more for term, more in zip(terms, added)]

    def settle(sums_of):
        norm_next, own_ridge, cross = sums_of
        ratio = norm_next / norm
        return ratio, [norm_next, own_ridge + ratio * (2.0 * cross + ratio * ridge), ratio]

    low = scal[...].astype(jnp.bfloat16)
    _, _, step_col, ratio_col = filtered_sum(1, low, terms, slice(0, plan.width), settle)

    def put(out, tile, value):
        out[(tile + 1) * LANES:(tile + 2) * LANES, :] = value

    held = {}
    for span in chunks:
        along = scal[:, span] + ratio_col * direc[:, span]
        ahead = solut[:, span] + step_col * along
        left = resid[:, span] - step_col * (transposed(span) + ridge_row[:, span] * along)
        for low in range(0, span.stop - span.start, LANES):
            held[(span.start + low) // LANES] = (ahead[:, low:low + LANES].T, left[:, low:low + LANES].T)
        for tile in [tile for tile in held if tile < plan.full]:
            new_ahead, new_left = held.pop(tile)
            put(solution_out, tile, new_ahead)
            put(residual_out, tile, new_left)
    mixed, last = held[plan.full], held[plan.full + 1]
    for out, edge, end in ((solution_out, mixed[0], last[0]), (residual_out, mixed[1], last[1])):
        out[:LANES, :] = edge
        put(out, plan.full, edge)
        low = pl.multiple_of((plan.full + 1) * LANES + offset, plan.rest)
        out[pl.ds(low, plan.rest), :] = end[:plan.rest]

    all_of(shown.at[others], show_send, show_recv).wait_send()
    all_of(seen_weight.at[others], weight_send, weight_recv).wait_send()
    for part, (low, size) in enumerate(((0, plan.cut), (plan.cut, plan.mixed_at - plan.cut), (plan.mixed_at, LANES))):
        all_of(block.at[others, :, pl.ds(low, size)], block_send.at[part], loose_recv).wait_send()
    all_of(loose.at[others], block_send.at[3], loose_recv).wait_send()
    all_of(early.at[core, near_others], early_send, early_recv).wait_send()
    all_of(early.at[core], early_relay_send, early_relay_recv).wait_send()
    for turn in range(2):
        all_of(received.at[turn], pair_send.at[turn], pair_recv.at[turn, 0]).wait_send()
        all_of(sent.at[turn, :, other_chips], fold_send.at[turn], fold_recv.at[turn, 0]).wait_send()
        all_of(sent_terms.at[turn, other_chips], term_send.at[turn], term_recv.at[turn]).wait_send()
        all_of(whole.at[turn, core], whole_send.at[turn], whole_recv.at[turn]).wait_send()
        middle_copy(turn, 1).wait_send()
        for group in range(len(plan.groups)):
            everyone = gathered.at[turn, group, core, other_chips, :, pl.ds(0, extent(group))]
            all_of(everyone, gather_send.at[turn, group], gather_recv.at[turn, group]).wait_send()
            relay_copy(turn, group, core).wait_send()


def far(value):
    return pltpu.with_memory_space_constraint(value, pltpu.HBM)


def fused_shards(design, observed, slab_counts, gap_mask, filter_taps, kaula_diag, precond):
    epoch_rows, coef_rows = design.shape
    columns = observed.shape[1]
    slabs, coefs = lax.axis_size("tm"), lax.axis_size("coef")
    plan = Plan(slabs, coefs, epoch_rows, coef_rows, columns)
    wide, chips, message = plan.width, plan.chips, plan.message
    half_slabs, half_chips = slabs // 2, chips // 2
    f32, bf16 = jnp.float32, jnp.bfloat16
    vmem = pl.BlockSpec(memory_space=pltpu.VMEM)
    hbm = pl.BlockSpec(memory_space=pltpu.HBM)
    sem = pltpu.SemaphoreType.DMA
    shape = jax.ShapeDtypeStruct((wide + LANES, columns), f32)
    tiles = (plan.tiles, LANES)
    outs = pl.pallas_call(
        functools.partial(fused, plan),
        out_shape=(shape, shape),
        in_specs=[hbm, hbm, hbm, pl.BlockSpec(memory_space=pltpu.SMEM), hbm, hbm, hbm],
        out_specs=(vmem, vmem),
        scratch_shapes=[
            pltpu.VMEM((epoch_rows, columns), f32),
            pltpu.VMEM((epoch_rows // LANES, LANES), jnp.int32),
            pltpu.VMEM((1, LANES), f32),
            pltpu.VMEM(tiles, f32),
            pltpu.VMEM(tiles, f32),
            pltpu.VMEM((slabs, epoch_rows, wide), bf16),
            pltpu.VMEM((slabs, wide, epoch_rows), bf16),
            pltpu.VMEM((slabs, 2, epoch_rows, LANES), bf16),
            pltpu.VMEM((slabs, epoch_rows + plan.packed_rows, LANES), bf16),
            pltpu.VMEM((slabs, plan.packed_rows, LANES), bf16),
            pltpu.VMEM((chips, GROUP, epoch_rows), f32),
            pltpu.VMEM((slabs, GROUP, epoch_rows), f32),
            pltpu.VMEM((slabs, epoch_rows // LANES, LANES), f32),
            pltpu.VMEM((2, half_chips, GROUP, slabs * epoch_rows), bf16),
            pltpu.VMEM((2, slabs, columns, epoch_rows), f32),
            pltpu.VMEM((2, half_slabs, columns, epoch_rows), f32),
            pltpu.VMEM((half_slabs, chips, GROUP, epoch_rows), f32),
            pltpu.VMEM((2, half_slabs, chips, GROUP, epoch_rows), bf16),
            pltpu.VMEM((2, half_slabs, chips, GROUP, epoch_rows), bf16),
            pltpu.VMEM((2, chips, GROUP, LANES), bf16),
            pltpu.VMEM((2, chips, GROUP, LANES), bf16),
            pltpu.VMEM((2, 2, GROUP, LANES), f32),
            pltpu.VMEM((2, plan.half_blocks + 2, GROUP, LANES), f32),
            pltpu.VMEM((plan.half_blocks, GROUP, LANES), f32),
            pltpu.VMEM((columns, slabs * epoch_rows), bf16),
            pltpu.VMEM((2, len(plan.groups), 2, chips, GROUP, message), bf16),
            pltpu.VMEM((columns, wide), f32),
            pltpu.VMEM((columns, wide), f32),
            pltpu.VMEM((columns, wide), f32),
            pltpu.VMEM((columns, wide), f32),
            pltpu.VMEM((2, plan.half_blocks, GROUP, LANES), f32),
            sem(()), sem((5,)), sem(()), sem((4,)), sem((2, slabs)), *[sem(())] * 5,
            sem(()), sem(()), sem(()), sem(()),
            sem((2,)), sem((2, half_slabs)), sem((2,)), sem((2, half_slabs)), sem((2,)), sem((2,)), sem((2,)), sem((2,)),
            sem((2,)), sem((2,)), *[sem((2, len(plan.groups)))] * 4,
        ],
        compiler_params=pltpu.CompilerParams(
            collective_id=0, has_side_effects=True, vmem_limit_bytes=48 * 1024 * 1024
        ),
    )(
        design, far(observed), far(gap_mask.reshape(-1, LANES)), slab_counts, far(filter_taps[None]),
        far(kaula_diag.reshape(tiles)), far(precond.reshape(tiles)),
    )
    owner = lax.axis_index("tm")
    low = owner * plan.owned - plan.first_tile(owner) * LANES
    return tuple(lax.dynamic_slice_in_dim(out, low, plan.owned, 0) for out in outs)


def shards(*arrays):
    design, observed, filter_taps = arrays[0], arrays[1], arrays[4]
    sizes = (lax.axis_size("tm"), lax.axis_size("coef"), *design.shape, observed.shape[1], filter_taps.shape[0])
    return fused_shards(*arrays) if fits(*sizes) else general_shards(*arrays)


def solution(mesh):
    placed = (P("tm", "coef"), P("tm", None), P("tm"), P("tm"), P(), P("coef"), P("coef"))
    return jax.shard_map(
        shards,
        mesh=mesh,
        in_specs=placed,
        out_specs=(P(("coef", "tm"), None), P(("coef", "tm"), None)),
        check_vma=False,
    )
```

```python
import functools

import jax
import jax.numpy as jnp
from jax import lax
from jax.experimental import pallas as pl
from jax.experimental.pallas import tpu as pltpu
from jax.sharding import PartitionSpec as P

ITERS = 2
HIGHEST = lax.Precision.HIGHEST


def toeplitz(pattern, band_len):
    tiled = jnp.tile(pattern, band_len)[: band_len * (2 * band_len - 1)]
    return tiled.reshape(band_len, 2 * band_len - 1)[:, :band_len]


def block_pair(filter_taps):
    band_len = filter_taps.shape[0]
    spacer = jnp.zeros((band_len,), jnp.float32)
    reversed_taps = filter_taps[:0:-1]
    lower = jnp.concatenate([filter_taps[:1], spacer, reversed_taps])
    upper = jnp.concatenate([jnp.zeros((1,), jnp.float32), reversed_taps, spacer])
    return (toeplitz(lower, band_len), toeplitz(upper, band_len))


def forward(values, lower_block, upper_block):
    band_len = lower_block.shape[0]
    blocks = values.reshape(-1, band_len, values.shape[1])
    previous = jnp.concatenate([jnp.zeros_like(blocks[:1]), blocks[:-1]], 0)
    result = jnp.einsum("ij,bjr->bir", lower_block, blocks, precision=HIGHEST)
    result = result + jnp.einsum("ij,bjr->bir", upper_block, previous, precision=HIGHEST)
    return result.reshape(values.shape)


def backward(values, lower_block, upper_block):
    band_len = lower_block.shape[0]
    blocks = values.reshape(-1, band_len, values.shape[1])
    following = jnp.concatenate([blocks[1:], jnp.zeros_like(blocks[:1])], 0)
    result = jnp.einsum("ji,bjr->bir", lower_block, blocks, precision=HIGHEST)
    result = result + jnp.einsum("ji,bjr->bir", upper_block, following, precision=HIGHEST)
    return result.reshape(values.shape)


def general_shards(design, observed, slab_counts, gap_mask, filter_taps, kaula_diag, precond):
    epoch_rows, coef_rows = design.shape
    columns = observed.shape[1]
    slabs = lax.axis_size("tm")
    epochs = slabs * epoch_rows
    owned_rows = coef_rows // slabs
    owner_index = lax.axis_index("tm")
    lower_block, upper_block = block_pair(filter_taps)
    position = jnp.arange(epoch_rows, dtype=jnp.int32)
    local_weight = ((gap_mask == 1) & (position < slab_counts[0])).astype(jnp.float32)
    packed = jnp.concatenate([observed, local_weight.reshape(-1, columns)], 0)
    gathered = lax.all_gather(packed, "tm", axis=0, tiled=False)
    all_observed = gathered[:, :epoch_rows].reshape(epochs, columns)
    weight = gathered[:, epoch_rows:].reshape(epochs, 1)
    block = lax.all_to_all(design, "tm", split_axis=1, concat_axis=0, tiled=True)

    def weighted(values):
        inner = forward(weight * values, lower_block, upper_block)
        return (weight * backward(inner, lower_block, upper_block)).astype(jnp.bfloat16)

    def transposed(filtered):
        return lax.dot_general(
            block, filtered, (((0,), (0,)), ((), ())), preferred_element_type=jnp.float32
        )

    def summed(scaled, terms):
        partial = jnp.dot(block, scaled.astype(jnp.bfloat16), preferred_element_type=jnp.float32)
        rows = [jnp.sum(term, 0)[None] for term in terms]
        rows.append(jnp.zeros((8 - len(rows), columns), jnp.float32))
        total = lax.psum(jnp.concatenate([partial] + rows, 0), ("tm", "coef"))
        return total[:epochs], [total[epochs + at] for at in range(len(terms))]

    start = owner_index * owned_rows
    kaula_col = lax.dynamic_slice_in_dim(kaula_diag, start, owned_rows, 0)[:, None]
    precond_col = lax.dynamic_slice_in_dim(precond, start, owned_rows, 0)[:, None]
    residual = transposed(weighted(all_observed))
    solution = jnp.zeros_like(residual)
    for iteration in range(ITERS):
        scaled = precond_col * residual
        terms = [residual * scaled, kaula_col * scaled * scaled]
        if iteration == 0:
            slab_values, (norm_now, ridge) = summed(scaled, terms)
            direction = scaled
        else:
            terms.append(kaula_col * scaled * direction)
            fresh, (norm_next, own_ridge, cross) = summed(scaled, terms)
            ratio = norm_next / norm_now
            slab_values = fresh + ratio * slab_values
            ridge = own_ridge + ratio * (2.0 * cross + ratio * ridge)
            direction = scaled + ratio * direction
            norm_now = norm_next
        filtered = weighted(slab_values)
        curvature = ridge + jnp.sum(slab_values * filtered.astype(jnp.float32), 0)
        step_len = norm_now / curvature
        image = transposed(filtered) + kaula_col * direction
        solution = solution + step_len * direction
        residual = residual - step_len * image
    return (solution, residual)


LANES = 128
GROUP = 8
MESH = pl.DeviceIdType.MESH
NN = ((1,), (0,))
NT = ((1,), (1,))


class Plan:
    def __init__(self, slabs, coefs, epoch_rows, coef_rows, columns):
        self.slabs, self.coefs, self.epoch_rows, self.columns = slabs, coefs, epoch_rows, columns
        self.tiles = coef_rows // LANES
        self.owned = coef_rows // slabs
        self.full = self.owned // LANES - 1
        self.rest = self.owned % LANES
        self.packed_rows = epoch_rows * self.rest // LANES
        self.mixed_at = self.full * LANES
        self.width = (self.full + 2) * LANES
        self.cut = (self.full - 1) * LANES
        self.across = coefs // 2
        self.chips = slabs * self.across
        self.blocks = slabs * epoch_rows // LANES
        self.half_blocks = self.blocks // 2
        per_slab, half_slabs = epoch_rows // LANES, slabs // 2
        ends = [(upto + 1) * per_slab - 1 for upto in range(1, half_slabs - 1)] + [self.half_blocks]
        self.groups = list(zip([0] + ends[:-1], ends))
        self.inner = (self.half_blocks - self.groups[-1][0], self.half_blocks + self.groups[-1][0])
        self.message = LANES * (1 + max(end - begin for begin, end in self.groups))

    def first_tile(self, owner):
        return lax.div(owner * self.owned, LANES)


def fits(slabs, coefs, epoch_rows, coef_rows, columns, taps):
    if slabs & (slabs - 1) or slabs < 4 or coefs % 2 or coefs & (coefs - 1) or epoch_rows % (2 * LANES) or coef_rows % LANES:
        return False
    if coef_rows % slabs or taps != LANES or columns != LANES or columns != GROUP * slabs * coefs // 2:
        return False
    owned = coef_rows // slabs
    rest = owned % LANES
    return owned >= 4 * LANES and rest >= 16 and LANES % rest == 0


def flips(index, count):
    steps, weight = [], 1
    while weight < count:
        steps.append(weight * (1 - 2 * lax.rem(lax.div(index, weight), 2)))
        weight *= 2
    return [sum((step for at, step in enumerate(steps) if bits >> at & 1), index) for bits in range(count)]


def pieces(values):
    high = values.astype(jnp.bfloat16).astype(jnp.float32)
    left = values - high
    middle = left.astype(jnp.bfloat16).astype(jnp.float32)
    low = (left - middle).astype(jnp.bfloat16).astype(jnp.float32)
    return high + pltpu.roll(middle, 8, 1) + pltpu.roll(low, 16, 1)


def joined(values, at):
    lane = lax.broadcasted_iota(jnp.int32, values.shape, 1)
    taken = (lane % 8 == at) & (lane < 24)
    return jnp.sum(jnp.where(taken, values, 0.0), 1, keepdims=True)


def in_lanes(terms, rows):
    lane = lax.broadcasted_iota(jnp.int32, (rows, LANES), 1)
    result = jnp.zeros((rows, LANES), jnp.float32)
    for at, term in enumerate(terms):
        result = jnp.where(lane == at, term, result)
    return result


def product(left, right, contract, precision=None):
    return lax.dot_general(
        left, right, (contract, ((), ())), precision=precision, preferred_element_type=jnp.float32
    )


def fused(plan, design, observed_in, gap_in, counts, taps_in, kaula_in, precond_in, solution_out, residual_out,
          observed, gap, taps, kaula, precond,
          block, turned_block, edges, packed, loose, shown, seen, seen_weight, early, sums, received, total, sent, folded_in, sent_terms, terms_in,
          whole, entering, weights, filtered, gathered, resid, direc, scal, solut, image, first_values,
          own_sem, small_sem, edge_sem, block_send, block_recv, loose_recv, show_send, show_recv, weight_send, weight_recv, early_send, early_recv,
          early_relay_send, early_relay_recv, pair_send, pair_recv, fold_send, fold_recv, term_send, term_recv,
          whole_send, whole_recv, middle_send, middle_recv, gather_send, gather_recv, relay_send, relay_recv):
    slabs, chips, rows = plan.slabs, plan.chips, plan.epoch_rows
    half_slabs, half_chips, half_blocks = slabs // 2, chips // 2, plan.half_blocks
    slab, coef = lax.axis_index("tm"), lax.axis_index("coef")
    across, core = lax.div(coef, 2), lax.rem(coef, 2)
    chip = slab * plan.across + across
    near_chip = lax.rem(chip, half_chips)
    partner = {"tm": slab, "coef": 2 * across + 1 - core}

    peers, sides = flips(slab, slabs), flips(across, plan.across)
    targets = [
        (peers[bits] * plan.across + sides[side], {"tm": peers[bits], "coef": coef + 2 * (sides[side] - across)})
        for bits in reversed(range(slabs)) for side in reversed(range(plan.across)) if bits or side
    ]
    near_targets = targets[-(half_chips - 1):]

    def remote(src, dst, send, recv, target):
        return pltpu.make_async_remote_copy(
            src_ref=src, dst_ref=dst, send_sem=send, recv_sem=recv, device_id=target, device_id_type=MESH
        )

    barrier = pltpu.get_barrier_semaphore()
    for _, target in targets:
        pl.semaphore_signal(barrier, inc=1, device_id=target, device_id_type=MESH)
    pl.semaphore_signal(barrier, inc=1, device_id=partner, device_id_type=MESH)

    small = [
        pltpu.make_async_copy(src, dst, small_sem.at[at])
        for at, (src, dst) in enumerate(
            ((observed_in, observed), (gap_in, gap), (taps_in, taps), (kaula_in, kaula), (precond_in, precond))
        )
    ]
    for copy in small:
        copy.start()
    first = plan.first_tile(slab)
    offset = slab * plan.owned - first * LANES

    def tile_columns(tile, size):
        return pl.ds(pl.multiple_of(tile * LANES, LANES), size)

    own = pltpu.make_async_copy(
        design.at[:, tile_columns(first + 1, plan.mixed_at)], block.at[slab, :, pl.ds(0, plan.mixed_at)], own_sem
    )
    own.start()
    for owner in range(slabs):
        begin = owner * plan.owned // LANES
        for at, tile in enumerate((begin, begin + plan.full + 1)):
            pltpu.make_async_copy(
                design.at[:, pl.ds(tile * LANES, LANES)], edges.at[owner, at], edge_sem
            ).start()

    for copy in small[:3]:
        copy.wait()
    tall = rows // LANES
    place = lax.broadcasted_iota(jnp.int32, (tall, LANES), 0) * LANES + lax.broadcasted_iota(jnp.int32, (tall, LANES), 1)
    local_weight = jnp.where((gap[...] == 1) & (place < counts[0]), 1.0, 0.0)
    seen_weight[slab] = local_weight
    weight_row = jnp.concatenate([local_weight[at:at + 1] for at in range(tall)], 1)
    turned = observed[...].T * weight_row
    shown[...] = turned.reshape(chips, GROUP, rows)
    seen[slab] = shown[2 * near_chip + core]
    for turn in range(2):
        for j in range(half_slabs):
            folded_in[turn, j, chip] = jnp.zeros((GROUP, rows), jnp.bfloat16)

    def block_copy(bits, part):
        peer = peers[bits]
        tile = plan.first_tile(peer) + 1
        if part == 0:
            src, dst = design.at[:, tile_columns(tile, plan.cut)], block.at[slab, :, pl.ds(0, plan.cut)]
        elif part == 1:
            src = design.at[:, tile_columns(tile + plan.cut // LANES, plan.mixed_at - plan.cut)]
            dst = block.at[slab, :, pl.ds(plan.cut, plan.mixed_at - plan.cut)]
        elif part == 2:
            src, dst = packed.at[peer, pl.ds(0, rows)], block.at[slab, :, pl.ds(plan.mixed_at, LANES)]
        else:
            src, dst = packed.at[peer, pl.ds(rows, plan.packed_rows)], loose.at[slab]
        return remote(src, dst, block_send.at[part], loose_recv if part == 3 else block_recv.at[min(part, 1), slab], {"tm": peer, "coef": coef})

    def block_arrival(bits, part):
        peer = peers[bits]
        low, size = ((0, plan.cut), (plan.cut, plan.mixed_at + LANES - plan.cut))[part]
        dst = block.at[peer, :, pl.ds(low, size)]
        return remote(dst, dst, block_send.at[part], block_recv.at[part, peer], {"tm": peer, "coef": coef})

    def all_of(ref, send, recv):
        return remote(ref, ref, send, recv, partner)

    def show_copy(bits):
        peer = peers[bits]
        src = shown.at[2 * lax.rem(peer * plan.across + across, half_chips) + core]
        return remote(src, seen.at[slab], show_send, show_recv, {"tm": peer, "coef": coef})

    def weight_copy(bits):
        src = seen_weight.at[slab]
        return remote(src, src, weight_send, weight_recv, {"tm": peers[bits], "coef": coef})

    others = pl.ds(0, slabs - 1)
    pl.semaphore_wait(barrier, chips)
    for bits in range(1, slabs):
        show_copy(bits).start()
        weight_copy(bits).start()
    for bits in range(1, half_slabs):
        block_copy(bits, 0).start()
        block_copy(bits, 1).start()
    for bits in range(half_slabs, slabs):
        block_copy(bits, 0).start()

    pltpu.make_async_copy(edges, edges, edge_sem).wait()
    lane_row = lax.broadcasted_iota(jnp.int32, (1, LANES), 1)
    for owner in range(slabs):
        skip = owner * plan.owned % LANES
        ahead = edges[owner, 0].astype(jnp.float32)
        behind = edges[owner, 1].astype(jnp.float32)
        packed[owner, :rows] = jnp.where(lane_row >= skip, ahead, behind).astype(jnp.bfloat16)
        tight = jnp.zeros((plan.packed_rows, LANES), jnp.float32)
        for at in range(LANES // plan.rest):
            part = behind[at * plan.packed_rows:(at + 1) * plan.packed_rows]
            shift = (at * plan.rest - skip) % LANES
            part = pltpu.roll(part, shift, 1) if shift else part
            tight = jnp.where(lax.div(lane_row, plan.rest) == at, part, tight)
        packed[owner, rows:] = tight.astype(jnp.bfloat16)
    for bits in range(1, slabs):
        block_copy(bits, 2).start()
        block_copy(bits, 3).start()

    def unpack(at, tight):
        tight = tight.astype(jnp.float32)
        for piece in range(LANES // plan.rest):
            part = pltpu.roll(tight, LANES - piece * plan.rest, 1) if piece else tight
            part = jnp.where(lane_row < plan.rest, part, 0.0).astype(jnp.bfloat16)
            block[at, piece * plan.packed_rows:(piece + 1) * plan.packed_rows, plan.mixed_at + LANES:] = part

    block[slab, :, plan.mixed_at:plan.mixed_at + LANES] = packed[slab, :rows]
    unpack(slab, packed[slab, rows:])

    base = jnp.concatenate([taps[...], jnp.zeros((1, LANES), jnp.float32)], 1)
    shifted = pltpu.roll(jnp.broadcast_to(base, (LANES, 2 * LANES)), 0, 1, stride=1, stride_axis=0)
    lower, upper = shifted[:, :LANES], shifted[:, LANES:]
    blank = jnp.zeros((GROUP, LANES), jnp.float32)

    all_of(seen.at[others], show_send, show_recv).wait_recv()
    all_of(seen_weight.at[others], weight_send, weight_recv).wait_recv()

    def repeated(at, j):
        return jnp.broadcast_to(seen_weight[at, j:j + 1, :], (GROUP, LANES))

    weight = jnp.concatenate([repeated(at, j) for at in range(slabs) for j in range(tall)], 0)
    own_series = jnp.concatenate([seen[at, :, j * LANES:(j + 1) * LANES] for at in range(slabs) for j in range(tall)], 0)

    def weighted(values):
        entering = weight * values
        before = jnp.concatenate([blank, entering[:-GROUP]], 0)
        inner = product(entering, lower, NN, lax.Precision.HIGHEST) + product(before, upper, NN, lax.Precision.HIGHEST)
        after = jnp.concatenate([inner[GROUP:], blank], 0)
        outer = product(inner, lower, NT, lax.Precision.HIGHEST) + product(after, upper, NT, lax.Precision.HIGHEST)
        return (weight * outer).astype(jnp.bfloat16)

    def nearer(span):
        parts = [span[:, at * LANES:(at + 1) * LANES] for at in range(rows // LANES)]
        return [jnp.where(core == 0, left, right) for left, right in zip(parts[::-1], parts)]

    def outward(at, which):
        return which * (half_slabs + at) + (1 - which) * (half_slabs - 1 - at)

    for at in range(half_slabs):
        place_of = outward(at, core)
        wide = jnp.concatenate([repeated(place_of, j) for j in range(tall)], 1)
        for j, part in enumerate(nearer(wide)):
            weights[at * tall + j] = part
    exact = lax.Precision.HIGHEST
    ends_block = product(lower, lower, NT, exact)
    same_block = ends_block + product(upper, upper, NT, exact)
    before_block, after_block = product(upper, lower, NT, exact), product(lower, upper, NT, exact)
    inside_block = jnp.where(core == 0, after_block, before_block)
    outside_block = jnp.where(core == 0, before_block, after_block)
    ends_block = jnp.where(core == 0, same_block, ends_block)

    kept = weighted(own_series).astype(jnp.float32)
    for j in range(plan.blocks):
        early[core, near_chip, :, j * LANES:(j + 1) * LANES] = kept[j * GROUP:(j + 1) * GROUP].astype(jnp.bfloat16)
    here = early.at[core, near_chip]
    for _, target in near_targets:
        remote(here, here, early_send, early_recv, target).start()
    for bits in range(half_slabs, slabs):
        block_copy(bits, 1).start()

    small[3].wait()
    small[4].wait()

    def local_row(table):
        inside = [table[pl.ds(first + 1 + at, 1), :] for at in range(plan.full)]
        ahead, behind = table[pl.ds(first, 1), :], table[pl.ds(first + plan.full + 1, 1), :]
        moved = pltpu.roll(jnp.broadcast_to(behind, (GROUP, LANES)), lax.rem(LANES - offset, LANES), 1)[:1]
        mixed = jnp.where(lane_row >= offset, ahead, behind)
        return jnp.concatenate(inside + [mixed, jnp.where(lane_row < plan.rest, moved, 0.0)], 1)

    ridge_row, scale_row = local_row(kaula), local_row(precond)

    near_others = pl.ds(0, half_chips - 1)
    all_of(early.at[core, near_others], early_send, early_recv).wait_recv()
    mine, theirs = early.at[core], early.at[1 - core]
    remote(mine, mine, early_relay_send, early_relay_recv, partner).start()
    remote(theirs, theirs, early_relay_send, early_relay_recv, partner).wait_recv()
    for at in range(slabs):
        span = slice(at * rows, (at + 1) * rows)
        both = jnp.stack([early[0, :, :, span].astype(jnp.float32), early[1, :, :, span].astype(jnp.float32)], 1)
        filtered[:, span] = both.reshape(plan.columns, rows).astype(jnp.bfloat16)

    def series(at):
        return filtered[:, pl.ds(pl.multiple_of(at * rows, rows), rows)]

    def over(terms):
        return jnp.sum(terms, 1, keepdims=True)

    own.wait()
    spans = (slice(0, plan.cut), slice(plan.cut, plan.width))
    part_terms = []

    def turn_over(at, span):
        turned_block[at, span] = block[at, :, span].T

    for part, span in enumerate(spans):
        if part:
            all_of(loose.at[others], block_send.at[3], loose_recv).wait_recv()
        turn_over(slab, span)
        resid[:, span] = product(series(slab), block[slab, :, span], NN)
        for bits in range(1, slabs):
            peer = peers[bits]
            block_arrival(bits, part).wait_recv()
            if part:
                unpack(peer, loose[peer])
            turn_over(peer, span)
            resid[:, span] += product(series(peer), block[peer, :, span], NN)
        direc[:, span] = scale_row[:, span] * resid[:, span]
        if part == 0:
            low = direc[:, span].astype(jnp.bfloat16)

            def body(at, carry):
                sums[0, at] = product(low, turned_block[at, :plan.cut], NN)
                return carry

            lax.fori_loop(0, slabs, body, 0)
        ridged = ridge_row[:, span] * direc[:, span]
        part_terms.append((over(resid[:, span] * direc[:, span]), over(ridged * direc[:, span])))

    def pair_copy(turn, j):
        src = sums.at[turn, outward(j, 1 - core)]
        return remote(src, received.at[turn, j], pair_send.at[turn], pair_recv.at[turn, j], partner)

    def fold_copy(turn, j, to, target):
        src, dst = sent.at[turn, j, to], folded_in.at[turn, j, chip]
        return remote(src, dst, fold_send.at[turn], fold_recv.at[turn, j], target)

    other_chips = pl.ds(0, chips - 1)

    def term_copy(turn, to, target):
        src, dst = sent_terms.at[turn, to], terms_in.at[turn, chip]
        return remote(src, dst, term_send.at[turn], term_recv.at[turn], target)

    chunks = [slice(low, min(low + 2 * LANES, plan.width)) for low in range(0, plan.width, 2 * LANES)]

    def transposed(span, blocks):
        begin, end = blocks
        parts, at = [], begin
        while at < end:
            upto = min(end, (at // tall + 1) * tall)
            parts.append(block[at // tall, at % tall * LANES:(upto - at // tall * tall) * LANES, span])
            at = upto
        return product(filtered[:, begin * LANES:end * LANES], jnp.concatenate(parts, 0), NN)

    def transposed_rest(span):
        begin, end = plan.inner
        return image[:, span] + transposed(span, (0, begin)) + transposed(span, (end, plan.blocks))

    def filtered_sum(turn, low, terms, span, settle):
        def partial(at):
            value = product(low, turned_block[at, span], NN)
            return value + sums[turn, at] if turn == 0 else value

        def give(j):
            at = outward(j, 1 - core)
            sums[turn, at] = partial(at)
            pair_copy(turn, j).start()

        def keep(j):
            value = partial(outward(j, core))
            pair_copy(turn, j).wait_recv()
            value = (value + received[turn, j]).reshape(chips, GROUP, rows)
            total[j] = value
            sent[turn, j] = value.astype(jnp.bfloat16)
            for to, target in targets:
                fold_copy(turn, j, to, target).start()

        def both(j, carry):
            give(j + 2)
            keep(j)
            return carry

        give(0)
        give(1)
        scalars = in_lanes(terms, plan.columns)
        sent_terms[turn] = pieces(scalars).reshape(chips, GROUP, LANES).astype(jnp.bfloat16)
        terms_in[turn, chip] = sent_terms[turn, chip]
        for to, target in targets:
            term_copy(turn, to, target).start()
        lax.fori_loop(0, half_slabs - 2, both, 0)
        keep(half_slabs - 2)
        keep(half_slabs - 1)

        def added(values):
            return jnp.sum(values.astype(jnp.float32), 0)

        all_of(terms_in.at[turn, other_chips], term_send.at[turn], term_recv.at[turn]).wait_recv()
        whole[turn, core] = added(terms_in[turn])
        mine, theirs = whole.at[turn, core], whole.at[turn, 1 - core]
        remote(mine, mine, whole_send.at[turn], whole_recv.at[turn], partner).start()
        remote(theirs, theirs, whole_send.at[turn], whole_recv.at[turn], partner).wait_recv()
        scalars = whole[turn, 0] + whole[turn, 1]
        scalars = [joined(scalars, at) for at in range(len(terms))]
        ratio, more = settle(scalars)

        per_slab = rows // LANES
        overlap = jnp.zeros((GROUP, LANES), jnp.float32)
        group = 0
        entering[turn, half_blocks + 1] = blank
        for j in range(half_slabs):
            all_of(folded_in.at[turn, j, other_chips], fold_send.at[turn], fold_recv.at[turn, j]).wait_recv()
            for at, value in enumerate(nearer(added(folded_in[turn, j]) + total[j, chip])):
                at = j * per_slab + at
                if ratio is not None:
                    value = value + ratio * first_values[0, at]
                first_values[turn, at] = value
                entering[turn, at + 1] = weights[at] * value
            if j == 0:
                middle_copy(turn, 1).start()
                continue
            if j == 1:
                middle_copy(turn, 0).wait_recv()
            begin, end = plan.groups[group]
            count = end - begin

            def rows_of(ref):
                return ref.reshape(count * GROUP, LANES)

            here = rows_of(entering[turn, begin + 1:end + 1])
            outer = product(rows_of(entering[turn, begin:end]), inside_block, NN, exact)
            outer = outer + product(rows_of(entering[turn, begin + 2:end + 2]), outside_block, NN, exact)
            if end == half_blocks:
                kept = jnp.concatenate([
                    product(here[:-GROUP], same_block, NN, exact), product(here[-GROUP:], ends_block, NN, exact)
                ], 0)
            else:
                kept = product(here, same_block, NN, exact)
            kept = (rows_of(weights[begin:end]) * (outer + kept)).astype(jnp.bfloat16).astype(jnp.float32)
            with_values = rows_of(first_values[turn, begin:end]) * kept
            overlap = overlap + jnp.sum(with_values.reshape(count, GROUP, LANES), 0)
            parts = [kept[at * GROUP:(at + 1) * GROUP] for at in range(count)]
            if end == half_blocks:
                parts.append(pieces(in_lanes([over(overlap)] + more, GROUP)))
            gathered[turn, group, core, chip, :, :len(parts) * LANES] = jnp.concatenate(parts, 1).astype(jnp.bfloat16)
            for _, target in targets:
                gather_copy(turn, group, target).start()
            group += 1
        def unfold(group):
            begin, end = plan.groups[group]
            relay_copy(turn, group, 1 - core).wait_recv()
            for half in range(2):
                for at in range(begin, end):
                    part = gathered[turn, group, half, :, :, (at - begin) * LANES:(at - begin + 1) * LANES]
                    part = part.astype(jnp.float32).reshape(plan.columns, LANES).astype(jnp.bfloat16)
                    low = (half_blocks + at if half else half_blocks - 1 - at) * LANES
                    filtered[:, low:low + LANES] = part

        for group in range(len(plan.groups)):
            everyone = gathered.at[turn, group, core, other_chips, :, pl.ds(0, extent(group))]
            all_of(everyone, gather_send.at[turn, group], gather_recv.at[turn, group]).wait_recv()
            relay_copy(turn, group, core).start()
        for group in range(len(plan.groups) - 1):
            unfold(group)
        for span in chunks:
            image[:, span] = transposed(span, plan.inner)
        unfold(len(plan.groups) - 1)
        last = len(plan.groups) - 1
        span = slice(extent(last) - LANES, extent(last))
        first_terms, second_terms = [
            gathered[turn, last, half, :, :, span].astype(jnp.float32).reshape(plan.columns, LANES) for half in range(2)
        ]
        norm, ridge = joined(first_terms, 1), joined(first_terms, 2)
        step_col = norm / (ridge + joined(first_terms, 0) + joined(second_terms, 0))
        return scalars, ratio, step_col, joined(first_terms, 3)

    def extent(group):
        begin, end = plan.groups[group]
        return LANES * (end - begin + (end == half_blocks))

    def middle_copy(turn, at):
        src, dst = entering.at[turn, 1], entering.at[turn, 0]
        return remote(src if at else dst, dst, middle_send.at[turn], middle_recv.at[turn], partner)

    def gather_copy(turn, group, target):
        here = gathered.at[turn, group, core, chip, :, pl.ds(0, extent(group))]
        return remote(here, here, gather_send.at[turn, group], gather_recv.at[turn, group], target)

    def relay_copy(turn, group, which):
        here = gathered.at[turn, group, which, :, :, pl.ds(0, extent(group))]
        return remote(here, here, relay_send.at[turn, group], relay_recv.at[turn, group], partner)

    terms = [left + right for left, right in zip(*part_terms)]
    low = direc[:, spans[1]].astype(jnp.bfloat16)
    (norm, ridge), _, step_col, _ = filtered_sum(0, low, terms, spans[1], lambda sums_of: (None, list(sums_of)))
    terms = [0.0, 0.0, 0.0]
    for span in chunks:
        along, ridge_part = direc[:, span], ridge_row[:, span]
        left = resid[:, span] - step_col * (transposed_rest(span) + ridge_part * along)
        ahead = scale_row[:, span] * left
        resid[:, span] = left
        solut[:, span] = step_col * along
        scal[:, span] = ahead
        ridged = ridge_part * ahead
        added = (over(left * ahead), over(ridged * ahead), over(ridged * along))
        terms = [term + more for term, more in zip(terms, added)]

    def settle(sums_of):
        norm_next, own_ridge, cross = sums_of
        ratio = norm_next / norm
        return ratio, [norm_next, own_ridge + ratio * (2.0 * cross + ratio * ridge), ratio]

    low = scal[...].astype(jnp.bfloat16)
    _, _, step_col, ratio_col = filtered_sum(1, low, terms, slice(0, plan.width), settle)

    def put(out, tile, value):
        out[(tile + 1) * LANES:(tile + 2) * LANES, :] = value

    held = {}
    for span in chunks:
        along = scal[:, span] + ratio_col * direc[:, span]
        ahead = solut[:, span] + step_col * along
        left = resid[:, span] - step_col * (transposed_rest(span) + ridge_row[:, span] * along)
        for low in range(0, span.stop - span.start, LANES):
            held[(span.start + low) // LANES] = (ahead[:, low:low + LANES].T, left[:, low:low + LANES].T)
        for tile in [tile for tile in held if tile < plan.full]:
            new_ahead, new_left = held.pop(tile)
            put(solution_out, tile, new_ahead)
            put(residual_out, tile, new_left)
    mixed, last = held[plan.full], held[plan.full + 1]
    for out, edge, end in ((solution_out, mixed[0], last[0]), (residual_out, mixed[1], last[1])):
        out[:LANES, :] = edge
        put(out, plan.full, edge)
        low = pl.multiple_of((plan.full + 1) * LANES + offset, plan.rest)
        out[pl.ds(low, plan.rest), :] = end[:plan.rest]

    all_of(shown.at[others], show_send, show_recv).wait_send()
    all_of(seen_weight.at[others], weight_send, weight_recv).wait_send()
    for part, (low, size) in enumerate(((0, plan.cut), (plan.cut, plan.mixed_at - plan.cut), (plan.mixed_at, LANES))):
        all_of(block.at[others, :, pl.ds(low, size)], block_send.at[part], loose_recv).wait_send()
    all_of(loose.at[others], block_send.at[3], loose_recv).wait_send()
    all_of(early.at[core, near_others], early_send, early_recv).wait_send()
    all_of(early.at[core], early_relay_send, early_relay_recv).wait_send()
    for turn in range(2):
        all_of(received.at[turn], pair_send.at[turn], pair_recv.at[turn, 0]).wait_send()
        all_of(sent.at[turn, :, other_chips], fold_send.at[turn], fold_recv.at[turn, 0]).wait_send()
        all_of(sent_terms.at[turn, other_chips], term_send.at[turn], term_recv.at[turn]).wait_send()
        all_of(whole.at[turn, core], whole_send.at[turn], whole_recv.at[turn]).wait_send()
        middle_copy(turn, 1).wait_send()
        for group in range(len(plan.groups)):
            everyone = gathered.at[turn, group, core, other_chips, :, pl.ds(0, extent(group))]
            all_of(everyone, gather_send.at[turn, group], gather_recv.at[turn, group]).wait_send()
            relay_copy(turn, group, core).wait_send()


def far(value):
    return pltpu.with_memory_space_constraint(value, pltpu.HBM)


def fused_shards(design, observed, slab_counts, gap_mask, filter_taps, kaula_diag, precond):
    epoch_rows, coef_rows = design.shape
    columns = observed.shape[1]
    slabs, coefs = lax.axis_size("tm"), lax.axis_size("coef")
    plan = Plan(slabs, coefs, epoch_rows, coef_rows, columns)
    wide, chips, message = plan.width, plan.chips, plan.message
    half_slabs, half_chips = slabs // 2, chips // 2
    f32, bf16 = jnp.float32, jnp.bfloat16
    vmem = pl.BlockSpec(memory_space=pltpu.VMEM)
    hbm = pl.BlockSpec(memory_space=pltpu.HBM)
    sem = pltpu.SemaphoreType.DMA
    shape = jax.ShapeDtypeStruct((wide + LANES, columns), f32)
    tiles = (plan.tiles, LANES)
    outs = pl.pallas_call(
        functools.partial(fused, plan),
        out_shape=(shape, shape),
        in_specs=[hbm, hbm, hbm, pl.BlockSpec(memory_space=pltpu.SMEM), hbm, hbm, hbm],
        out_specs=(vmem, vmem),
        scratch_shapes=[
            pltpu.VMEM((epoch_rows, columns), f32),
            pltpu.VMEM((epoch_rows // LANES, LANES), jnp.int32),
            pltpu.VMEM((1, LANES), f32),
            pltpu.VMEM(tiles, f32),
            pltpu.VMEM(tiles, f32),
            pltpu.VMEM((slabs, epoch_rows, wide), bf16),
            pltpu.VMEM((slabs, wide, epoch_rows), bf16),
            pltpu.VMEM((slabs, 2, epoch_rows, LANES), bf16),
            pltpu.VMEM((slabs, epoch_rows + plan.packed_rows, LANES), bf16),
            pltpu.VMEM((slabs, plan.packed_rows, LANES), bf16),
            pltpu.VMEM((chips, GROUP, epoch_rows), f32),
            pltpu.VMEM((slabs, GROUP, epoch_rows), f32),
            pltpu.VMEM((slabs, epoch_rows // LANES, LANES), f32),
            pltpu.VMEM((2, half_chips, GROUP, slabs * epoch_rows), bf16),
            pltpu.VMEM((2, slabs, columns, epoch_rows), f32),
            pltpu.VMEM((2, half_slabs, columns, epoch_rows), f32),
            pltpu.VMEM((half_slabs, chips, GROUP, epoch_rows), f32),
            pltpu.VMEM((2, half_slabs, chips, GROUP, epoch_rows), bf16),
            pltpu.VMEM((2, half_slabs, chips, GROUP, epoch_rows), bf16),
            pltpu.VMEM((2, chips, GROUP, LANES), bf16),
            pltpu.VMEM((2, chips, GROUP, LANES), bf16),
            pltpu.VMEM((2, 2, GROUP, LANES), f32),
            pltpu.VMEM((2, plan.half_blocks + 2, GROUP, LANES), f32),
            pltpu.VMEM((plan.half_blocks, GROUP, LANES), f32),
            pltpu.VMEM((columns, slabs * epoch_rows), bf16),
            pltpu.VMEM((2, len(plan.groups), 2, chips, GROUP, message), bf16),
            pltpu.VMEM((columns, wide), f32),
            pltpu.VMEM((columns, wide), f32),
            pltpu.VMEM((columns, wide), f32),
            pltpu.VMEM((columns, wide), f32),
            pltpu.VMEM((columns, wide), f32),
            pltpu.VMEM((2, plan.half_blocks, GROUP, LANES), f32),
            sem(()), sem((5,)), sem(()), sem((4,)), sem((2, slabs)), *[sem(())] * 5,
            sem(()), sem(()), sem(()), sem(()),
            sem((2,)), sem((2, half_slabs)), sem((2,)), sem((2, half_slabs)), sem((2,)), sem((2,)), sem((2,)), sem((2,)),
            sem((2,)), sem((2,)), *[sem((2, len(plan.groups)))] * 4,
        ],
        compiler_params=pltpu.CompilerParams(
            collective_id=0, has_side_effects=True, vmem_limit_bytes=48 * 1024 * 1024
        ),
    )(
        design, far(observed), far(gap_mask.reshape(-1, LANES)), slab_counts, far(filter_taps[None]),
        far(kaula_diag.reshape(tiles)), far(precond.reshape(tiles)),
    )
    owner = lax.axis_index("tm")
    low = owner * plan.owned - plan.first_tile(owner) * LANES
    return tuple(lax.dynamic_slice_in_dim(out, low, plan.owned, 0) for out in outs)


def shards(*arrays):
    design, observed, filter_taps = arrays[0], arrays[1], arrays[4]
    sizes = (lax.axis_size("tm"), lax.axis_size("coef"), *design.shape, observed.shape[1], filter_taps.shape[0])
    return fused_shards(*arrays) if fits(*sizes) else general_shards(*arrays)


def solution(mesh):
    placed = (P("tm", "coef"), P("tm", None), P("tm"), P("tm"), P(), P("coef"), P("coef"))
    return jax.shard_map(
        shards,
        mesh=mesh,
        in_specs=placed,
        out_specs=(P(("coef", "tm"), None), P(("coef", "tm"), None)),
        check_vma=False,
    )
```

```python
import functools

import jax
import jax.numpy as jnp
from jax import lax
from jax.experimental import pallas as pl
from jax.experimental.pallas import tpu as pltpu
from jax.sharding import PartitionSpec as P

ITERS = 2
HIGHEST = lax.Precision.HIGHEST


def toeplitz(pattern, band_len):
    tiled = jnp.tile(pattern, band_len)[: band_len * (2 * band_len - 1)]
    return tiled.reshape(band_len, 2 * band_len - 1)[:, :band_len]


def block_pair(filter_taps):
    band_len = filter_taps.shape[0]
    spacer = jnp.zeros((band_len,), jnp.float32)
    reversed_taps = filter_taps[:0:-1]
    lower = jnp.concatenate([filter_taps[:1], spacer, reversed_taps])
    upper = jnp.concatenate([jnp.zeros((1,), jnp.float32), reversed_taps, spacer])
    return (toeplitz(lower, band_len), toeplitz(upper, band_len))


def forward(values, lower_block, upper_block):
    band_len = lower_block.shape[0]
    blocks = values.reshape(-1, band_len, values.shape[1])
    previous = jnp.concatenate([jnp.zeros_like(blocks[:1]), blocks[:-1]], 0)
    result = jnp.einsum("ij,bjr->bir", lower_block, blocks, precision=HIGHEST)
    result = result + jnp.einsum("ij,bjr->bir", upper_block, previous, precision=HIGHEST)
    return result.reshape(values.shape)


def backward(values, lower_block, upper_block):
    band_len = lower_block.shape[0]
    blocks = values.reshape(-1, band_len, values.shape[1])
    following = jnp.concatenate([blocks[1:], jnp.zeros_like(blocks[:1])], 0)
    result = jnp.einsum("ji,bjr->bir", lower_block, blocks, precision=HIGHEST)
    result = result + jnp.einsum("ji,bjr->bir", upper_block, following, precision=HIGHEST)
    return result.reshape(values.shape)


def general_shards(design, observed, slab_counts, gap_mask, filter_taps, kaula_diag, precond):
    epoch_rows, coef_rows = design.shape
    columns = observed.shape[1]
    slabs = lax.axis_size("tm")
    epochs = slabs * epoch_rows
    owned_rows = coef_rows // slabs
    owner_index = lax.axis_index("tm")
    lower_block, upper_block = block_pair(filter_taps)
    position = jnp.arange(epoch_rows, dtype=jnp.int32)
    local_weight = ((gap_mask == 1) & (position < slab_counts[0])).astype(jnp.float32)
    packed = jnp.concatenate([observed, local_weight.reshape(-1, columns)], 0)
    gathered = lax.all_gather(packed, "tm", axis=0, tiled=False)
    all_observed = gathered[:, :epoch_rows].reshape(epochs, columns)
    weight = gathered[:, epoch_rows:].reshape(epochs, 1)
    block = lax.all_to_all(design, "tm", split_axis=1, concat_axis=0, tiled=True)

    def weighted(values):
        inner = forward(weight * values, lower_block, upper_block)
        return (weight * backward(inner, lower_block, upper_block)).astype(jnp.bfloat16)

    def transposed(filtered):
        return lax.dot_general(
            block, filtered, (((0,), (0,)), ((), ())), preferred_element_type=jnp.float32
        )

    def summed(scaled, terms):
        partial = jnp.dot(block, scaled.astype(jnp.bfloat16), preferred_element_type=jnp.float32)
        rows = [jnp.sum(term, 0)[None] for term in terms]
        rows.append(jnp.zeros((8 - len(rows), columns), jnp.float32))
        total = lax.psum(jnp.concatenate([partial] + rows, 0), ("tm", "coef"))
        return total[:epochs], [total[epochs + at] for at in range(len(terms))]

    start = owner_index * owned_rows
    kaula_col = lax.dynamic_slice_in_dim(kaula_diag, start, owned_rows, 0)[:, None]
    precond_col = lax.dynamic_slice_in_dim(precond, start, owned_rows, 0)[:, None]
    residual = transposed(weighted(all_observed))
    solution = jnp.zeros_like(residual)
    for iteration in range(ITERS):
        scaled = precond_col * residual
        terms = [residual * scaled, kaula_col * scaled * scaled]
        if iteration == 0:
            slab_values, (norm_now, ridge) = summed(scaled, terms)
            direction = scaled
        else:
            terms.append(kaula_col * scaled * direction)
            fresh, (norm_next, own_ridge, cross) = summed(scaled, terms)
            ratio = norm_next / norm_now
            slab_values = fresh + ratio * slab_values
            ridge = own_ridge + ratio * (2.0 * cross + ratio * ridge)
            direction = scaled + ratio * direction
            norm_now = norm_next
        filtered = weighted(slab_values)
        curvature = ridge + jnp.sum(slab_values * filtered.astype(jnp.float32), 0)
        step_len = norm_now / curvature
        image = transposed(filtered) + kaula_col * direction
        solution = solution + step_len * direction
        residual = residual - step_len * image
    return (solution, residual)


LANES = 128
GROUP = 8
PAIRED = 2 * GROUP
MESH = pl.DeviceIdType.MESH
NN = ((1,), (0,))
NT = ((1,), (1,))


class Plan:
    def __init__(self, slabs, coefs, epoch_rows, coef_rows, columns):
        self.slabs, self.coefs, self.epoch_rows, self.columns = slabs, coefs, epoch_rows, columns
        self.tiles = coef_rows // LANES
        self.owned = coef_rows // slabs
        self.full = self.owned // LANES - 1
        self.rest = self.owned % LANES
        self.packed_rows = epoch_rows * self.rest // LANES
        self.mixed_at = self.full * LANES
        self.width = (self.full + 2) * LANES
        self.cut = (self.full - 1) * LANES
        self.across = coefs // 2
        self.chips = slabs * self.across
        self.blocks = slabs * epoch_rows // LANES
        self.half_blocks = self.blocks // 2
        per_slab, half_slabs = epoch_rows // LANES, slabs // 2
        ends = [(upto + 1) * per_slab - 1 for upto in range(1, half_slabs - 1)] + [self.half_blocks]
        self.groups = list(zip([0] + ends[:-1], ends))
        self.inner = (self.half_blocks - self.groups[-1][0], self.half_blocks + self.groups[-1][0])
        self.message = LANES * (1 + max(end - begin for begin, end in self.groups))

    def first_tile(self, owner):
        return lax.div(owner * self.owned, LANES)


def fits(slabs, coefs, epoch_rows, coef_rows, columns, taps):
    if slabs & (slabs - 1) or slabs < 4 or coefs % 2 or coefs & (coefs - 1) or epoch_rows % (2 * LANES) or coef_rows % LANES:
        return False
    if coef_rows % slabs or taps != LANES or columns != LANES or columns != GROUP * slabs * coefs // 2:
        return False
    owned = coef_rows // slabs
    rest = owned % LANES
    return owned >= 4 * LANES and rest >= 16 and LANES % rest == 0


def flips(index, count):
    steps, weight = [], 1
    while weight < count:
        steps.append(weight * (1 - 2 * lax.rem(lax.div(index, weight), 2)))
        weight *= 2
    return [sum((step for at, step in enumerate(steps) if bits >> at & 1), index) for bits in range(count)]


def pieces(values):
    high = values.astype(jnp.bfloat16).astype(jnp.float32)
    left = values - high
    middle = left.astype(jnp.bfloat16).astype(jnp.float32)
    low = (left - middle).astype(jnp.bfloat16).astype(jnp.float32)
    return high + pltpu.roll(middle, 8, 1) + pltpu.roll(low, 16, 1)


def joined(values, at):
    lane = lax.broadcasted_iota(jnp.int32, values.shape, 1)
    taken = (lane % 8 == at) & (lane < 24)
    return jnp.sum(jnp.where(taken, values, 0.0), 1, keepdims=True)


def in_lanes(terms, rows):
    lane = lax.broadcasted_iota(jnp.int32, (rows, LANES), 1)
    result = jnp.zeros((rows, LANES), jnp.float32)
    for at, term in enumerate(terms):
        result = jnp.where(lane == at, term, result)
    return result


def product(left, right, contract, precision=None):
    return lax.dot_general(
        left, right, (contract, ((), ())), precision=precision, preferred_element_type=jnp.float32
    )


def fused(plan, design, observed_in, gap_in, counts, taps_in, kaula_in, precond_in, solution_out, residual_out,
          observed, gap, taps, kaula, precond,
          block, turned_block, edges, packed, loose, shown, seen, seen_weight, early, sums, received, total, sent, folded_in, sent_terms, terms_in,
          whole, whole_parts, crossed, entering, weights, filtered, gathered, resid, direc, scal, solut, image, first_values,
          own_sem, small_sem, edge_sem, block_send, block_recv, loose_recv, show_send, show_recv, weight_send, weight_recv, early_send, early_recv,
          early_relay_send, early_relay_recv, pair_send, pair_recv, fold_send, fold_recv, term_send, term_recv,
          whole_send, whole_recv, cross_send, cross_recv, middle_send, middle_recv, gather_send, gather_recv, relay_send, relay_recv):
    slabs, chips, rows = plan.slabs, plan.chips, plan.epoch_rows
    half_slabs, half_chips, half_blocks = slabs // 2, chips // 2, plan.half_blocks
    slab, coef = lax.axis_index("tm"), lax.axis_index("coef")
    across, core = lax.div(coef, 2), lax.rem(coef, 2)
    chip = slab * plan.across + across
    near_chip = lax.rem(chip, half_chips)
    partner = {"tm": slab, "coef": 2 * across + 1 - core}

    peers, sides = flips(slab, slabs), flips(across, plan.across)
    targets = [
        (peers[bits] * plan.across + sides[side], {"tm": peers[bits], "coef": coef + 2 * (sides[side] - across)})
        for bits in reversed(range(slabs)) for side in reversed(range(plan.across)) if bits or side
    ]
    near_targets = [
        (at - lax.div(slab, half_slabs) * half_chips, target) for at, target in targets[-(half_chips - 1):]
    ]
    this_half = lax.div(slab, half_slabs)
    mirror = {"tm": peers[half_slabs], "coef": coef}
    across_mirror = {"tm": peers[half_slabs], "coef": 2 * across + 1 - core}

    def remote(src, dst, send, recv, target):
        return pltpu.make_async_remote_copy(
            src_ref=src, dst_ref=dst, send_sem=send, recv_sem=recv, device_id=target, device_id_type=MESH
        )

    barrier = pltpu.get_barrier_semaphore()
    for _, target in targets:
        pl.semaphore_signal(barrier, inc=1, device_id=target, device_id_type=MESH)
    for target in (partner, across_mirror):
        pl.semaphore_signal(barrier, inc=1, device_id=target, device_id_type=MESH)

    small = [
        pltpu.make_async_copy(src, dst, small_sem.at[at])
        for at, (src, dst) in enumerate(
            ((observed_in, observed), (gap_in, gap), (taps_in, taps), (kaula_in, kaula), (precond_in, precond))
        )
    ]
    for copy in small:
        copy.start()
    first = plan.first_tile(slab)
    offset = slab * plan.owned - first * LANES

    def tile_columns(tile, size):
        return pl.ds(pl.multiple_of(tile * LANES, LANES), size)

    own = pltpu.make_async_copy(
        design.at[:, tile_columns(first + 1, plan.mixed_at)], block.at[slab, :, pl.ds(0, plan.mixed_at)], own_sem
    )
    own.start()
    for owner in range(slabs):
        begin = owner * plan.owned // LANES
        for at, tile in enumerate((begin, begin + plan.full + 1)):
            pltpu.make_async_copy(
                design.at[:, pl.ds(tile * LANES, LANES)], edges.at[owner, at], edge_sem
            ).start()

    for copy in small[:3]:
        copy.wait()
    tall = rows // LANES
    place = lax.broadcasted_iota(jnp.int32, (tall, LANES), 0) * LANES + lax.broadcasted_iota(jnp.int32, (tall, LANES), 1)
    local_weight = jnp.where((gap[...] == 1) & (place < counts[0]), 1.0, 0.0)
    seen_weight[slab] = local_weight
    weight_row = jnp.concatenate([local_weight[at:at + 1] for at in range(tall)], 1)
    turned = observed[...].T * weight_row
    shown[...] = turned.reshape(chips, GROUP, rows)
    seen[slab] = shown[2 * near_chip + core]
    for turn in range(2):
        for j in range(half_slabs):
            folded_in[turn, j, near_chip] = jnp.zeros((PAIRED, rows), jnp.bfloat16)

    def block_copy(bits, part):
        peer = peers[bits]
        tile = plan.first_tile(peer) + 1
        if part == 0:
            src, dst = design.at[:, tile_columns(tile, plan.cut)], block.at[slab, :, pl.ds(0, plan.cut)]
        elif part == 1:
            src = design.at[:, tile_columns(tile + plan.cut // LANES, plan.mixed_at - plan.cut)]
            dst = block.at[slab, :, pl.ds(plan.cut, plan.mixed_at - plan.cut)]
        elif part == 2:
            src, dst = packed.at[peer, pl.ds(0, rows)], block.at[slab, :, pl.ds(plan.mixed_at, LANES)]
        else:
            src, dst = packed.at[peer, pl.ds(rows, plan.packed_rows)], loose.at[slab]
        return remote(src, dst, block_send.at[part], loose_recv if part == 3 else block_recv.at[min(part, 1), slab], {"tm": peer, "coef": coef})

    def block_arrival(bits, part):
        peer = peers[bits]
        low, size = ((0, plan.cut), (plan.cut, plan.mixed_at + LANES - plan.cut))[part]
        dst = block.at[peer, :, pl.ds(low, size)]
        return remote(dst, dst, block_send.at[part], block_recv.at[part, peer], {"tm": peer, "coef": coef})

    def all_of(ref, send, recv):
        return remote(ref, ref, send, recv, partner)

    def show_copy(bits):
        peer = peers[bits]
        src = shown.at[2 * lax.rem(peer * plan.across + across, half_chips) + core]
        return remote(src, seen.at[slab], show_send, show_recv, {"tm": peer, "coef": coef})

    def weight_copy(bits):
        src = seen_weight.at[slab]
        return remote(src, src, weight_send, weight_recv, {"tm": peers[bits], "coef": coef})

    others = pl.ds(0, slabs - 1)
    pl.semaphore_wait(barrier, chips + 1)
    for bits in range(1, slabs):
        show_copy(bits).start()
        weight_copy(bits).start()
    for bits in range(1, half_slabs):
        block_copy(bits, 0).start()
        block_copy(bits, 1).start()
    for bits in range(half_slabs, slabs):
        block_copy(bits, 0).start()

    pltpu.make_async_copy(edges, edges, edge_sem).wait()
    lane_row = lax.broadcasted_iota(jnp.int32, (1, LANES), 1)
    for owner in range(slabs):
        skip = owner * plan.owned % LANES
        ahead = edges[owner, 0].astype(jnp.float32)
        behind = edges[owner, 1].astype(jnp.float32)
        packed[owner, :rows] = jnp.where(lane_row >= skip, ahead, behind).astype(jnp.bfloat16)
        tight = jnp.zeros((plan.packed_rows, LANES), jnp.float32)
        for at in range(LANES // plan.rest):
            part = behind[at * plan.packed_rows:(at + 1) * plan.packed_rows]
            shift = (at * plan.rest - skip) % LANES
            part = pltpu.roll(part, shift, 1) if shift else part
            tight = jnp.where(lax.div(lane_row, plan.rest) == at, part, tight)
        packed[owner, rows:] = tight.astype(jnp.bfloat16)
    for bits in range(1, slabs):
        block_copy(bits, 2).start()
        block_copy(bits, 3).start()

    def unpack(at, tight):
        tight = tight.astype(jnp.float32)
        for piece in range(LANES // plan.rest):
            part = pltpu.roll(tight, LANES - piece * plan.rest, 1) if piece else tight
            part = jnp.where(lane_row < plan.rest, part, 0.0).astype(jnp.bfloat16)
            block[at, piece * plan.packed_rows:(piece + 1) * plan.packed_rows, plan.mixed_at + LANES:] = part

    block[slab, :, plan.mixed_at:plan.mixed_at + LANES] = packed[slab, :rows]
    unpack(slab, packed[slab, rows:])

    base = jnp.concatenate([taps[...], jnp.zeros((1, LANES), jnp.float32)], 1)
    shifted = pltpu.roll(jnp.broadcast_to(base, (LANES, 2 * LANES)), 0, 1, stride=1, stride_axis=0)
    lower, upper = shifted[:, :LANES], shifted[:, LANES:]
    blank = jnp.zeros((GROUP, LANES), jnp.float32)

    all_of(seen.at[others], show_send, show_recv).wait_recv()
    all_of(seen_weight.at[others], weight_send, weight_recv).wait_recv()

    def repeated(at, j):
        return jnp.broadcast_to(seen_weight[at, j:j + 1, :], (GROUP, LANES))

    weight = jnp.concatenate([repeated(at, j) for at in range(slabs) for j in range(tall)], 0)
    own_series = jnp.concatenate([seen[at, :, j * LANES:(j + 1) * LANES] for at in range(slabs) for j in range(tall)], 0)

    def weighted(values):
        entering = weight * values
        before = jnp.concatenate([blank, entering[:-GROUP]], 0)
        inner = product(entering, lower, NN, lax.Precision.HIGHEST) + product(before, upper, NN, lax.Precision.HIGHEST)
        after = jnp.concatenate([inner[GROUP:], blank], 0)
        outer = product(inner, lower, NT, lax.Precision.HIGHEST) + product(after, upper, NT, lax.Precision.HIGHEST)
        return (weight * outer).astype(jnp.bfloat16)

    def nearer(span):
        parts = [span[:, at * LANES:(at + 1) * LANES] for at in range(rows // LANES)]
        return [jnp.where(core == 0, left, right) for left, right in zip(parts[::-1], parts)]

    def outward(at, which):
        return which * (half_slabs + at) + (1 - which) * (half_slabs - 1 - at)

    for at in range(half_slabs):
        place_of = outward(at, core)
        wide = jnp.concatenate([repeated(place_of, j) for j in range(tall)], 1)
        for j, part in enumerate(nearer(wide)):
            weights[at * tall + j] = jnp.concatenate([part, part], 0)
    exact = lax.Precision.HIGHEST
    ends_block = product(lower, lower, NT, exact)
    same_block = ends_block + product(upper, upper, NT, exact)
    before_block, after_block = product(upper, lower, NT, exact), product(lower, upper, NT, exact)
    inside_block = jnp.where(core == 0, after_block, before_block)
    outside_block = jnp.where(core == 0, before_block, after_block)
    ends_block = jnp.where(core == 0, same_block, ends_block)

    kept = weighted(own_series).astype(jnp.float32)
    for j in range(plan.blocks):
        early[core, near_chip, :, j * LANES:(j + 1) * LANES] = kept[j * GROUP:(j + 1) * GROUP].astype(jnp.bfloat16)
    here = early.at[core, near_chip]
    for _, target in near_targets:
        remote(here, here, early_send, early_recv, target).start()
    for bits in range(half_slabs, slabs):
        block_copy(bits, 1).start()

    small[3].wait()
    small[4].wait()

    def local_row(table):
        inside = [table[pl.ds(first + 1 + at, 1), :] for at in range(plan.full)]
        ahead, behind = table[pl.ds(first, 1), :], table[pl.ds(first + plan.full + 1, 1), :]
        moved = pltpu.roll(jnp.broadcast_to(behind, (GROUP, LANES)), lax.rem(LANES - offset, LANES), 1)[:1]
        mixed = jnp.where(lane_row >= offset, ahead, behind)
        return jnp.concatenate(inside + [mixed, jnp.where(lane_row < plan.rest, moved, 0.0)], 1)

    ridge_row, scale_row = local_row(kaula), local_row(precond)

    near_others = pl.ds(0, half_chips - 1)
    all_of(early.at[core, near_others], early_send, early_recv).wait_recv()
    mine, theirs = early.at[core], early.at[1 - core]
    remote(mine, mine, early_relay_send, early_relay_recv, partner).start()
    remote(theirs, theirs, early_relay_send, early_relay_recv, partner).wait_recv()
    for at in range(slabs):
        span = slice(at * rows, (at + 1) * rows)
        both = jnp.stack([early[0, :, :, span].astype(jnp.float32), early[1, :, :, span].astype(jnp.float32)], 1)
        filtered[:, span] = both.reshape(plan.columns, rows).astype(jnp.bfloat16)

    def series(at):
        return filtered[:, pl.ds(pl.multiple_of(at * rows, rows), rows)]

    def over(terms):
        return jnp.sum(terms, 1, keepdims=True)

    own.wait()
    spans = (slice(0, plan.cut), slice(plan.cut, plan.width))
    part_terms = []

    def turn_over(at, span):
        turned_block[at, span] = block[at, :, span].T

    for part, span in enumerate(spans):
        if part:
            all_of(loose.at[others], block_send.at[3], loose_recv).wait_recv()
        turn_over(slab, span)
        resid[:, span] = product(series(slab), block[slab, :, span], NN)
        for bits in range(1, slabs):
            peer = peers[bits]
            block_arrival(bits, part).wait_recv()
            if part:
                unpack(peer, loose[peer])
            turn_over(peer, span)
            resid[:, span] += product(series(peer), block[peer, :, span], NN)
        direc[:, span] = scale_row[:, span] * resid[:, span]
        if part == 0:
            low = direc[:, span].astype(jnp.bfloat16)

            def body(at, carry):
                sums[0, at] = product(low, turned_block[at, :plan.cut], NN)
                return carry

            lax.fori_loop(0, slabs, body, 0)
        ridged = ridge_row[:, span] * direc[:, span]
        part_terms.append((over(resid[:, span] * direc[:, span]), over(ridged * direc[:, span])))

    def pair_copy(turn, j):
        src = sums.at[turn, outward(j, 1 - core)]
        return remote(src, received.at[turn, j], pair_send.at[turn], pair_recv.at[turn, j], partner)

    def fold_copy(turn, j, to, target):
        src, dst = sent.at[turn, j, to], folded_in.at[turn, j, near_chip]
        return remote(src, dst, fold_send.at[turn], fold_recv.at[turn, j], target)

    def cross_copy(turn, j):
        here = crossed.at[turn, j, this_half]
        return remote(here, here, cross_send.at[turn], cross_recv.at[turn, j], mirror)

    def whole_copy(turn, target):
        here = whole.at[turn, this_half, core]
        return remote(here, here, whole_send.at[turn], whole_recv.at[turn], target)


    def term_copy(turn, to, target):
        src, dst = sent_terms.at[turn, to], terms_in.at[turn, near_chip]
        return remote(src, dst, term_send.at[turn], term_recv.at[turn], target)

    chunks = [slice(low, min(low + 2 * LANES, plan.width)) for low in range(0, plan.width, 2 * LANES)]

    def transposed(span, blocks):
        begin, end = blocks
        parts, at = [], begin
        while at < end:
            upto = min(end, (at // tall + 1) * tall)
            parts.append(block[at // tall, at % tall * LANES:(upto - at // tall * tall) * LANES, span])
            at = upto
        return product(filtered[:, begin * LANES:end * LANES], jnp.concatenate(parts, 0), NN)

    def transposed_rest(span):
        begin, end = plan.inner
        return image[:, span] + transposed(span, (0, begin)) + transposed(span, (end, plan.blocks))

    def filtered_sum(turn, low, terms, span, settle):
        def partial(at):
            value = product(low, turned_block[at, span], NN)
            return value + sums[turn, at] if turn == 0 else value

        def give(j):
            at = outward(j, 1 - core)
            sums[turn, at] = partial(at)
            pair_copy(turn, j).start()

        def keep(j):
            value = partial(outward(j, core))
            pair_copy(turn, j).wait_recv()
            value = (value + received[turn, j]).reshape(half_chips, PAIRED, rows)
            total[j] = value
            sent[turn, j] = value.astype(jnp.bfloat16)
            for to, target in near_targets:
                fold_copy(turn, j, to, target).start()

        def both(j, carry):
            give(j + 2)
            keep(j)
            return carry

        give(0)
        give(1)
        scalars = in_lanes(terms, plan.columns)
        sent_terms[turn] = pieces(scalars).reshape(half_chips, PAIRED, LANES).astype(jnp.bfloat16)
        terms_in[turn, near_chip] = sent_terms[turn, near_chip]
        for to, target in near_targets:
            term_copy(turn, to, target).start()
        lax.fori_loop(0, half_slabs - 2, both, 0)
        keep(half_slabs - 2)
        keep(half_slabs - 1)

        def added(values):
            return jnp.sum(values.astype(jnp.float32), 0)

        all_of(terms_in.at[turn, near_others], term_send.at[turn], term_recv.at[turn]).wait_recv()
        half_terms = added(terms_in[turn])
        half_terms = half_terms + pltpu.roll(half_terms, LANES - 8, 1) + pltpu.roll(half_terms, LANES - 16, 1)
        whole[turn, this_half, core] = half_terms
        for target in (mirror, across_mirror, partner):
            whole_copy(turn, target).start()
        for j in range(half_slabs):
            all_of(folded_in.at[turn, j, near_others], fold_send.at[turn], fold_recv.at[turn, j]).wait_recv()
            crossed[turn, j, this_half] = added(folded_in[turn, j]) + total[j, near_chip]
            cross_copy(turn, j).start()
        all_of(whole_parts.at[pl.ds(0, 3)], whole_send.at[turn], whole_recv.at[turn]).wait_recv()
        scalars = (whole[turn, 0, 0] + whole[turn, 0, 1]) + (whole[turn, 1, 0] + whole[turn, 1, 1])
        scalars = [scalars[:, at:at + 1] for at in range(len(terms))]
        ratio, more = settle(scalars)

        per_slab = rows // LANES
        overlap = jnp.zeros((PAIRED, LANES), jnp.float32)
        group = 0
        entering[turn, half_blocks + 1] = jnp.zeros((PAIRED, LANES), jnp.float32)
        for j in range(half_slabs):
            theirs = crossed.at[turn, j, 1 - this_half]
            remote(theirs, theirs, cross_send.at[turn], cross_recv.at[turn, j], mirror).wait_recv()
            for at, value in enumerate(nearer(crossed[turn, j, 0] + crossed[turn, j, 1])):
                at = j * per_slab + at
                if ratio is not None:
                    value = value + ratio * first_values[0, at]
                first_values[turn, at] = value
                entering[turn, at + 1] = weights[at] * value
            if j == 0:
                middle_copy(turn, 1).start()
                continue
            if j == 1:
                middle_copy(turn, 0).wait_recv()
            begin, end = plan.groups[group]
            count = end - begin

            def rows_of(ref):
                return ref.reshape(count * PAIRED, LANES)

            here = rows_of(entering[turn, begin + 1:end + 1])
            outer = product(rows_of(entering[turn, begin:end]), inside_block, NN, exact)
            outer = outer + product(rows_of(entering[turn, begin + 2:end + 2]), outside_block, NN, exact)
            if end == half_blocks:
                kept = jnp.concatenate([
                    product(here[:-PAIRED], same_block, NN, exact), product(here[-PAIRED:], ends_block, NN, exact)
                ], 0)
            else:
                kept = product(here, same_block, NN, exact)
            kept = (rows_of(weights[begin:end]) * (outer + kept)).astype(jnp.bfloat16).astype(jnp.float32)
            with_values = rows_of(first_values[turn, begin:end]) * kept
            overlap = overlap + jnp.sum(with_values.reshape(count, PAIRED, LANES), 0)
            parts = [kept[at * PAIRED:(at + 1) * PAIRED] for at in range(count)]
            if end == half_blocks:
                parts.append(pieces(in_lanes([over(overlap)] + more, PAIRED)))
            gathered[turn, group, core, near_chip, :, :len(parts) * LANES] = jnp.concatenate(parts, 1).astype(jnp.bfloat16)
            for _, target in near_targets:
                gather_copy(turn, group, target).start()
            group += 1
        def unfold(group):
            begin, end = plan.groups[group]
            relay_copy(turn, group, 1 - core).wait_recv()
            for half in range(2):
                for at in range(begin, end):
                    part = gathered[turn, group, half, :, :, (at - begin) * LANES:(at - begin + 1) * LANES]
                    part = part.reshape(plan.columns, LANES)
                    low = (half_blocks + at if half else half_blocks - 1 - at) * LANES
                    filtered[:, low:low + LANES] = part

        for group in range(len(plan.groups)):
            everyone = gathered.at[turn, group, core, near_others, :, pl.ds(0, extent(group))]
            all_of(everyone, gather_send.at[turn, group], gather_recv.at[turn, group]).wait_recv()
            relay_copy(turn, group, core).start()
        for group in range(len(plan.groups) - 1):
            unfold(group)
        for span in chunks:
            image[:, span] = transposed(span, plan.inner)
        unfold(len(plan.groups) - 1)
        last = len(plan.groups) - 1
        span = slice(extent(last) - LANES, extent(last))
        first_terms, second_terms = [
            gathered[turn, last, half, :, :, span].astype(jnp.float32).reshape(plan.columns, LANES) for half in range(2)
        ]
        norm, ridge = joined(first_terms, 1), joined(first_terms, 2)
        step_col = norm / (ridge + joined(first_terms, 0) + joined(second_terms, 0))
        return scalars, ratio, step_col, joined(first_terms, 3)

    def extent(group):
        begin, end = plan.groups[group]
        return LANES * (end - begin + (end == half_blocks))

    def middle_copy(turn, at):
        src, dst = entering.at[turn, 1], entering.at[turn, 0]
        return remote(src if at else dst, dst, middle_send.at[turn], middle_recv.at[turn], partner)

    def gather_copy(turn, group, target):
        here = gathered.at[turn, group, core, near_chip, :, pl.ds(0, extent(group))]
        return remote(here, here, gather_send.at[turn, group], gather_recv.at[turn, group], target)

    def relay_copy(turn, group, which):
        here = gathered.at[turn, group, which, :, :, pl.ds(0, extent(group))]
        return remote(here, here, relay_send.at[turn, group], relay_recv.at[turn, group], partner)

    terms = [left + right for left, right in zip(*part_terms)]
    low = direc[:, spans[1]].astype(jnp.bfloat16)
    (norm, ridge), _, step_col, _ = filtered_sum(0, low, terms, spans[1], lambda sums_of: (None, list(sums_of)))
    terms = [0.0, 0.0, 0.0]
    for span in chunks:
        along, ridge_part = direc[:, span], ridge_row[:, span]
        left = resid[:, span] - step_col * (transposed_rest(span) + ridge_part * along)
        ahead = scale_row[:, span] * left
        resid[:, span] = left
        solut[:, span] = step_col * along
        scal[:, span] = ahead
        ridged = ridge_part * ahead
        added = (over(left * ahead), over(ridged * ahead), over(ridged * along))
        terms = [term + more for term, more in zip(terms, added)]

    def settle(sums_of):
        norm_next, own_ridge, cross = sums_of
        ratio = norm_next / norm
        return ratio, [norm_next, own_ridge + ratio * (2.0 * cross + ratio * ridge), ratio]

    low = scal[...].astype(jnp.bfloat16)
    _, _, step_col, ratio_col = filtered_sum(1, low, terms, slice(0, plan.width), settle)

    def put(out, tile, value):
        out[(tile + 1) * LANES:(tile + 2) * LANES, :] = value

    held = {}
    for span in chunks:
        along = scal[:, span] + ratio_col * direc[:, span]
        ahead = solut[:, span] + step_col * along
        left = resid[:, span] - step_col * (transposed_rest(span) + ridge_row[:, span] * along)
        for low in range(0, span.stop - span.start, LANES):
            held[(span.start + low) // LANES] = (ahead[:, low:low + LANES].T, left[:, low:low + LANES].T)
        for tile in [tile for tile in held if tile < plan.full]:
            new_ahead, new_left = held.pop(tile)
            put(solution_out, tile, new_ahead)
            put(residual_out, tile, new_left)
    mixed, last = held[plan.full], held[plan.full + 1]
    for out, edge, end in ((solution_out, mixed[0], last[0]), (residual_out, mixed[1], last[1])):
        out[:LANES, :] = edge
        put(out, plan.full, edge)
        low = pl.multiple_of((plan.full + 1) * LANES + offset, plan.rest)
        out[pl.ds(low, plan.rest), :] = end[:plan.rest]

    all_of(shown.at[others], show_send, show_recv).wait_send()
    all_of(seen_weight.at[others], weight_send, weight_recv).wait_send()
    for part, (low, size) in enumerate(((0, plan.cut), (plan.cut, plan.mixed_at - plan.cut), (plan.mixed_at, LANES))):
        all_of(block.at[others, :, pl.ds(low, size)], block_send.at[part], loose_recv).wait_send()
    all_of(loose.at[others], block_send.at[3], loose_recv).wait_send()
    all_of(early.at[core, near_others], early_send, early_recv).wait_send()
    all_of(early.at[core], early_relay_send, early_relay_recv).wait_send()
    for turn in range(2):
        all_of(received.at[turn], pair_send.at[turn], pair_recv.at[turn, 0]).wait_send()
        all_of(sent.at[turn, :, near_others], fold_send.at[turn], fold_recv.at[turn, 0]).wait_send()
        all_of(sent_terms.at[turn, near_others], term_send.at[turn], term_recv.at[turn]).wait_send()
        all_of(whole_parts.at[pl.ds(0, 3)], whole_send.at[turn], whole_recv.at[turn]).wait_send()
        all_of(crossed.at[turn, :, 0], cross_send.at[turn], cross_recv.at[turn, 0]).wait_send()
        middle_copy(turn, 1).wait_send()
        for group in range(len(plan.groups)):
            everyone = gathered.at[turn, group, core, near_others, :, pl.ds(0, extent(group))]
            all_of(everyone, gather_send.at[turn, group], gather_recv.at[turn, group]).wait_send()
            relay_copy(turn, group, core).wait_send()


def far(value):
    return pltpu.with_memory_space_constraint(value, pltpu.HBM)


def fused_shards(design, observed, slab_counts, gap_mask, filter_taps, kaula_diag, precond):
    epoch_rows, coef_rows = design.shape
    columns = observed.shape[1]
    slabs, coefs = lax.axis_size("tm"), lax.axis_size("coef")
    plan = Plan(slabs, coefs, epoch_rows, coef_rows, columns)
    wide, chips, message = plan.width, plan.chips, plan.message
    half_slabs, half_chips = slabs // 2, chips // 2
    f32, bf16 = jnp.float32, jnp.bfloat16
    vmem = pl.BlockSpec(memory_space=pltpu.VMEM)
    hbm = pl.BlockSpec(memory_space=pltpu.HBM)
    sem = pltpu.SemaphoreType.DMA
    shape = jax.ShapeDtypeStruct((wide + LANES, columns), f32)
    tiles = (plan.tiles, LANES)
    outs = pl.pallas_call(
        functools.partial(fused, plan),
        out_shape=(shape, shape),
        in_specs=[hbm, hbm, hbm, pl.BlockSpec(memory_space=pltpu.SMEM), hbm, hbm, hbm],
        out_specs=(vmem, vmem),
        scratch_shapes=[
            pltpu.VMEM((epoch_rows, columns), f32),
            pltpu.VMEM((epoch_rows // LANES, LANES), jnp.int32),
            pltpu.VMEM((1, LANES), f32),
            pltpu.VMEM(tiles, f32),
            pltpu.VMEM(tiles, f32),
            pltpu.VMEM((slabs, epoch_rows, wide), bf16),
            pltpu.VMEM((slabs, wide, epoch_rows), bf16),
            pltpu.VMEM((slabs, 2, epoch_rows, LANES), bf16),
            pltpu.VMEM((slabs, epoch_rows + plan.packed_rows, LANES), bf16),
            pltpu.VMEM((slabs, plan.packed_rows, LANES), bf16),
            pltpu.VMEM((chips, GROUP, epoch_rows), f32),
            pltpu.VMEM((slabs, GROUP, epoch_rows), f32),
            pltpu.VMEM((slabs, epoch_rows // LANES, LANES), f32),
            pltpu.VMEM((2, half_chips, GROUP, slabs * epoch_rows), bf16),
            pltpu.VMEM((2, slabs, columns, epoch_rows), f32),
            pltpu.VMEM((2, half_slabs, columns, epoch_rows), f32),
            pltpu.VMEM((half_slabs, half_chips, PAIRED, epoch_rows), f32),
            pltpu.VMEM((2, half_slabs, half_chips, PAIRED, epoch_rows), bf16),
            pltpu.VMEM((2, half_slabs, half_chips, PAIRED, epoch_rows), bf16),
            pltpu.VMEM((2, half_chips, PAIRED, LANES), bf16),
            pltpu.VMEM((2, half_chips, PAIRED, LANES), bf16),
            pltpu.VMEM((2, 2, 2, PAIRED, LANES), f32),
            pltpu.VMEM((4, PAIRED, LANES), f32),
            pltpu.VMEM((2, half_slabs, 2, PAIRED, epoch_rows), f32),
            pltpu.VMEM((2, plan.half_blocks + 2, PAIRED, LANES), f32),
            pltpu.VMEM((plan.half_blocks, PAIRED, LANES), f32),
            pltpu.VMEM((columns, slabs * epoch_rows), bf16),
            pltpu.VMEM((2, len(plan.groups), 2, half_chips, PAIRED, message), bf16),
            pltpu.VMEM((columns, wide), f32),
            pltpu.VMEM((columns, wide), f32),
            pltpu.VMEM((columns, wide), f32),
            pltpu.VMEM((columns, wide), f32),
            pltpu.VMEM((columns, wide), f32),
            pltpu.VMEM((2, plan.half_blocks, PAIRED, LANES), f32),
            sem(()), sem((5,)), sem(()), sem((4,)), sem((2, slabs)), *[sem(())] * 5,
            sem(()), sem(()), sem(()), sem(()),
            sem((2,)), sem((2, half_slabs)), sem((2,)), sem((2, half_slabs)), sem((2,)), sem((2,)), sem((2,)), sem((2,)), sem((2,)), sem((2, half_slabs)),
            sem((2,)), sem((2,)), *[sem((2, len(plan.groups)))] * 4,
        ],
        compiler_params=pltpu.CompilerParams(
            collective_id=0, has_side_effects=True, vmem_limit_bytes=48 * 1024 * 1024
        ),
    )(
        design, far(observed), far(gap_mask.reshape(-1, LANES)), slab_counts, far(filter_taps[None]),
        far(kaula_diag.reshape(tiles)), far(precond.reshape(tiles)),
    )
    owner = lax.axis_index("tm")
    low = owner * plan.owned - plan.first_tile(owner) * LANES
    return tuple(lax.dynamic_slice_in_dim(out, low, plan.owned, 0) for out in outs)


def shards(*arrays):
    design, observed, filter_taps = arrays[0], arrays[1], arrays[4]
    sizes = (lax.axis_size("tm"), lax.axis_size("coef"), *design.shape, observed.shape[1], filter_taps.shape[0])
    return fused_shards(*arrays) if fits(*sizes) else general_shards(*arrays)


def solution(mesh):
    placed = (P("tm", "coef"), P("tm", None), P("tm"), P("tm"), P(), P("coef"), P("coef"))
    return jax.shard_map(
        shards,
        mesh=mesh,
        in_specs=placed,
        out_specs=(P(("coef", "tm"), None), P(("coef", "tm"), None)),
        check_vma=False,
    )
```

```python
import functools

import jax
import jax.numpy as jnp
from jax import lax
from jax.experimental import pallas as pl
from jax.experimental.pallas import tpu as pltpu
from jax.sharding import PartitionSpec as P

ITERS = 2
HIGHEST = lax.Precision.HIGHEST


def toeplitz(pattern, band_len):
    tiled = jnp.tile(pattern, band_len)[: band_len * (2 * band_len - 1)]
    return tiled.reshape(band_len, 2 * band_len - 1)[:, :band_len]


def block_pair(filter_taps):
    band_len = filter_taps.shape[0]
    spacer = jnp.zeros((band_len,), jnp.float32)
    reversed_taps = filter_taps[:0:-1]
    lower = jnp.concatenate([filter_taps[:1], spacer, reversed_taps])
    upper = jnp.concatenate([jnp.zeros((1,), jnp.float32), reversed_taps, spacer])
    return (toeplitz(lower, band_len), toeplitz(upper, band_len))


def forward(values, lower_block, upper_block):
    band_len = lower_block.shape[0]
    blocks = values.reshape(-1, band_len, values.shape[1])
    previous = jnp.concatenate([jnp.zeros_like(blocks[:1]), blocks[:-1]], 0)
    result = jnp.einsum("ij,bjr->bir", lower_block, blocks, precision=HIGHEST)
    result = result + jnp.einsum("ij,bjr->bir", upper_block, previous, precision=HIGHEST)
    return result.reshape(values.shape)


def backward(values, lower_block, upper_block):
    band_len = lower_block.shape[0]
    blocks = values.reshape(-1, band_len, values.shape[1])
    following = jnp.concatenate([blocks[1:], jnp.zeros_like(blocks[:1])], 0)
    result = jnp.einsum("ji,bjr->bir", lower_block, blocks, precision=HIGHEST)
    result = result + jnp.einsum("ji,bjr->bir", upper_block, following, precision=HIGHEST)
    return result.reshape(values.shape)


def general_shards(design, observed, slab_counts, gap_mask, filter_taps, kaula_diag, precond):
    epoch_rows, coef_rows = design.shape
    columns = observed.shape[1]
    slabs = lax.axis_size("tm")
    epochs = slabs * epoch_rows
    owned_rows = coef_rows // slabs
    owner_index = lax.axis_index("tm")
    lower_block, upper_block = block_pair(filter_taps)
    position = jnp.arange(epoch_rows, dtype=jnp.int32)
    local_weight = ((gap_mask == 1) & (position < slab_counts[0])).astype(jnp.float32)
    packed = jnp.concatenate([observed, local_weight.reshape(-1, columns)], 0)
    gathered = lax.all_gather(packed, "tm", axis=0, tiled=False)
    all_observed = gathered[:, :epoch_rows].reshape(epochs, columns)
    weight = gathered[:, epoch_rows:].reshape(epochs, 1)
    block = lax.all_to_all(design, "tm", split_axis=1, concat_axis=0, tiled=True)

    def weighted(values):
        inner = forward(weight * values, lower_block, upper_block)
        return (weight * backward(inner, lower_block, upper_block)).astype(jnp.bfloat16)

    def transposed(filtered):
        return lax.dot_general(
            block, filtered, (((0,), (0,)), ((), ())), preferred_element_type=jnp.float32
        )

    def summed(scaled, terms):
        partial = jnp.dot(block, scaled.astype(jnp.bfloat16), preferred_element_type=jnp.float32)
        rows = [jnp.sum(term, 0)[None] for term in terms]
        rows.append(jnp.zeros((8 - len(rows), columns), jnp.float32))
        total = lax.psum(jnp.concatenate([partial] + rows, 0), ("tm", "coef"))
        return total[:epochs], [total[epochs + at] for at in range(len(terms))]

    start = owner_index * owned_rows
    kaula_col = lax.dynamic_slice_in_dim(kaula_diag, start, owned_rows, 0)[:, None]
    precond_col = lax.dynamic_slice_in_dim(precond, start, owned_rows, 0)[:, None]
    residual = transposed(weighted(all_observed))
    solution = jnp.zeros_like(residual)
    for iteration in range(ITERS):
        scaled = precond_col * residual
        terms = [residual * scaled, kaula_col * scaled * scaled]
        if iteration == 0:
            slab_values, (norm_now, ridge) = summed(scaled, terms)
            direction = scaled
        else:
            terms.append(kaula_col * scaled * direction)
            fresh, (norm_next, own_ridge, cross) = summed(scaled, terms)
            ratio = norm_next / norm_now
            slab_values = fresh + ratio * slab_values
            ridge = own_ridge + ratio * (2.0 * cross + ratio * ridge)
            direction = scaled + ratio * direction
            norm_now = norm_next
        filtered = weighted(slab_values)
        curvature = ridge + jnp.sum(slab_values * filtered.astype(jnp.float32), 0)
        step_len = norm_now / curvature
        image = transposed(filtered) + kaula_col * direction
        solution = solution + step_len * direction
        residual = residual - step_len * image
    return (solution, residual)


LANES = 128
GROUP = 8
PAIRED = 2 * GROUP
MESH = pl.DeviceIdType.MESH
NN = ((1,), (0,))
NT = ((1,), (1,))


class Plan:
    def __init__(self, slabs, coefs, epoch_rows, coef_rows, columns):
        self.slabs, self.coefs, self.epoch_rows, self.columns = slabs, coefs, epoch_rows, columns
        self.tiles = coef_rows // LANES
        self.owned = coef_rows // slabs
        self.full = self.owned // LANES - 1
        self.rest = self.owned % LANES
        self.packed_rows = epoch_rows * self.rest // LANES
        self.mixed_at = self.full * LANES
        self.width = (self.full + 2) * LANES
        self.cut = (self.full - 1) * LANES
        self.across = coefs // 2
        self.chips = slabs * self.across
        self.blocks = slabs * epoch_rows // LANES
        self.half_blocks = self.blocks // 2
        per_slab, half_slabs = epoch_rows // LANES, slabs // 2
        ends = [(upto + 1) * per_slab - 1 for upto in range(1, half_slabs - 1)] + [self.half_blocks]
        self.groups = list(zip([0] + ends[:-1], ends))
        self.inner = (self.half_blocks - self.groups[-1][0], self.half_blocks + self.groups[-1][0])
        self.message = LANES * (1 + max(end - begin for begin, end in self.groups))

    def first_tile(self, owner):
        return lax.div(owner * self.owned, LANES)


def fits(slabs, coefs, epoch_rows, coef_rows, columns, taps):
    if slabs & (slabs - 1) or slabs < 4 or coefs % 2 or coefs & (coefs - 1) or epoch_rows % (2 * LANES) or coef_rows % LANES:
        return False
    if coef_rows % slabs or taps != LANES or columns != LANES or columns != GROUP * slabs * coefs // 2:
        return False
    owned = coef_rows // slabs
    rest = owned % LANES
    return owned >= 4 * LANES and rest >= 16 and LANES % rest == 0


def flips(index, count):
    steps, weight = [], 1
    while weight < count:
        steps.append(weight * (1 - 2 * lax.rem(lax.div(index, weight), 2)))
        weight *= 2
    return [sum((step for at, step in enumerate(steps) if bits >> at & 1), index) for bits in range(count)]


def pieces(values):
    high = values.astype(jnp.bfloat16).astype(jnp.float32)
    left = values - high
    middle = left.astype(jnp.bfloat16).astype(jnp.float32)
    low = (left - middle).astype(jnp.bfloat16).astype(jnp.float32)
    return high + pltpu.roll(middle, 8, 1) + pltpu.roll(low, 16, 1)


def joined(values, at):
    lane = lax.broadcasted_iota(jnp.int32, values.shape, 1)
    taken = (lane % 8 == at) & (lane < 24)
    return jnp.sum(jnp.where(taken, values, 0.0), 1, keepdims=True)


def in_lanes(terms, rows):
    lane = lax.broadcasted_iota(jnp.int32, (rows, LANES), 1)
    result = jnp.zeros((rows, LANES), jnp.float32)
    for at, term in enumerate(terms):
        result = jnp.where(lane == at, term, result)
    return result


def product(left, right, contract, precision=None):
    return lax.dot_general(
        left, right, (contract, ((), ())), precision=precision, preferred_element_type=jnp.float32
    )


def fused(plan, design, observed_in, gap_in, counts, taps_in, kaula_in, precond_in, solution_out, residual_out,
          observed, gap, taps, kaula, precond,
          block, turned_block, edges, packed, loose, shown, seen, seen_weight, early, sums, received, total, sent, folded_in, sent_terms, terms_in,
          whole, whole_parts, crossed, entering, weights, filtered, gathered, resid, direc, scal, solut, image, first_values,
          own_sem, small_sem, edge_sem, block_send, block_recv, loose_recv, show_send, show_recv, weight_send, weight_recv, early_send, early_recv,
          early_relay_send, early_relay_recv, pair_send, pair_recv, fold_send, fold_recv, term_send, term_recv,
          whole_send, whole_recv, cross_send, cross_recv, middle_send, middle_recv, gather_send, gather_recv, relay_send, relay_recv):
    slabs, chips, rows = plan.slabs, plan.chips, plan.epoch_rows
    half_slabs, half_chips, half_blocks = slabs // 2, chips // 2, plan.half_blocks
    slab, coef = lax.axis_index("tm"), lax.axis_index("coef")
    across, core = lax.div(coef, 2), lax.rem(coef, 2)
    chip = slab * plan.across + across
    near_chip = lax.rem(chip, half_chips)
    partner = {"tm": slab, "coef": 2 * across + 1 - core}

    peers, sides = flips(slab, slabs), flips(across, plan.across)
    targets = [
        (peers[bits] * plan.across + sides[side], {"tm": peers[bits], "coef": coef + 2 * (sides[side] - across)})
        for bits in reversed(range(slabs)) for side in reversed(range(plan.across)) if bits or side
    ]
    near_targets = [
        (at - lax.div(slab, half_slabs) * half_chips, target) for at, target in targets[-(half_chips - 1):]
    ]
    this_half = lax.div(slab, half_slabs)
    mirror = {"tm": peers[half_slabs], "coef": coef}
    across_mirror = {"tm": peers[half_slabs], "coef": 2 * across + 1 - core}
    met = [
        {"tm": peers[bits], "coef": coef + 2 * (sides[side] - across)}
        for bits in range(slabs) for side in range(plan.across)
        if (bits or side) and (bits < half_slabs or not side)
    ] + [partner, across_mirror]

    def remote(src, dst, send, recv, target):
        return pltpu.make_async_remote_copy(
            src_ref=src, dst_ref=dst, send_sem=send, recv_sem=recv, device_id=target, device_id_type=MESH
        )

    barrier = pltpu.get_barrier_semaphore()
    for target in met:
        pl.semaphore_signal(barrier, inc=1, device_id=target, device_id_type=MESH)

    small = [
        pltpu.make_async_copy(src, dst, small_sem.at[at])
        for at, (src, dst) in enumerate(
            ((observed_in, observed), (gap_in, gap), (taps_in, taps), (kaula_in, kaula), (precond_in, precond))
        )
    ]
    for copy in small:
        copy.start()
    first = plan.first_tile(slab)
    offset = slab * plan.owned - first * LANES

    def tile_columns(tile, size):
        return pl.ds(pl.multiple_of(tile * LANES, LANES), size)

    own = pltpu.make_async_copy(
        design.at[:, tile_columns(first + 1, plan.mixed_at)], block.at[slab, :, pl.ds(0, plan.mixed_at)], own_sem
    )
    own.start()
    for owner in range(slabs):
        begin = owner * plan.owned // LANES
        for at, tile in enumerate((begin, begin + plan.full + 1)):
            pltpu.make_async_copy(
                design.at[:, pl.ds(tile * LANES, LANES)], edges.at[owner, at], edge_sem
            ).start()

    for copy in small[:3]:
        copy.wait()
    tall = rows // LANES
    place = lax.broadcasted_iota(jnp.int32, (tall, LANES), 0) * LANES + lax.broadcasted_iota(jnp.int32, (tall, LANES), 1)
    local_weight = jnp.where((gap[...] == 1) & (place < counts[0]), 1.0, 0.0)
    seen_weight[slab] = local_weight
    weight_row = jnp.concatenate([local_weight[at:at + 1] for at in range(tall)], 1)
    turned = observed[...].T * weight_row
    shown[...] = turned.reshape(chips, GROUP, rows)
    seen[slab] = shown[2 * near_chip + core]
    for turn in range(2):
        for j in range(half_slabs):
            folded_in[turn, j, near_chip] = jnp.zeros((PAIRED, rows), jnp.bfloat16)

    def block_copy(bits, part):
        peer = peers[bits]
        tile = plan.first_tile(peer) + 1
        if part == 0:
            src, dst = design.at[:, tile_columns(tile, plan.cut)], block.at[slab, :, pl.ds(0, plan.cut)]
        elif part == 1:
            src = design.at[:, tile_columns(tile + plan.cut // LANES, plan.mixed_at - plan.cut)]
            dst = block.at[slab, :, pl.ds(plan.cut, plan.mixed_at - plan.cut)]
        elif part == 2:
            src, dst = packed.at[peer, pl.ds(0, rows)], block.at[slab, :, pl.ds(plan.mixed_at, LANES)]
        else:
            src, dst = packed.at[peer, pl.ds(rows, plan.packed_rows)], loose.at[slab]
        return remote(src, dst, block_send.at[part], loose_recv if part == 3 else block_recv.at[min(part, 1), slab], {"tm": peer, "coef": coef})

    def block_arrival(bits, part):
        peer = peers[bits]
        low, size = ((0, plan.cut), (plan.cut, plan.mixed_at + LANES - plan.cut))[part]
        dst = block.at[peer, :, pl.ds(low, size)]
        return remote(dst, dst, block_send.at[part], block_recv.at[part, peer], {"tm": peer, "coef": coef})

    def all_of(ref, send, recv):
        return remote(ref, ref, send, recv, partner)

    def show_copy(bits):
        peer = peers[bits]
        src = shown.at[2 * lax.rem(peer * plan.across + across, half_chips) + core]
        return remote(src, seen.at[slab], show_send, show_recv, {"tm": peer, "coef": coef})

    def weight_copy(bits):
        src = seen_weight.at[slab]
        return remote(src, src, weight_send, weight_recv, {"tm": peers[bits], "coef": coef})

    others = pl.ds(0, slabs - 1)
    pl.semaphore_wait(barrier, len(met))
    for bits in range(1, slabs):
        show_copy(bits).start()
        weight_copy(bits).start()
    for bits in range(1, half_slabs):
        block_copy(bits, 0).start()
        block_copy(bits, 1).start()
    for bits in range(half_slabs, slabs):
        block_copy(bits, 0).start()

    pltpu.make_async_copy(edges, edges, edge_sem).wait()
    lane_row = lax.broadcasted_iota(jnp.int32, (1, LANES), 1)
    for owner in range(slabs):
        skip = owner * plan.owned % LANES
        ahead = edges[owner, 0].astype(jnp.float32)
        behind = edges[owner, 1].astype(jnp.float32)
        packed[owner, :rows] = jnp.where(lane_row >= skip, ahead, behind).astype(jnp.bfloat16)
        tight = jnp.zeros((plan.packed_rows, LANES), jnp.float32)
        for at in range(LANES // plan.rest):
            part = behind[at * plan.packed_rows:(at + 1) * plan.packed_rows]
            shift = (at * plan.rest - skip) % LANES
            part = pltpu.roll(part, shift, 1) if shift else part
            tight = jnp.where(lax.div(lane_row, plan.rest) == at, part, tight)
        packed[owner, rows:] = tight.astype(jnp.bfloat16)
    for bits in range(1, slabs):
        block_copy(bits, 2).start()
        block_copy(bits, 3).start()

    def unpack(at, tight):
        tight = tight.astype(jnp.float32)
        for piece in range(LANES // plan.rest):
            part = pltpu.roll(tight, LANES - piece * plan.rest, 1) if piece else tight
            part = jnp.where(lane_row < plan.rest, part, 0.0).astype(jnp.bfloat16)
            block[at, piece * plan.packed_rows:(piece + 1) * plan.packed_rows, plan.mixed_at + LANES:] = part

    block[slab, :, plan.mixed_at:plan.mixed_at + LANES] = packed[slab, :rows]
    unpack(slab, packed[slab, rows:])

    base = jnp.concatenate([taps[...], jnp.zeros((1, LANES), jnp.float32)], 1)
    shifted = pltpu.roll(jnp.broadcast_to(base, (LANES, 2 * LANES)), 0, 1, stride=1, stride_axis=0)
    lower, upper = shifted[:, :LANES], shifted[:, LANES:]
    blank = jnp.zeros((GROUP, LANES), jnp.float32)

    all_of(seen.at[others], show_send, show_recv).wait_recv()
    all_of(seen_weight.at[others], weight_send, weight_recv).wait_recv()

    def repeated(at, j):
        return jnp.broadcast_to(seen_weight[at, j:j + 1, :], (GROUP, LANES))

    weight = jnp.concatenate([repeated(at, j) for at in range(slabs) for j in range(tall)], 0)
    own_series = jnp.concatenate([seen[at, :, j * LANES:(j + 1) * LANES] for at in range(slabs) for j in range(tall)], 0)

    def weighted(values):
        entering = weight * values
        before = jnp.concatenate([blank, entering[:-GROUP]], 0)
        inner = product(entering, lower, NN, lax.Precision.HIGHEST) + product(before, upper, NN, lax.Precision.HIGHEST)
        after = jnp.concatenate([inner[GROUP:], blank], 0)
        outer = product(inner, lower, NT, lax.Precision.HIGHEST) + product(after, upper, NT, lax.Precision.HIGHEST)
        return (weight * outer).astype(jnp.bfloat16)

    def nearer(span):
        parts = [span[:, at * LANES:(at + 1) * LANES] for at in range(rows // LANES)]
        return [jnp.where(core == 0, left, right) for left, right in zip(parts[::-1], parts)]

    def outward(at, which):
        return which * (half_slabs + at) + (1 - which) * (half_slabs - 1 - at)

    for at in range(half_slabs):
        place_of = outward(at, core)
        wide = jnp.concatenate([repeated(place_of, j) for j in range(tall)], 1)
        for j, part in enumerate(nearer(wide)):
            weights[at * tall + j] = jnp.concatenate([part, part], 0)
    exact = lax.Precision.HIGHEST
    ends_block = product(lower, lower, NT, exact)
    same_block = ends_block + product(upper, upper, NT, exact)
    before_block, after_block = product(upper, lower, NT, exact), product(lower, upper, NT, exact)
    inside_block = jnp.where(core == 0, after_block, before_block)
    outside_block = jnp.where(core == 0, before_block, after_block)
    ends_block = jnp.where(core == 0, same_block, ends_block)

    kept = weighted(own_series).astype(jnp.float32)
    for j in range(plan.blocks):
        early[core, near_chip, :, j * LANES:(j + 1) * LANES] = kept[j * GROUP:(j + 1) * GROUP].astype(jnp.bfloat16)
    here = early.at[core, near_chip]
    for _, target in near_targets:
        remote(here, here, early_send, early_recv, target).start()
    for bits in range(half_slabs, slabs):
        block_copy(bits, 1).start()

    small[3].wait()
    small[4].wait()

    def local_row(table):
        inside = [table[pl.ds(first + 1 + at, 1), :] for at in range(plan.full)]
        ahead, behind = table[pl.ds(first, 1), :], table[pl.ds(first + plan.full + 1, 1), :]
        moved = pltpu.roll(jnp.broadcast_to(behind, (GROUP, LANES)), lax.rem(LANES - offset, LANES), 1)[:1]
        mixed = jnp.where(lane_row >= offset, ahead, behind)
        return jnp.concatenate(inside + [mixed, jnp.where(lane_row < plan.rest, moved, 0.0)], 1)

    ridge_row, scale_row = local_row(kaula), local_row(precond)

    near_others = pl.ds(0, half_chips - 1)
    all_of(early.at[core, near_others], early_send, early_recv).wait_recv()
    mine, theirs = early.at[core], early.at[1 - core]
    remote(mine, mine, early_relay_send, early_relay_recv, partner).start()
    remote(theirs, theirs, early_relay_send, early_relay_recv, partner).wait_recv()
    for at in range(slabs):
        span = slice(at * rows, (at + 1) * rows)
        both = jnp.stack([early[0, :, :, span].astype(jnp.float32), early[1, :, :, span].astype(jnp.float32)], 1)
        filtered[:, span] = both.reshape(plan.columns, rows).astype(jnp.bfloat16)

    def series(at):
        return filtered[:, pl.ds(pl.multiple_of(at * rows, rows), rows)]

    def over(terms):
        return jnp.sum(terms, 1, keepdims=True)

    own.wait()
    spans = (slice(0, plan.cut), slice(plan.cut, plan.width))
    part_terms = []

    def turn_over(at, span):
        turned_block[at, span] = block[at, :, span].T

    for part, span in enumerate(spans):
        if part:
            all_of(loose.at[others], block_send.at[3], loose_recv).wait_recv()
        turn_over(slab, span)
        resid[:, span] = product(series(slab), block[slab, :, span], NN)
        for bits in range(1, slabs):
            peer = peers[bits]
            block_arrival(bits, part).wait_recv()
            if part:
                unpack(peer, loose[peer])
            turn_over(peer, span)
            resid[:, span] += product(series(peer), block[peer, :, span], NN)
        direc[:, span] = scale_row[:, span] * resid[:, span]
        if part == 0:
            low = direc[:, span].astype(jnp.bfloat16)

            def body(at, carry):
                sums[0, at] = product(low, turned_block[at, :plan.cut], NN)
                return carry

            lax.fori_loop(0, slabs, body, 0)
        ridged = ridge_row[:, span] * direc[:, span]
        part_terms.append((over(resid[:, span] * direc[:, span]), over(ridged * direc[:, span])))

    def pair_copy(turn, j):
        src = sums.at[turn, outward(j, 1 - core)]
        return remote(src, received.at[turn, j], pair_send.at[turn], pair_recv.at[turn, j], partner)

    def fold_copy(turn, j, to, target):
        src, dst = sent.at[turn, j, to], folded_in.at[turn, j, near_chip]
        return remote(src, dst, fold_send.at[turn], fold_recv.at[turn, j], target)

    def cross_copy(turn, j):
        here = crossed.at[turn, j, this_half]
        return remote(here, here, cross_send.at[turn], cross_recv.at[turn, j], mirror)

    def whole_copy(turn, target):
        here = whole.at[turn, this_half, core]
        return remote(here, here, whole_send.at[turn], whole_recv.at[turn], target)


    def term_copy(turn, to, target):
        src, dst = sent_terms.at[turn, to], terms_in.at[turn, near_chip]
        return remote(src, dst, term_send.at[turn], term_recv.at[turn], target)

    chunks = [slice(low, min(low + 2 * LANES, plan.width)) for low in range(0, plan.width, 2 * LANES)]

    def transposed(span, blocks):
        begin, end = blocks
        parts, at = [], begin
        while at < end:
            upto = min(end, (at // tall + 1) * tall)
            parts.append(block[at // tall, at % tall * LANES:(upto - at // tall * tall) * LANES, span])
            at = upto
        return product(filtered[:, begin * LANES:end * LANES], jnp.concatenate(parts, 0), NN)

    def transposed_rest(span):
        begin, end = plan.inner
        return image[:, span] + transposed(span, (0, begin)) + transposed(span, (end, plan.blocks))

    def filtered_sum(turn, low, terms, span, settle):
        def partial(at):
            value = product(low, turned_block[at, span], NN)
            return value + sums[turn, at] if turn == 0 else value

        def give(j, value):
            sums[turn, outward(j, 1 - core)] = value
            pair_copy(turn, j).start()

        def keep(j, value):
            pair_copy(turn, j).wait_recv()
            value = (value + received[turn, j]).reshape(half_chips, PAIRED, rows)
            total[j] = value
            sent[turn, j] = value.astype(jnp.bfloat16)
            for to, target in near_targets:
                fold_copy(turn, j, to, target).start()

        def theirs_at(j):
            return partial(outward(j, 1 - core))

        def ours_at(j):
            return partial(outward(j, core))

        def both(j, carry):
            theirs, ours = theirs_at(j + 2), ours_at(j)
            give(j + 2, theirs)
            keep(j, ours)
            return carry

        first_value, second_value = theirs_at(0), theirs_at(1)
        give(0, first_value)
        give(1, second_value)
        scalars = in_lanes(terms, plan.columns)
        sent_terms[turn] = pieces(scalars).reshape(half_chips, PAIRED, LANES).astype(jnp.bfloat16)
        terms_in[turn, near_chip] = sent_terms[turn, near_chip]
        for to, target in near_targets:
            term_copy(turn, to, target).start()
        lax.fori_loop(0, half_slabs - 2, both, 0)
        first_value, second_value = ours_at(half_slabs - 2), ours_at(half_slabs - 1)
        keep(half_slabs - 2, first_value)
        keep(half_slabs - 1, second_value)

        def added(values):
            return jnp.sum(values.astype(jnp.float32), 0)

        all_of(terms_in.at[turn, near_others], term_send.at[turn], term_recv.at[turn]).wait_recv()
        half_terms = added(terms_in[turn])
        half_terms = half_terms + pltpu.roll(half_terms, LANES - 8, 1) + pltpu.roll(half_terms, LANES - 16, 1)
        whole[turn, this_half, core] = half_terms
        for target in (mirror, across_mirror, partner):
            whole_copy(turn, target).start()
        for j in range(half_slabs):
            all_of(folded_in.at[turn, j, near_others], fold_send.at[turn], fold_recv.at[turn, j]).wait_recv()
            crossed[turn, j, this_half] = added(folded_in[turn, j]) + total[j, near_chip]
            cross_copy(turn, j).start()
        def settled():
            all_of(whole_parts.at[pl.ds(0, 3)], whole_send.at[turn], whole_recv.at[turn]).wait_recv()
            scalars = (whole[turn, 0, 0] + whole[turn, 0, 1]) + (whole[turn, 1, 0] + whole[turn, 1, 1])
            scalars = [scalars[:, at:at + 1] for at in range(len(terms))]
            return scalars, *settle(scalars)

        ratio = None
        if turn:
            scalars, ratio, more = settled()

        per_slab = rows // LANES
        overlap = jnp.zeros((PAIRED, LANES), jnp.float32)
        group = 0
        entering[turn, half_blocks + 1] = jnp.zeros((PAIRED, LANES), jnp.float32)
        for j in range(half_slabs):
            theirs = crossed.at[turn, j, 1 - this_half]
            remote(theirs, theirs, cross_send.at[turn], cross_recv.at[turn, j], mirror).wait_recv()
            for at, value in enumerate(nearer(crossed[turn, j, 0] + crossed[turn, j, 1])):
                at = j * per_slab + at
                if ratio is not None:
                    value = value + ratio * first_values[0, at]
                first_values[turn, at] = value
                entering[turn, at + 1] = weights[at] * value
            if j == 0:
                middle_copy(turn, 1).start()
                continue
            if j == 1:
                middle_copy(turn, 0).wait_recv()
            begin, end = plan.groups[group]
            count = end - begin

            def rows_of(ref):
                return ref.reshape(count * PAIRED, LANES)

            here = rows_of(entering[turn, begin + 1:end + 1])
            outer = product(rows_of(entering[turn, begin:end]), inside_block, NN, exact)
            outer = outer + product(rows_of(entering[turn, begin + 2:end + 2]), outside_block, NN, exact)
            if end == half_blocks:
                kept = jnp.concatenate([
                    product(here[:-PAIRED], same_block, NN, exact), product(here[-PAIRED:], ends_block, NN, exact)
                ], 0)
            else:
                kept = product(here, same_block, NN, exact)
            kept = (rows_of(weights[begin:end]) * (outer + kept)).astype(jnp.bfloat16).astype(jnp.float32)
            with_values = rows_of(first_values[turn, begin:end]) * kept
            overlap = overlap + jnp.sum(with_values.reshape(count, PAIRED, LANES), 0)
            parts = [kept[at * PAIRED:(at + 1) * PAIRED] for at in range(count)]
            if end == half_blocks:
                if not turn:
                    scalars, _, more = settled()
                parts.append(pieces(in_lanes([over(overlap)] + more, PAIRED)))
            gathered[turn, group, core, near_chip, :, :len(parts) * LANES] = jnp.concatenate(parts, 1).astype(jnp.bfloat16)
            for _, target in near_targets:
                gather_copy(turn, group, target).start()
            group += 1
        def unfold(group):
            begin, end = plan.groups[group]
            relay_copy(turn, group, 1 - core).wait_recv()
            for half in range(2):
                for at in range(begin, end):
                    part = gathered[turn, group, half, :, :, (at - begin) * LANES:(at - begin + 1) * LANES]
                    part = part.reshape(plan.columns, LANES)
                    low = (half_blocks + at if half else half_blocks - 1 - at) * LANES
                    filtered[:, low:low + LANES] = part

        final = len(plan.groups) - 1
        for group in range(final + 1):
            everyone = gathered.at[turn, group, core, near_others, :, pl.ds(0, extent(group))]
            all_of(everyone, gather_send.at[turn, group], gather_recv.at[turn, group]).wait_recv()
            relay_copy(turn, group, core).start()
            if group < 1 or group > final:
                continue
            unfold(group - 1)
            begin, end = plan.groups[group - 1]
            low, high = half_blocks - end, half_blocks + end
            ranges = [(low, half_blocks - begin), (half_blocks + begin, high)] if begin else [(low, high)]
            for span in chunks:
                for at, blocks in enumerate(ranges):
                    value = transposed(span, blocks)
                    image[:, span] = image[:, span] + value if group > 1 or at else value
        unfold(final)
        last = len(plan.groups) - 1
        span = slice(extent(last) - LANES, extent(last))
        first_terms, second_terms = [
            gathered[turn, last, half, :, :, span].astype(jnp.float32).reshape(plan.columns, LANES) for half in range(2)
        ]
        norm, ridge = joined(first_terms, 1), joined(first_terms, 2)
        step_col = norm / (ridge + joined(first_terms, 0) + joined(second_terms, 0))
        return scalars, ratio, step_col, joined(first_terms, 3)

    def extent(group):
        begin, end = plan.groups[group]
        return LANES * (end - begin + (end == half_blocks))

    def middle_copy(turn, at):
        src, dst = entering.at[turn, 1], entering.at[turn, 0]
        return remote(src if at else dst, dst, middle_send.at[turn], middle_recv.at[turn], partner)

    def gather_copy(turn, group, target):
        here = gathered.at[turn, group, core, near_chip, :, pl.ds(0, extent(group))]
        return remote(here, here, gather_send.at[turn, group], gather_recv.at[turn, group], target)

    def relay_copy(turn, group, which):
        here = gathered.at[turn, group, which, :, :, pl.ds(0, extent(group))]
        return remote(here, here, relay_send.at[turn, group], relay_recv.at[turn, group], partner)

    terms = [left + right for left, right in zip(*part_terms)]
    low = direc[:, spans[1]].astype(jnp.bfloat16)
    (norm, ridge), _, step_col, _ = filtered_sum(0, low, terms, spans[1], lambda sums_of: (None, list(sums_of)))
    terms = [0.0, 0.0, 0.0]
    for span in chunks:
        along, ridge_part = direc[:, span], ridge_row[:, span]
        left = resid[:, span] - step_col * (transposed_rest(span) + ridge_part * along)
        ahead = scale_row[:, span] * left
        resid[:, span] = left
        solut[:, span] = step_col * along
        scal[:, span] = ahead
        ridged = ridge_part * ahead
        added = (over(left * ahead), over(ridged * ahead), over(ridged * along))
        terms = [term + more for term, more in zip(terms, added)]

    def settle(sums_of):
        norm_next, own_ridge, cross = sums_of
        ratio = norm_next / norm
        return ratio, [norm_next, own_ridge + ratio * (2.0 * cross + ratio * ridge), ratio]

    low = scal[...].astype(jnp.bfloat16)
    _, _, step_col, ratio_col = filtered_sum(1, low, terms, slice(0, plan.width), settle)

    def put(out, tile, value):
        out[(tile + 1) * LANES:(tile + 2) * LANES, :] = value

    held = {}
    for span in chunks:
        along = scal[:, span] + ratio_col * direc[:, span]
        ahead = solut[:, span] + step_col * along
        left = resid[:, span] - step_col * (transposed_rest(span) + ridge_row[:, span] * along)
        for low in range(0, span.stop - span.start, LANES):
            held[(span.start + low) // LANES] = (ahead[:, low:low + LANES].T, left[:, low:low + LANES].T)
        for tile in [tile for tile in held if tile < plan.full]:
            new_ahead, new_left = held.pop(tile)
            put(solution_out, tile, new_ahead)
            put(residual_out, tile, new_left)
    mixed, last = held[plan.full], held[plan.full + 1]
    for out, edge, end in ((solution_out, mixed[0], last[0]), (residual_out, mixed[1], last[1])):
        out[:LANES, :] = edge
        put(out, plan.full, edge)
        low = pl.multiple_of((plan.full + 1) * LANES + offset, plan.rest)
        out[pl.ds(low, plan.rest), :] = end[:plan.rest]

    all_of(shown.at[others], show_send, show_recv).wait_send()
    all_of(seen_weight.at[others], weight_send, weight_recv).wait_send()
    for part, (low, size) in enumerate(((0, plan.cut), (plan.cut, plan.mixed_at - plan.cut), (plan.mixed_at, LANES))):
        all_of(block.at[others, :, pl.ds(low, size)], block_send.at[part], loose_recv).wait_send()
    all_of(loose.at[others], block_send.at[3], loose_recv).wait_send()
    all_of(early.at[core, near_others], early_send, early_recv).wait_send()
    all_of(early.at[core], early_relay_send, early_relay_recv).wait_send()
    for turn in range(2):
        all_of(received.at[turn], pair_send.at[turn], pair_recv.at[turn, 0]).wait_send()
        all_of(sent.at[turn, :, near_others], fold_send.at[turn], fold_recv.at[turn, 0]).wait_send()
        all_of(sent_terms.at[turn, near_others], term_send.at[turn], term_recv.at[turn]).wait_send()
        all_of(whole_parts.at[pl.ds(0, 3)], whole_send.at[turn], whole_recv.at[turn]).wait_send()
        all_of(crossed.at[turn, :, 0], cross_send.at[turn], cross_recv.at[turn, 0]).wait_send()
        middle_copy(turn, 1).wait_send()
        for group in range(len(plan.groups)):
            everyone = gathered.at[turn, group, core, near_others, :, pl.ds(0, extent(group))]
            all_of(everyone, gather_send.at[turn, group], gather_recv.at[turn, group]).wait_send()
            relay_copy(turn, group, core).wait_send()


def far(value):
    return pltpu.with_memory_space_constraint(value, pltpu.HBM)


def fused_shards(design, observed, slab_counts, gap_mask, filter_taps, kaula_diag, precond):
    epoch_rows, coef_rows = design.shape
    columns = observed.shape[1]
    slabs, coefs = lax.axis_size("tm"), lax.axis_size("coef")
    plan = Plan(slabs, coefs, epoch_rows, coef_rows, columns)
    wide, chips, message = plan.width, plan.chips, plan.message
    half_slabs, half_chips = slabs // 2, chips // 2
    f32, bf16 = jnp.float32, jnp.bfloat16
    vmem = pl.BlockSpec(memory_space=pltpu.VMEM)
    hbm = pl.BlockSpec(memory_space=pltpu.HBM)
    sem = pltpu.SemaphoreType.DMA
    shape = jax.ShapeDtypeStruct((wide + LANES, columns), f32)
    tiles = (plan.tiles, LANES)
    outs = pl.pallas_call(
        functools.partial(fused, plan),
        out_shape=(shape, shape),
        in_specs=[hbm, hbm, hbm, pl.BlockSpec(memory_space=pltpu.SMEM), hbm, hbm, hbm],
        out_specs=(vmem, vmem),
        scratch_shapes=[
            pltpu.VMEM((epoch_rows, columns), f32),
            pltpu.VMEM((epoch_rows // LANES, LANES), jnp.int32),
            pltpu.VMEM((1, LANES), f32),
            pltpu.VMEM(tiles, f32),
            pltpu.VMEM(tiles, f32),
            pltpu.VMEM((slabs, epoch_rows, wide), bf16),
            pltpu.VMEM((slabs, wide, epoch_rows), bf16),
            pltpu.VMEM((slabs, 2, epoch_rows, LANES), bf16),
            pltpu.VMEM((slabs, epoch_rows + plan.packed_rows, LANES), bf16),
            pltpu.VMEM((slabs, plan.packed_rows, LANES), bf16),
            pltpu.VMEM((chips, GROUP, epoch_rows), f32),
            pltpu.VMEM((slabs, GROUP, epoch_rows), f32),
            pltpu.VMEM((slabs, epoch_rows // LANES, LANES), f32),
            pltpu.VMEM((2, half_chips, GROUP, slabs * epoch_rows), bf16),
            pltpu.VMEM((2, slabs, columns, epoch_rows), f32),
            pltpu.VMEM((2, half_slabs, columns, epoch_rows), f32),
            pltpu.VMEM((half_slabs, half_chips, PAIRED, epoch_rows), f32),
            pltpu.VMEM((2, half_slabs, half_chips, PAIRED, epoch_rows), bf16),
            pltpu.VMEM((2, half_slabs, half_chips, PAIRED, epoch_rows), bf16),
            pltpu.VMEM((2, half_chips, PAIRED, LANES), bf16),
            pltpu.VMEM((2, half_chips, PAIRED, LANES), bf16),
            pltpu.VMEM((2, 2, 2, PAIRED, LANES), f32),
            pltpu.VMEM((4, PAIRED, LANES), f32),
            pltpu.VMEM((2, half_slabs, 2, PAIRED, epoch_rows), f32),
            pltpu.VMEM((2, plan.half_blocks + 2, PAIRED, LANES), f32),
            pltpu.VMEM((plan.half_blocks, PAIRED, LANES), f32),
            pltpu.VMEM((columns, slabs * epoch_rows), bf16),
            pltpu.VMEM((2, len(plan.groups), 2, half_chips, PAIRED, message), bf16),
            pltpu.VMEM((columns, wide), f32),
            pltpu.VMEM((columns, wide), f32),
            pltpu.VMEM((columns, wide), f32),
            pltpu.VMEM((columns, wide), f32),
            pltpu.VMEM((columns, wide), f32),
            pltpu.VMEM((2, plan.half_blocks, PAIRED, LANES), f32),
            sem(()), sem((5,)), sem(()), sem((4,)), sem((2, slabs)), *[sem(())] * 5,
            sem(()), sem(()), sem(()), sem(()),
            sem((2,)), sem((2, half_slabs)), sem((2,)), sem((2, half_slabs)), sem((2,)), sem((2,)), sem((2,)), sem((2,)), sem((2,)), sem((2, half_slabs)),
            sem((2,)), sem((2,)), *[sem((2, len(plan.groups)))] * 4,
        ],
        compiler_params=pltpu.CompilerParams(
            collective_id=0, has_side_effects=True, vmem_limit_bytes=48 * 1024 * 1024
        ),
    )(
        design, far(observed), far(gap_mask.reshape(-1, LANES)), slab_counts, far(filter_taps[None]),
        far(kaula_diag.reshape(tiles)), far(precond.reshape(tiles)),
    )
    owner = lax.axis_index("tm")
    low = owner * plan.owned - plan.first_tile(owner) * LANES
    return tuple(lax.dynamic_slice_in_dim(out, low, plan.owned, 0) for out in outs)


def shards(*arrays):
    design, observed, filter_taps = arrays[0], arrays[1], arrays[4]
    sizes = (lax.axis_size("tm"), lax.axis_size("coef"), *design.shape, observed.shape[1], filter_taps.shape[0])
    return fused_shards(*arrays) if fits(*sizes) else general_shards(*arrays)


def solution(mesh):
    placed = (P("tm", "coef"), P("tm", None), P("tm"), P("tm"), P(), P("coef"), P("coef"))
    return jax.shard_map(
        shards,
        mesh=mesh,
        in_specs=placed,
        out_specs=(P(("coef", "tm"), None), P(("coef", "tm"), None)),
        check_vma=False,
    )
```
